128 devices in a mesh: dp: 16 (over z, x_lo, core), tensor: 8 (over x_hi, y).
Axes of the slice: x: 4 (x_hi: 2, x_lo: 2; x = x_hi * 2 + x_lo), y: 4, z: 4, core: 2. Of those that a mesh axis runs over, the one named last changes fastest.
Arguments:
- prompt_ids: int32 [16384], P(('dp', 'tensor')), may hold values from 0 to 128255
- prompt_lengths: int32 [32], replicated, may hold values from 1 to 512, as said below
- embed_table: bfloat16 [4096, 128256], P(('dp', 'tensor')), may hold values from -4 to 4
- norm_gain: float32 [4096], replicated, may hold values from 0.5 to 1.5
- w_query: bfloat16 [4096, 4096], P('dp', 'tensor'), may hold values from -3 to 3
- w_key: bfloat16 [4096, 1024], P('dp', 'tensor'), may hold values from -1 to 1
- w_value: bfloat16 [4096, 1024], P('dp', 'tensor'), may hold values from -0.09375 to 0.09375
- w_out: bfloat16 [4096, 4096], P('tensor', 'dp'), may hold values from -0.09375 to 0.09375
Outputs:
- hidden: bfloat16 [16384, 4096], P(('dp', 'tensor'))
- kv_cache: bfloat16 [128, 2, 512, 256], P(('dp', 'tensor'))
The draws below stay inside these ranges and needn't reach their ends.
Inputs may be any that keep to these rules, and one draw needn't show every extreme that they name: `prompt_lengths`: each group's prompt has 1 to 512 live tokens, and some group's has 512.
All inputs are finite; a program needn't handle non-finite values.
Results may differ from the reference program's by a relative error of at most 0.0095.
Values may be sent and summed in bfloat16 or wider, within the bound.
No kernel may reach another device: no remote copies, remote signals or barrier semaphores. Data moves between devices by JAX's collectives and lax.ppermute only.
A program may use at most 192 MiB of HBM per device.

```python
import math
import jax
import jax.numpy as jnp
import numpy as np
from jax import lax

D = 4096
HEADS = 32
KVH = 8
HD = 128
VOCAB = 128256
TPG = 4
PROMPT = 512
GROUPS = 32
TOKENS = 16384
N_TENSOR = 8


def draw_prompt_lengths(key, part):
    base = jax.random.randint(jax.random.fold_in(key, 11), (GROUPS,), 1, PROMPT + 1)
    chosen = jax.random.randint(jax.random.fold_in(key, 12), (), 0, GROUPS)
    return jnp.where(jnp.arange(GROUPS) == chosen, PROMPT, base).astype(jnp.int32)


def draw_embed_table(key, part):
    base = jnp.clip(jax.random.normal(jax.random.fold_in(key, 21), (D, VOCAB), jnp.float32), -6.0, 6.0)
    return jnp.clip(0.2 * base, -4.0, 4.0).astype(jnp.bfloat16)


def shared_keys(key):
    base = jax.random.normal(jax.random.fold_in(key, 31), (D, KVH * HD), jnp.float32)
    return jnp.clip(base, -6.0, 6.0) * D ** (-0.5)


def draw_w_key(key, part):
    return jnp.clip(shared_keys(key), -1.0, 1.0).astype(jnp.bfloat16)


def draw_w_query(key, part):
    own = jnp.clip(jax.random.normal(jax.random.fold_in(key, 32), (D, D), jnp.float32), -6.0, 6.0) * D ** (-0.5)
    return jnp.clip(own, -3.0, 3.0).astype(jnp.bfloat16)


def set_ends(values, own_key, smallest, top_value):
    longest = values.shape.index(max(values.shape))
    spots = []
    for shift in (0, 1):
        where = [jax.random.randint(jax.random.fold_in(own_key, axis), (), 0, length) for axis, length in enumerate(values.shape)]
        where[longest] = (where[longest] + shift) % values.shape[longest]
        spots.append(tuple(where))
    return values.at[spots[0]].set(smallest).at[spots[1]].set(top_value)


def level_of(stream_key, shape, pieces, least, top_value):
    gain, own = 1.0, jax.random.fold_in(stream_key, 6)
    for dim, blocks in pieces:
        heights = jnp.exp(jax.random.uniform(jax.random.fold_in(own, dim), (blocks,), jnp.float32, least / len(pieces), top_value / len(pieces)))
        gain = gain * jnp.repeat(heights, shape[dim] // blocks).reshape([-1 if axis == dim else 1 for axis in range(len(shape))])
    return gain


def skewed_wide(stream_key, extent, number_of, slope):
    portions = [min(1 << octave, number_of + 1 - (1 << octave)) * (1 << 20) // math.isqrt((1 << octave) ** slope) + 1 for octave in range((number_of + 1).bit_length()) if 1 << octave <= number_of]
    width = 1 + sum(portions) // (1 << 30)
    grid = np.cumsum(np.array([max(1, weight // width) for weight in portions]))
    lot = jax.random.randint(jax.random.fold_in(stream_key, 1), extent, 0, int(grid[len(portions) - 1]))
    start = jnp.left_shift(1, jnp.searchsorted(jnp.asarray(grid, jnp.int32), lot, side="right").astype(jnp.int32))
    rank = start - 1 + jax.random.randint(jax.random.fold_in(stream_key, 4), extent, 0, 1 << 30) % jnp.minimum(start, number_of + 1 - start)
    return jax.random.permutation(jax.random.fold_in(stream_key, 2), number_of)[rank].astype(jnp.int32)


def scatter_about(stream_key, shape, deviation, bound, split=(), kind=jnp.bfloat16):
    entries = jax.random.normal(stream_key, shape, jnp.float32) * deviation
    if len(split) > 0:
        entries = level_of(stream_key, shape, split, -0.22, 0.18) * entries
    return jnp.clip(entries, min=-bound, max=bound).astype(kind)


def setup_inputs(seed: int = 0) -> dict:
    arg_keys = jax.random.split(jax.random.key(seed), 9)
    return {
        "prompt_ids": set_ends(skewed_wide(arg_keys[0], (TOKENS,), VOCAB, 2), jax.random.fold_in(arg_keys[0], 3), 0, VOCAB - 1).astype(jnp.int32),
        "prompt_lengths": draw_prompt_lengths(jax.random.fold_in(arg_keys[8], 71), 0),
        "embed_table": draw_embed_table(jax.random.fold_in(arg_keys[8], 71), 0),
        "norm_gain": jnp.clip(1.0 + 0.1 * jax.random.normal(arg_keys[3], (D,), jnp.float32), 0.5, 1.5),
        "w_query": draw_w_query(jax.random.fold_in(arg_keys[8], 71), 0),
        "w_key": draw_w_key(jax.random.fold_in(arg_keys[8], 71), 0),
        "w_value": scatter_about(arg_keys[6], (D, KVH * HD), D ** -0.5, 0.09375, ((0, 16), (1, 8))),
        "w_out": scatter_about(arg_keys[7], (D, D), D ** -0.5, 0.09375, ((0, 8), (1, 16))),
    }


norm_eps = 1e-05
rope_theta = 500000.0

def rotate(heads_in, positions):
    half = heads_in.shape[-1] // 2
    freq = rope_theta ** (-2.0 * jnp.arange(half, dtype=jnp.float32) / heads_in.shape[-1])
    angle = positions.astype(jnp.float32)[:, None] * freq[None, :]
    cosine = jnp.cos(angle)[:, None, :]
    sine = jnp.sin(angle)[:, None, :]
    first = heads_in[..., :half]
    second = heads_in[..., half:]
    return jnp.concatenate([first * cosine - second * sine, second * cosine + first * sine], axis=-1)

def attend(query_rot, key_rot, value_rows, length):
    row_count = query_rot.shape[0]
    block = min(512, row_count)
    positions = jnp.arange(row_count, dtype=jnp.int32)
    keys_wide = key_rot.astype(jnp.float32)
    values_wide = value_rows.astype(jnp.float32)

    def one_block(offset):
        queries = lax.dynamic_slice_in_dim(query_rot, offset, block, 0).astype(jnp.float32)
        scores = jnp.einsum('qhgd,khd->hgqk', queries, keys_wide) / jnp.sqrt(jnp.float32(HD))
        query_pos = offset + jnp.arange(block, dtype=jnp.int32)
        allowed = (positions[None, :] <= query_pos[:, None]) & (positions[None, :] < length)
        scores = jnp.where(allowed, scores, -1e+30)
        biggest = lax.optimization_barrier(jnp.max(scores, axis=-1, keepdims=True))
        expd = jnp.exp(scores - biggest)
        weights = (expd / lax.optimization_barrier(jnp.sum(expd, axis=-1, keepdims=True))).astype(jnp.bfloat16)
        result = jnp.einsum('hgqk,khd->qhgd', weights.astype(jnp.float32), values_wide)
        return result.astype(jnp.bfloat16)
    starts = jnp.arange(0, row_count, block, dtype=jnp.int32)
    outs = lax.map(one_block, starts)
    return outs.reshape(row_count, -1)

def layer_group(token_ids, length, embed_table, norm_gain, w_query, w_key, w_value, w_out):
    row_count = token_ids.shape[0]
    tokens_in = jnp.take(embed_table, token_ids, axis=1).T
    wide_in = tokens_in.astype(jnp.float32)
    scale = lax.rsqrt(lax.optimization_barrier(jnp.mean(wide_in * wide_in, axis=1, keepdims=True)) + norm_eps)
    normed = (wide_in * scale * norm_gain.astype(jnp.float32)[None, :]).astype(jnp.bfloat16)
    query = jnp.dot(normed, w_query, preferred_element_type=jnp.float32)
    key_raw = jnp.dot(normed, w_key, preferred_element_type=jnp.float32)
    value_raw = jnp.dot(normed, w_value, preferred_element_type=jnp.float32)
    positions = jnp.arange(row_count, dtype=jnp.int32)
    query_rot = rotate(query.reshape(row_count, HEADS, HD), positions).astype(jnp.bfloat16)
    key_rot = rotate(key_raw.reshape(row_count, KVH, HD), positions).astype(jnp.bfloat16)
    value_rows = value_raw.reshape(row_count, KVH, HD).astype(jnp.bfloat16)
    attended = attend(query_rot.reshape(row_count, KVH, HEADS // KVH, HD), key_rot, value_rows, length)
    blocks = N_TENSOR // TPG
    block_width = D // N_TENSOR
    attended_four = attended.reshape(row_count, blocks, TPG, block_width).astype(jnp.float32)
    out_four = w_out.reshape(blocks, TPG, block_width, D).astype(jnp.float32)
    parts = jnp.einsum('rkmw,kmwd->mrd', attended_four, out_four)
    parts = lax.optimization_barrier(parts.astype(jnp.bfloat16)).astype(jnp.float32)
    hidden = (wide_in + lax.optimization_barrier(jnp.sum(parts, axis=0))).astype(jnp.bfloat16)
    kv_width = KVH * HD // N_TENSOR

    def member_major(table_rows):
        shaped = table_rows.reshape(row_count, blocks, TPG, kv_width)
        return shaped.transpose(2, 0, 1, 3).reshape(TPG, row_count, blocks * kv_width)
    cache = jnp.stack([member_major(key_rot.reshape(row_count, KVH * HD)), member_major(value_rows.reshape(row_count, KVH * HD))], axis=1)
    return (hidden, cache)

def reference(prompt_ids, prompt_lengths, embed_table, norm_gain, w_query, w_key, w_value, w_out):
    grouped_ids = prompt_ids.reshape(GROUPS, PROMPT)

    def one_group(pair):
        return layer_group(pair[0], pair[1], embed_table, norm_gain, w_query, w_key, w_value, w_out)
    hidden, cache = lax.map(one_group, (grouped_ids, prompt_lengths))
    return (hidden.reshape(GROUPS * PROMPT, D), cache.reshape(GROUPS * TPG, 2, PROMPT, KVH * HD // TPG))
```

```python
import functools

import jax
import jax.numpy as jnp
from jax import lax
from jax.experimental import pallas as pl
from jax.experimental.pallas import tpu as pltpu
from jax.sharding import Mesh
from jax.sharding import PartitionSpec as P

HEADS = 32
KVH = 8
HD = 128
TPG = 4
TENSOR = ("tensor_0", "tensor_1")
DP_TENSOR = ("dp_0", "dp_1", "dp_2", "tensor_0", "tensor_1")
DP = ("dp_0", "dp_1", "dp_2")
RING = "tensor_1"
LANES = 128

norm_eps = 1e-05
rope_theta = 500000.0


def swapped(block, axis, apart):
    count = lax.axis_size(axis)
    route = []
    for low in range(count):
        high = low | 1 << apart
        if high != low and high < count:
            route += [(low, high), (high, low)]
    return lax.ppermute(block, axis, route)


def ordered_pair(mine, theirs, bit_index):
    upper_half = lax.axis_index(TENSOR) >> bit_index & 1 == 1
    first_half = jnp.where(upper_half, theirs, mine)
    second_half = jnp.where(upper_half, mine, theirs)
    return jnp.concatenate([first_half, second_half], axis=0)


def collect_blocks(shard):
    stacked = shard[None]
    return ordered_pair(stacked, swapped(stacked, TENSOR, 2), 2)


def lane_gather(block, lanes):
    dims = lax.GatherDimensionNumbers(
        offset_dims=(),
        collapsed_slice_dims=(1,),
        start_index_map=(1,),
        operand_batching_dims=(0,),
        start_indices_batching_dims=(0,),
    )
    return lax.gather(
        block,
        lanes[..., None],
        dims,
        slice_sizes=(1, 1),
        mode=lax.GatherScatterMode.PROMISE_IN_BOUNDS,
    )


def lookup_kernel(slots_ref, lanes_ref, table_ref, out_ref, tiles):
    columns = table_ref.shape[0]
    tile_count = tiles.shape[0] // 2
    lane = lax.broadcasted_iota(jnp.int32, (columns, LANES), 1).astype(jnp.int16)
    left = lane < jnp.int16(LANES // 2)
    unroll = next(u for u in (6, 4, 3, 2, 1) if tile_count % u == 0)

    def prepare(step, carry):
        for u in range(unroll):
            t = step * unroll + u
            tile = table_ref[:, pl.ds(pl.multiple_of(t * LANES, LANES), LANES)]
            tiles[t] = tile
            tiles[t + tile_count] = lane_gather(tile, lane ^ jnp.int16(LANES // 2))
        return carry

    lax.fori_loop(0, tile_count // unroll, prepare, 0)
    groups, copies, _, row_count = out_ref.shape
    per_group = row_count // LANES

    def one_block(block, carry):
        first = block * LANES
        wanted = jnp.broadcast_to(lanes_ref[pl.ds(block, 1), :], (columns, LANES)).astype(jnp.int16)
        picked = jnp.zeros((columns, LANES), jnp.bfloat16)
        for i in range(0, LANES, 2):
            pair = jnp.where(left, tiles[slots_ref[first + i]], tiles[slots_ref[first + i + 1]])
            picked = jnp.where(lane >= jnp.int16(i), lane_gather(pair, wanted), picked)
        group = lax.div(block, per_group)
        place = pl.multiple_of(lax.rem(block, per_group) * LANES, LANES)
        for copy in range(copies):
            out_ref[group, copy, :, pl.ds(place, LANES)] = picked
        return carry

    lax.fori_loop(0, groups * per_group, one_block, 0)


def lookup(embed_table, token_ids, group_count):
    columns, vocab_size = embed_table.shape
    tile_count = vocab_size // LANES
    count = token_ids.shape[0]
    odd = jnp.arange(count, dtype=jnp.int32) & 1
    lane = token_ids & (LANES - 1)
    half = LANES // 2
    slots = lax.shift_right_logical(token_ids, 7) + tile_count * (lax.shift_right_logical(lane, 6) ^ odd)
    lanes = ((lane & (half - 1)) | (odd * half)).reshape(count // LANES, LANES)
    return pl.pallas_call(
        lookup_kernel,
        out_shape=jax.ShapeDtypeStruct(
            (group_count, TPG, columns, count // group_count), jnp.bfloat16
        ),
        in_specs=[
            pl.BlockSpec(memory_space=pltpu.SMEM),
            pl.BlockSpec(memory_space=pltpu.VMEM),
            pl.BlockSpec(memory_space=pltpu.VMEM),
        ],
        out_specs=pl.BlockSpec(memory_space=pltpu.VMEM),
        scratch_shapes=[pltpu.VMEM((2 * tile_count, columns, LANES), jnp.bfloat16)],
        compiler_params=pltpu.CompilerParams(vmem_limit_bytes=40 * 2**20),
        cost_estimate=pl.CostEstimate(
            flops=30_000_000_000, bytes_accessed=embed_table.size * 2, transcendentals=0
        ),
    )(slots, lanes, embed_table)


def attention_kernel(length_ref, proj_ref, cos_ref, sin_ref, attended_ref, cache_ref):
    row_count = proj_ref.shape[0]
    q_heads = HEADS // KVH
    cosine = cos_ref[...]
    sine = sin_ref[...]

    def rotate(part):
        return (part * cosine + pltpu.roll(part, HD // 2, 1) * sine).astype(jnp.bfloat16)

    key_rot = rotate(proj_ref[:, q_heads * HD : (q_heads + 1) * HD])
    value = proj_ref[:, (q_heads + 1) * HD : (q_heads + 2) * HD].astype(jnp.bfloat16)
    cache_ref[0] = key_rot
    cache_ref[1] = value
    length = length_ref[0]
    block = min(256, row_count)
    root = jnp.float32(HD) ** 0.5
    for h in range(q_heads):
        query = rotate(proj_ref[:, h * HD : (h + 1) * HD])
        for start in range(0, row_count, block):
            keys = start + block
            scores = (
                lax.dot_general(
                    query[start : start + block],
                    key_rot[:keys],
                    (((1,), (1,)), ((), ())),
                    preferred_element_type=jnp.float32,
                )
                / root
            )
            q_pos = start + lax.broadcasted_iota(jnp.int32, (block, keys), 0)
            k_pos = lax.broadcasted_iota(jnp.int32, (block, keys), 1)
            scores = jnp.where((k_pos <= q_pos) & (k_pos < length), scores, -1e30)
            expd = jnp.exp(scores - jnp.max(scores, axis=-1, keepdims=True))
            weights = (expd / jnp.sum(expd, axis=-1, keepdims=True)).astype(jnp.bfloat16)
            attended_ref[start : start + block, h * HD : (h + 1) * HD] = jnp.dot(
                weights, value[:keys], preferred_element_type=jnp.float32
            ).astype(jnp.bfloat16)


def rotated_attention(projected, length, cosine, sine):
    row_count, blocks, width = projected.shape
    query_width = HEADS // KVH * HD
    flat = projected.reshape(row_count, blocks * width)
    attended, cache = pl.pallas_call(
        attention_kernel,
        grid=(blocks,),
        out_shape=(
            jax.ShapeDtypeStruct((row_count, blocks * query_width), jnp.bfloat16),
            jax.ShapeDtypeStruct((2, row_count, blocks * HD), jnp.bfloat16),
        ),
        in_specs=[
            pl.BlockSpec(memory_space=pltpu.SMEM),
            pl.BlockSpec((row_count, width), lambda k: (0, k)),
            pl.BlockSpec((row_count, HD), lambda k: (0, 0)),
            pl.BlockSpec((row_count, HD), lambda k: (0, 0)),
        ],
        out_specs=(
            pl.BlockSpec((row_count, query_width), lambda k: (0, k)),
            pl.BlockSpec((2, row_count, HD), lambda k: (0, 0, k)),
        ),
        compiler_params=pltpu.CompilerParams(vmem_limit_bytes=40 * 2**20),
        cost_estimate=pl.CostEstimate(
            flops=2_000_000_000, bytes_accessed=6_000_000, transcendentals=2_000_000
        ),
    )(length, flat, cosine, sine)
    return attended, cache


def rope_tables(row_count):
    half = HD // 2
    freq = rope_theta ** (-2.0 * jnp.arange(half, dtype=jnp.float32) / HD)
    angle = jnp.arange(row_count, dtype=jnp.int32).astype(jnp.float32)[:, None] * freq[None, :]
    cosine, sine = jnp.cos(angle), jnp.sin(angle)
    return jnp.concatenate([cosine, cosine], axis=1), jnp.concatenate([-sine, sine], axis=1)


def ring_reduced(attended, weight, quarter):
    place = lax.axis_index(RING)
    count = lax.axis_size(RING)
    half = weight.shape[1] // 2

    def part(turn, columns):
        rows = lax.dynamic_slice_in_dim(attended, (place + turn) % count * quarter, quarter, 0)
        return jnp.dot(rows, columns, preferred_element_type=jnp.float32)

    sums = []
    for way, columns in ((1, weight[:, :half]), (-1, weight[:, half:])):
        route = [(k, (k + way) % count) for k in range(count)]
        running = part(-way, columns)
        for step in range(1, count):
            running = lax.ppermute(running.astype(jnp.bfloat16), RING, route)
            running = running.astype(jnp.float32) + part(-way * (step + 1), columns)
        sums.append(running)
    return jnp.concatenate(sums, axis=1)


def shards(prompt_ids, prompt_lengths, embed_table, norm_gain, w_query, w_key, w_value, w_out):
    quarter = prompt_ids.shape[0]
    row_count = quarter * TPG
    devices = lax.axis_size(DP_TENSOR)
    columns = embed_table.shape[0]
    model_width = columns * devices
    group_count = devices // TPG
    member = lax.axis_index(TENSOR) % TPG
    group_index = (
        lax.axis_index(DP) * (lax.axis_size(TENSOR) // TPG) + lax.axis_index(TENSOR) // TPG
    )
    length = lax.dynamic_slice_in_dim(prompt_lengths, group_index, 1, 0)
    cosine, sine = rope_tables(row_count)

    packed = jnp.concatenate([w_query, w_key, w_value], axis=1)
    w_in = lax.all_gather(collect_blocks(packed), DP, axis=1, tiled=True)
    w_back = lax.all_gather(collect_blocks(w_out), DP, axis=2, tiled=True)

    all_ids = lax.all_to_all(
        jnp.broadcast_to(prompt_ids[None], (devices, quarter)),
        DP_TENSOR,
        split_axis=0,
        concat_axis=0,
        tiled=True,
    ).reshape(-1)
    outgoing = lookup(embed_table, all_ids, group_count)
    arrived = lax.all_to_all(
        outgoing.reshape(devices, columns, row_count),
        DP_TENSOR,
        split_axis=0,
        concat_axis=0,
        tiled=True,
    )
    tokens_t = arrived.reshape(model_width, row_count)
    wide = tokens_t.astype(jnp.float32)
    scale = lax.rsqrt(jnp.mean(wide * wide, axis=0, keepdims=True) + norm_eps)
    normed_t = (wide * scale * norm_gain[:, None]).astype(jnp.bfloat16)
    own_rows = lax.dynamic_slice_in_dim(tokens_t, member * quarter, quarter, 1).T

    projected = jnp.einsum("dr,kdc->rkc", normed_t, w_in, preferred_element_type=jnp.float32)
    attended, cache = rotated_attention(projected, length, cosine, sine)
    summed = ring_reduced(attended, w_back.reshape(-1, model_width), quarter)
    hidden = (own_rows.astype(jnp.float32) + summed).astype(jnp.bfloat16)
    return hidden, cache[None]


def solution(mesh):
    split = Mesh(
        mesh.devices.reshape(4, 2, 2, 2, 4), ("dp_0", "dp_1", "dp_2", "tensor_0", "tensor_1")
    )
    placed = (
        P(DP_TENSOR),
        P(),
        P(DP_TENSOR, None),
        P(),
        P(DP, TENSOR),
        P(DP, TENSOR),
        P(DP, TENSOR),
        P(TENSOR, DP),
    )
    return jax.shard_map(
        shards,
        mesh=split,
        in_specs=placed,
        out_specs=(P(DP_TENSOR, None), P(DP_TENSOR, None, None, None)),
        check_vma=False,
    )
```

```python
import functools

import jax
import jax.numpy as jnp
from jax import lax
from jax.experimental import pallas as pl
from jax.experimental.pallas import tpu as pltpu
from jax.sharding import Mesh
from jax.sharding import PartitionSpec as P


HEADS = 32
KVH = 8
HD = 128
TPG = 4
TENSOR = ("tensor_0", "tensor_1")
DP_TENSOR = ("dp_0", "dp_1", "dp_2", "tensor_0", "tensor_1")
DP = ("dp_0", "dp_1", "dp_2")
RING = "tensor_1"
PLANE = ("dp_0", "dp_1", "dp_2", "tensor_0")
LANES = 128

norm_eps = 1e-05
rope_theta = 500000.0


def swapped(block, axis, apart):
    count = lax.axis_size(axis)
    route = []
    for low in range(count):
        high = low | 1 << apart
        if high != low and high < count:
            route += [(low, high), (high, low)]
    return lax.ppermute(block, axis, route)


def ordered_pair(mine, theirs, bit_index):
    upper_half = lax.axis_index(TENSOR) >> bit_index & 1 == 1
    first_half = jnp.where(upper_half, theirs, mine)
    second_half = jnp.where(upper_half, mine, theirs)
    return jnp.concatenate([first_half, second_half], axis=0)


def collect_blocks(shard, after):
    stacked = shard[None]
    theirs, _ = lax.optimization_barrier((swapped(stacked, TENSOR, 2), after))
    return ordered_pair(stacked, theirs, 2)


def lane_gather(block, lanes):
    dims = lax.GatherDimensionNumbers(
        offset_dims=(),
        collapsed_slice_dims=(1,),
        start_index_map=(1,),
        operand_batching_dims=(0,),
        start_indices_batching_dims=(0,),
    )
    return lax.gather(
        block,
        lanes[..., None],
        dims,
        slice_sizes=(1, 1),
        mode=lax.GatherScatterMode.PROMISE_IN_BOUNDS,
    )


def prepare_kernel(table_ref, tiles_ref):
    columns = table_ref.shape[0]
    tile_count = tiles_ref.shape[0] // 2
    lane = lax.broadcasted_iota(jnp.int32, (columns, LANES), 1).astype(jnp.int16)
    unroll = min(32, tile_count)

    def prepare(step, carry):
        first = jnp.minimum(step * unroll, tile_count - unroll)
        for u in range(unroll):
            t = first + u
            tile = table_ref[:, pl.ds(pl.multiple_of(t * LANES, LANES), LANES)]
            tiles_ref[t] = tile
            tiles_ref[t + tile_count] = lane_gather(tile, lane ^ jnp.int16(LANES // 2))
        return carry

    lax.fori_loop(0, -(-tile_count // unroll), prepare, 0)


def lookup_kernel(slots_ref, lanes_ref, tiles_ref, out_ref):
    groups, columns, row_count = out_ref.shape
    lane = lax.broadcasted_iota(jnp.int32, (columns, LANES), 1).astype(jnp.int16)
    left = lane < jnp.int16(LANES // 2)
    per_group = row_count // LANES
    together = 2

    def one_block(step, carry):
        for part in range(together):
            block = step * together + part
            first = block * LANES
            wanted = jnp.broadcast_to(lanes_ref[pl.ds(block, 1), :], (columns, LANES)).astype(
                jnp.int16
            )
            picked = jnp.zeros((columns, LANES), jnp.bfloat16)
            for i in range(0, LANES, 2):
                pair = jnp.where(
                    left, tiles_ref[slots_ref[first + i]], tiles_ref[slots_ref[first + i + 1]]
                )
                picked = jnp.where(lane >= jnp.int16(i), lane_gather(pair, wanted), picked)
            place = pl.multiple_of(lax.rem(block, per_group) * LANES, LANES)
            out_ref[lax.div(block, per_group), :, pl.ds(place, LANES)] = picked
        return carry

    lax.fori_loop(0, groups * per_group // together, one_block, 0)


def prepared(embed_table):
    columns, vocab_size = embed_table.shape
    return pl.pallas_call(
        prepare_kernel,
        out_shape=jax.ShapeDtypeStruct((2 * vocab_size // LANES, columns, LANES), jnp.bfloat16),
        in_specs=[pl.BlockSpec(memory_space=pltpu.VMEM)],
        out_specs=pl.BlockSpec(memory_space=pltpu.VMEM),
        compiler_params=pltpu.CompilerParams(vmem_limit_bytes=4 * 2**20),
        cost_estimate=pl.CostEstimate(
            flops=8_000_000_000, bytes_accessed=embed_table.size * 6, transcendentals=0
        ),
        name="prepare",
    )(embed_table)


def lookup(tiles, token_ids, group_count):
    tile_count, columns = tiles.shape[0] // 2, tiles.shape[1]
    count = token_ids.shape[0]
    odd = jnp.arange(count, dtype=jnp.int32) & 1
    lane = token_ids & (LANES - 1)
    half = LANES // 2
    slots = lax.shift_right_logical(token_ids, 7) + tile_count * (lax.shift_right_logical(lane, 6) ^ odd)
    lanes = ((lane & (half - 1)) | (odd * half)).reshape(count // LANES, LANES)
    return pl.pallas_call(
        lookup_kernel,
        out_shape=jax.ShapeDtypeStruct((group_count, columns, count // group_count), jnp.bfloat16),
        in_specs=[
            pl.BlockSpec(memory_space=pltpu.SMEM),
            pl.BlockSpec(memory_space=pltpu.VMEM),
            pl.BlockSpec(memory_space=pltpu.VMEM),
        ],
        out_specs=pl.BlockSpec(memory_space=pltpu.VMEM),
        compiler_params=pltpu.CompilerParams(vmem_limit_bytes=4 * 2**20),
        cost_estimate=pl.CostEstimate(
            flops=30_000_000_000, bytes_accessed=tiles.size * 2, transcendentals=0
        ),
        name="lookup",
    )(slots, lanes, tiles)


def transposed_product(rows_ref, weight_ref):
    weight = weight_ref[...]
    width = weight.shape[-1]
    return lax.dot_general(
        rows_ref[...],
        weight.reshape(-1, width),
        (((0,), (0,)), ((), ())),
        preferred_element_type=jnp.float32,
    )


def square_sum(rows_ref):
    wide = rows_ref[...].astype(jnp.float32)
    return jnp.sum(wide * wide, axis=0, keepdims=True)


def project_kernel(places_ref, *refs, parts, carried):
    rows, weights = refs[:parts], refs[parts : 2 * parts]
    total_ref, squares_ref = refs[-2:]
    total = sum(transposed_product(r, w) for r, w in zip(rows, weights))
    squares = sum(square_sum(r) for r in rows)
    if carried:
        total += refs[2 * parts][...]
        squares += refs[2 * parts + 1][...]
    total_ref[...] = total
    squares_ref[...] = squares


def weight_spec(weights, turn, share, which):
    dp_count, _, plane, _, columns, width = weights.shape
    return pl.BlockSpec(
        (dp_count // share, 1, plane, 1, columns, width),
        lambda b, places: (which, b, 0, places[turn], 0, 0),
    )


def project(places, weights, parts, carried=None):
    row_count = parts[0][0].shape[1]
    blocks, width = weights.shape[1], weights.shape[-1]
    in_specs = [pl.BlockSpec(rows.shape, lambda b, places: (0, 0)) for rows, *_ in parts]
    in_specs += [weight_spec(weights, *where) for _, *where in parts]
    total_spec = pl.BlockSpec((row_count, width), lambda b, places: (0, b))
    squares_spec = pl.BlockSpec((1, row_count), lambda b, places: (0, 0))
    operands = [rows for rows, *_ in parts] + [weights] * len(parts)
    if carried is not None:
        in_specs += [total_spec, squares_spec]
        operands += list(carried)
    depth = sum(rows.shape[0] for rows, *_ in parts)
    return pl.pallas_call(
        functools.partial(project_kernel, parts=len(parts), carried=carried is not None),
        grid_spec=pltpu.PrefetchScalarGridSpec(
            num_scalar_prefetch=1,
            grid=(blocks,),
            in_specs=in_specs,
            out_specs=(total_spec, squares_spec),
        ),
        out_shape=(
            jax.ShapeDtypeStruct((row_count, blocks * width), jnp.float32),
            jax.ShapeDtypeStruct((1, row_count), jnp.float32),
        ),
        compiler_params=pltpu.CompilerParams(vmem_limit_bytes=52 * 2**20),
        cost_estimate=pl.CostEstimate(
            flops=2 * row_count * depth * blocks * width,
            bytes_accessed=2 * depth * (blocks * width + row_count),
            transcendentals=0,
        ),
        name="project",
    )(places, *operands)


def attention_kernel(
    places_ref, length_ref, *refs, parts, model_width
):
    rows, weights = refs[:parts], refs[parts : 2 * parts]
    total_ref, squares_ref, cos_ref, sin_ref, attended_ref, cache_ref, proj_ref = refs[2 * parts :]
    row_count = cos_ref.shape[0]
    q_heads = HEADS // KVH
    proj_ref[...] = total_ref[...] + sum(transposed_product(r, w) for r, w in zip(rows, weights))
    squares = squares_ref[...] + sum(square_sum(r) for r in rows)
    scale = lax.rsqrt(squares / model_width + norm_eps)
    scale = jnp.transpose(jnp.broadcast_to(scale, (HD, row_count)))
    cosine = cos_ref[...] * scale
    sine = sin_ref[...] * scale

    def rotate(part):
        return (part * cosine + pltpu.roll(part, HD // 2, 1) * sine).astype(jnp.bfloat16)

    key_rot = rotate(proj_ref[:, q_heads * HD : (q_heads + 1) * HD])
    value = (proj_ref[:, (q_heads + 1) * HD : (q_heads + 2) * HD] * scale).astype(jnp.bfloat16)
    cache_ref[0] = key_rot
    cache_ref[1] = value
    length = length_ref[0]
    block = min(256, row_count)
    root = jnp.float32(HD) ** 0.5
    for h in range(q_heads):
        query = rotate(proj_ref[:, h * HD : (h + 1) * HD])
        for start in range(0, row_count, block):
            keys = start + block
            scores = (
                lax.dot_general(
                    query[start : start + block],
                    key_rot[:keys],
                    (((1,), (1,)), ((), ())),
                    preferred_element_type=jnp.float32,
                )
                / root
            )
            q_pos = start + lax.broadcasted_iota(jnp.int32, (block, keys), 0)
            k_pos = lax.broadcasted_iota(jnp.int32, (block, keys), 1)
            scores = jnp.where((k_pos <= q_pos) & (k_pos < length), scores, -1e30)
            expd = jnp.exp(scores - jnp.max(scores, axis=-1, keepdims=True))
            weights_now = (expd / jnp.sum(expd, axis=-1, keepdims=True)).astype(jnp.bfloat16)
            attended_ref[start : start + block, h * HD : (h + 1) * HD] = jnp.dot(
                weights_now, value[:keys], preferred_element_type=jnp.float32
            ).astype(jnp.bfloat16)


def attend(places, weights, parts, carried, length, cosine, sine, model_width):
    row_count = cosine.shape[0]
    blocks, width = weights.shape[1], weights.shape[-1]
    query_width = HEADS // KVH * HD
    in_specs = [pl.BlockSpec(memory_space=pltpu.SMEM)]
    in_specs += [pl.BlockSpec(rows.shape, lambda b, places: (0, 0)) for rows, *_ in parts]
    in_specs += [weight_spec(weights, *where) for _, *where in parts]
    in_specs += [
        pl.BlockSpec((row_count, width), lambda b, places: (0, b)),
        pl.BlockSpec((1, row_count), lambda b, places: (0, 0)),
        pl.BlockSpec((row_count, HD), lambda b, places: (0, 0)),
        pl.BlockSpec((row_count, HD), lambda b, places: (0, 0)),
    ]
    return pl.pallas_call(
        functools.partial(attention_kernel, parts=len(parts), model_width=model_width),
        grid_spec=pltpu.PrefetchScalarGridSpec(
            num_scalar_prefetch=1,
            grid=(blocks,),
            in_specs=in_specs,
            out_specs=(
                pl.BlockSpec((row_count, query_width), lambda b, places: (0, b)),
                pl.BlockSpec((2, row_count, HD), lambda b, places: (0, 0, b)),
            ),
            scratch_shapes=[pltpu.VMEM((row_count, width), jnp.float32)],
        ),
        out_shape=(
            jax.ShapeDtypeStruct((row_count, blocks * query_width), jnp.bfloat16),
            jax.ShapeDtypeStruct((2, row_count, blocks * HD), jnp.bfloat16),
        ),
        compiler_params=pltpu.CompilerParams(vmem_limit_bytes=52 * 2**20),
        cost_estimate=pl.CostEstimate(
            flops=4_000_000_000, bytes_accessed=9_000_000, transcendentals=2_000_000
        ),
        name="attend",
    )(
        places,
        length,
        *[rows for rows, *_ in parts],
        *[weights] * len(parts),
        *carried,
        cosine,
        sine,
    )


def rope_tables(row_count):
    half = HD // 2
    freq = rope_theta ** (-2.0 * jnp.arange(half, dtype=jnp.float32) / HD)
    angle = jnp.arange(row_count, dtype=jnp.int32).astype(jnp.float32)[:, None] * freq[None, :]
    cosine, sine = jnp.cos(angle), jnp.sin(angle)
    return jnp.concatenate([cosine, cosine], axis=1), jnp.concatenate([-sine, sine], axis=1)


def residual_kernel(places_ref, *refs, shares):
    rows_ref, ordered_ref = refs[-2:]
    plane, ring, columns, quarter = ordered_ref.shape
    at = 0
    for turn, share in enumerate(shares):
        count = plane // share
        for piece in range(share):
            ordered_ref[piece * count : (piece + 1) * count, places_ref[turn]] = refs[at][
                ...
            ].reshape(count, columns, quarter)
            at += 1
    width = ring * columns
    for p in range(plane):
        rows_ref[:, p * width : (p + 1) * width] = jnp.transpose(
            ordered_ref[p].reshape(width, quarter).astype(jnp.float32)
        ).astype(jnp.bfloat16)


def residual(places, pieces, columns, quarter):
    flat = [rows for turn in pieces for rows in turn]
    depth = sum(rows.shape[0] for rows in flat)
    ring = len(pieces)
    return pl.pallas_call(
        functools.partial(residual_kernel, shares=[len(turn) for turn in pieces]),
        grid_spec=pltpu.PrefetchScalarGridSpec(
            num_scalar_prefetch=1,
            grid=(1,),
            in_specs=[
                pl.BlockSpec((rows.shape[0], quarter), lambda i, places: (0, places[0]))
                for rows in flat
            ],
            out_specs=pl.BlockSpec((quarter, depth), lambda i, places: (0, 0)),
            scratch_shapes=[
                pltpu.VMEM((depth // (ring * columns), ring, columns, quarter), jnp.bfloat16)
            ],
        ),
        out_shape=jax.ShapeDtypeStruct((quarter, depth), jnp.bfloat16),
        compiler_params=pltpu.CompilerParams(vmem_limit_bytes=16 * 2**20),
        cost_estimate=pl.CostEstimate(
            flops=1_000_000_000, bytes_accessed=4 * depth * quarter, transcendentals=0
        ),
        name="residual",
    )(places, *flat)


def ring_route(way):
    count = lax.axis_size(RING)
    return [(k, (k + way) % count) for k in range(count)]


def ring_reduced(attended, weight, quarter):
    place = lax.axis_index(RING)
    count = lax.axis_size(RING)
    half = weight.shape[1] // 2
    sums = []
    for way, columns in ((1, weight[:, :half]), (-1, weight[:, half:])):
        product = lax.optimization_barrier(
            jnp.dot(attended, columns, preferred_element_type=jnp.float32).astype(jnp.bfloat16)
        )

        def part(turn):
            return lax.dynamic_slice_in_dim(product, (place + turn) % count * quarter, quarter, 0)

        running = part(-way)
        for step in range(1, count):
            running = lax.ppermute(running.astype(jnp.bfloat16), RING, ring_route(way))
            running = running.astype(jnp.float32) + part(-way * (step + 1)).astype(jnp.float32)
        sums.append(running)
    return jnp.concatenate(sums, axis=1)


def sublayer(prompt_ids, prompt_lengths, embed_table, norm_gain, w_query, w_key, w_value, w_out):
    quarter = prompt_ids.shape[0]
    row_count = quarter * TPG
    devices = lax.axis_size(DP_TENSOR)
    columns = embed_table.shape[0]
    model_width = columns * devices
    group_count = devices // TPG
    dp_count = lax.axis_size(DP)
    place = lax.axis_index(RING)
    ring = lax.axis_size(RING)
    group_index = lax.axis_index(DP) * lax.axis_size("tensor_0") + lax.axis_index("tensor_0")
    length = lax.dynamic_slice_in_dim(prompt_lengths, group_index, 1, 0)
    cosine, sine = rope_tables(row_count)

    depth = w_query.shape[0]
    gain = lax.dynamic_slice_in_dim(norm_gain, lax.axis_index(DP) * depth, depth, 0)
    packed = jnp.concatenate([w_query, w_key, w_value], axis=1).astype(jnp.float32)
    packed = (packed * gain[:, None]).astype(jnp.bfloat16)
    w_in = lax.all_gather(packed, PLANE, axis=0, tiled=True).reshape(
        dp_count, devices // ring // dp_count, devices // ring // dp_count, ring, columns, -1
    )

    all_ids = lax.all_to_all(
        jnp.broadcast_to(prompt_ids[None], (devices, quarter)),
        DP_TENSOR,
        split_axis=0,
        concat_axis=0,
        tiled=True,
    ).reshape(-1)
    tiles = prepared(embed_table)
    outgoing = lookup(tiles, all_ids, group_count)
    w_back = lax.all_gather(collect_blocks(w_out, outgoing), DP, axis=2, tiled=True)
    own = lax.all_to_all(outgoing, PLANE, split_axis=0, concat_axis=0, tiled=True).reshape(
        -1, row_count
    )
    half = own.shape[0] // 2
    low, high = own[:half], own[half:]
    low_before = lax.ppermute(low, RING, ring_route(1))
    high_after = lax.ppermute(high, RING, ring_route(-1))
    high_before = lax.ppermute(high, RING, ring_route(1))
    low_after = lax.ppermute(low, RING, ring_route(-1))
    low_across = lax.ppermute(low_before, RING, ring_route(1))
    high_across = lax.ppermute(high_after, RING, ring_route(-1))

    places = (place + jnp.arange(ring, dtype=jnp.int32)) % ring
    first = project(places, w_in, [(own, 0, 1, 0)])
    second = project(
        places,
        w_in,
        [
            (low_before, ring - 1, 2, 0),
            (high_before, ring - 1, 2, 1),
            (low_after, 1, 2, 0),
            (high_after, 1, 2, 1),
        ],
        first,
    )
    attended, cache = attend(
        places,
        w_in,
        [(low_across, 2, 2, 0), (high_across, 2, 2, 1)],
        second,
        length,
        cosine,
        sine,
        model_width,
    )

    pieces = [[own], [low_after, high_after], [low_across, high_across], [low_before, high_before]]
    pieces, _ = lax.optimization_barrier((pieces, attended))
    own_rows = residual(places, pieces, columns, quarter)

    summed = ring_reduced(attended, w_back.reshape(-1, model_width), quarter)
    hidden = (own_rows.astype(jnp.float32) + summed).astype(jnp.bfloat16)
    return hidden, cache[None]


def solution(mesh):
    split = Mesh(
        mesh.devices.reshape(4, 2, 2, 2, 4), ("dp_0", "dp_1", "dp_2", "tensor_0", "tensor_1")
    )
    placed = (
        P(DP_TENSOR),
        P(),
        P(DP_TENSOR, None),
        P(),
        P(DP, TENSOR),
        P(DP, TENSOR),
        P(DP, TENSOR),
        P(TENSOR, DP),
    )
    return jax.shard_map(
        sublayer,
        mesh=split,
        in_specs=placed,
        out_specs=(P(DP_TENSOR, None), P(DP_TENSOR, None, None, None)),
        check_vma=False,
    )
```

```python
import functools

import jax
import jax.numpy as jnp
from jax import lax
from jax.experimental import pallas as pl
from jax.experimental.pallas import tpu as pltpu
from jax.sharding import Mesh
from jax.sharding import PartitionSpec as P


HEADS = 32
KVH = 8
HD = 128
TPG = 4
TENSOR = ("tensor_0", "tensor_1")
DP_TENSOR = ("dp_0", "dp_1", "dp_2", "tensor_0", "tensor_1")
DP = ("dp_0", "dp_1", "dp_2")
RING = "tensor_1"
PLANE = ("dp_0", "dp_1", "dp_2", "tensor_0")
LANES = 128

norm_eps = 1e-05
rope_theta = 500000.0


def swapped(block, axis, apart):
    count = lax.axis_size(axis)
    route = []
    for low in range(count):
        high = low | 1 << apart
        if high != low and high < count:
            route += [(low, high), (high, low)]
    return lax.ppermute(block, axis, route)


def ordered_pair(mine, theirs, bit_index):
    upper_half = lax.axis_index(TENSOR) >> bit_index & 1 == 1
    first_half = jnp.where(upper_half, theirs, mine)
    second_half = jnp.where(upper_half, mine, theirs)
    return jnp.concatenate([first_half, second_half], axis=0)


def collect_blocks(shard):
    stacked = shard[None]
    theirs = swapped(stacked, TENSOR, 2)
    return ordered_pair(stacked, theirs, 2)


def lane_gather(block, lanes):
    dims = lax.GatherDimensionNumbers(
        offset_dims=(),
        collapsed_slice_dims=(1,),
        start_index_map=(1,),
        operand_batching_dims=(0,),
        start_indices_batching_dims=(0,),
    )
    return lax.gather(
        block,
        lanes[..., None],
        dims,
        slice_sizes=(1, 1),
        mode=lax.GatherScatterMode.PROMISE_IN_BOUNDS,
    )


def lookup_kernel(slots_ref, lanes_ref, table_ref, out_ref, table, tiles, arrived):
    groups, columns, row_count = out_ref.shape
    tile_count = tiles.shape[0] // 2
    slabs = arrived.shape[0]
    slab = tile_count // slabs
    lane = lax.broadcasted_iota(jnp.int32, (columns, LANES), 1).astype(jnp.int16)
    left = lane < jnp.int16(LANES // 2)
    unroll = min(32, slab)

    def incoming(k):
        part = pl.ds(k * slab * LANES, slab * LANES)
        return pltpu.make_async_copy(table_ref.at[:, part], table.at[:, part], arrived.at[k])

    for k in range(slabs):
        incoming(k).start()

    for k in range(slabs):
        incoming(k).wait()

        def prepare(step, carry, k=k):
            first = k * slab + jnp.minimum(step * unroll, slab - unroll)
            for u in range(unroll):
                t = first + u
                tile = table[:, pl.ds(pl.multiple_of(t * LANES, LANES), LANES)]
                tiles[t] = tile
                tiles[t + tile_count] = lane_gather(tile, lane ^ jnp.int16(LANES // 2))
            return carry

        lax.fori_loop(0, -(-slab // unroll), prepare, 0)

    per_group = row_count // LANES
    together = 2

    def one_block(step, carry):
        for part in range(together):
            block = step * together + part
            first = block * LANES
            wanted = jnp.broadcast_to(lanes_ref[pl.ds(block, 1), :], (columns, LANES)).astype(
                jnp.int16
            )
            picked = jnp.zeros((columns, LANES), jnp.bfloat16)
            for i in range(0, LANES, 2):
                pair = jnp.where(
                    left, tiles[slots_ref[first + i]], tiles[slots_ref[first + i + 1]]
                )
                picked = jnp.where(lane >= jnp.int16(i), lane_gather(pair, wanted), picked)
            place = pl.multiple_of(lax.rem(block, per_group) * LANES, LANES)
            out_ref[lax.div(block, per_group), :, pl.ds(place, LANES)] = picked
        return carry

    lax.fori_loop(0, groups * per_group // together, one_block, 0)


def lookup(embed_table, token_ids, group_count):
    columns, vocab_size = embed_table.shape
    tile_count = vocab_size // LANES
    slabs = next(k for k in (6, 4, 3, 2, 1) if tile_count % k == 0)
    count = token_ids.shape[0]
    half = LANES // 2
    odd = jnp.arange(count, dtype=jnp.int32) & 1
    lane = token_ids & (LANES - 1)
    swapped_half = lax.shift_right_logical(lane, 6) ^ odd
    slots = lax.shift_right_logical(token_ids, 7) + tile_count * swapped_half
    lanes = ((lane & (half - 1)) | (odd * half)).reshape(count // LANES, LANES)
    return pl.pallas_call(
        lookup_kernel,
        out_shape=jax.ShapeDtypeStruct((group_count, columns, count // group_count), jnp.bfloat16),
        in_specs=[
            pl.BlockSpec(memory_space=pltpu.SMEM),
            pl.BlockSpec(memory_space=pltpu.VMEM),
            pl.BlockSpec(memory_space=pltpu.HBM),
        ],
        out_specs=pl.BlockSpec(memory_space=pltpu.VMEM),
        scratch_shapes=[
            pltpu.VMEM((columns, vocab_size), jnp.bfloat16),
            pltpu.VMEM((2 * tile_count, columns, LANES), jnp.bfloat16),
            pltpu.SemaphoreType.DMA((slabs,)),
        ],
        compiler_params=pltpu.CompilerParams(vmem_limit_bytes=60 * 2**20),
        cost_estimate=pl.CostEstimate(
            flops=30_000_000_000, bytes_accessed=embed_table.size * 2, transcendentals=0
        ),
        name="lookup",
    )(slots, lanes, embed_table)


def transposed_product(rows_ref, weight_ref):
    weight = weight_ref[...]
    width = weight.shape[-1]
    return lax.dot_general(
        rows_ref[...],
        weight.reshape(-1, width),
        (((0,), (0,)), ((), ())),
        preferred_element_type=jnp.float32,
    )


def square_sum(rows_ref):
    wide = rows_ref[...].astype(jnp.float32)
    return jnp.sum(wide * wide, axis=0, keepdims=True)


def project_kernel(places_ref, *refs, parts, carried):
    rows, weights = refs[:parts], refs[parts : 2 * parts]
    total_ref, squares_ref = refs[-2:]
    total = sum(transposed_product(r, w) for r, w in zip(rows, weights))
    squares = sum(square_sum(r) for r in rows)
    if carried:
        total += refs[2 * parts][...]
        squares += refs[2 * parts + 1][...]
    total_ref[...] = total
    squares_ref[...] = squares


def weight_spec(weights, turn, share, which):
    _, plane, _, columns, width = weights.shape
    return pl.BlockSpec(
        (1, plane // share, 1, columns, width),
        lambda b, places: (b, which, places[turn], 0, 0),
    )


def project(places, weights, parts, carried=None):
    row_count = parts[0][0].shape[1]
    blocks, width = weights.shape[0], weights.shape[-1]
    in_specs = [pl.BlockSpec(rows.shape, lambda b, places: (0, 0)) for rows, *_ in parts]
    in_specs += [weight_spec(weights, *where) for _, *where in parts]
    total_spec = pl.BlockSpec((row_count, width), lambda b, places: (0, b))
    squares_spec = pl.BlockSpec((1, row_count), lambda b, places: (0, 0))
    operands = [rows for rows, *_ in parts] + [weights] * len(parts)
    if carried is not None:
        in_specs += [total_spec, squares_spec]
        operands += list(carried)
    depth = sum(rows.shape[0] for rows, *_ in parts)
    return pl.pallas_call(
        functools.partial(project_kernel, parts=len(parts), carried=carried is not None),
        grid_spec=pltpu.PrefetchScalarGridSpec(
            num_scalar_prefetch=1,
            grid=(blocks,),
            in_specs=in_specs,
            out_specs=(total_spec, squares_spec),
        ),
        out_shape=(
            jax.ShapeDtypeStruct((row_count, blocks * width), jnp.float32),
            jax.ShapeDtypeStruct((1, row_count), jnp.float32),
        ),
        compiler_params=pltpu.CompilerParams(vmem_limit_bytes=52 * 2**20),
        cost_estimate=pl.CostEstimate(
            flops=2 * row_count * depth * blocks * width,
            bytes_accessed=2 * depth * (blocks * width + row_count),
            transcendentals=0,
        ),
        name="project",
    )(places, *operands)


def attention_kernel(
    places_ref, length_ref, *refs, parts, model_width
):
    rows, weights = refs[:parts], refs[parts : 2 * parts]
    total_ref, squares_ref, cos_ref, sin_ref, attended_ref, cache_ref, proj_ref = refs[2 * parts :]
    row_count = cos_ref.shape[0]
    q_heads = HEADS // KVH
    proj_ref[...] = total_ref[...] + sum(transposed_product(r, w) for r, w in zip(rows, weights))
    squares = squares_ref[...] + sum(square_sum(r) for r in rows)
    scale = lax.rsqrt(squares / model_width + norm_eps)
    scale = jnp.transpose(jnp.broadcast_to(scale, (HD, row_count)))
    cosine = cos_ref[...] * scale
    sine = sin_ref[...] * scale

    def rotate(part):
        return (part * cosine + pltpu.roll(part, HD // 2, 1) * sine).astype(jnp.bfloat16)

    key_rot = rotate(proj_ref[:, q_heads * HD : (q_heads + 1) * HD])
    value = (proj_ref[:, (q_heads + 1) * HD : (q_heads + 2) * HD] * scale).astype(jnp.bfloat16)
    cache_ref[0] = key_rot
    cache_ref[1] = value
    length = length_ref[0]
    block = min(256, row_count)
    root = jnp.float32(HD) ** 0.5
    for h in range(q_heads):
        query = rotate(proj_ref[:, h * HD : (h + 1) * HD])
        for start in range(0, row_count, block):
            keys = start + block
            scores = (
                lax.dot_general(
                    query[start : start + block],
                    key_rot[:keys],
                    (((1,), (1,)), ((), ())),
                    preferred_element_type=jnp.float32,
                )
                / root
            )
            q_pos = start + lax.broadcasted_iota(jnp.int32, (block, keys), 0)
            k_pos = lax.broadcasted_iota(jnp.int32, (block, keys), 1)
            scores = jnp.where((k_pos <= q_pos) & (k_pos < length), scores, -1e30)
            expd = jnp.exp(scores - jnp.max(scores, axis=-1, keepdims=True))
            weights_now = (expd / jnp.sum(expd, axis=-1, keepdims=True)).astype(jnp.bfloat16)
            attended_ref[start : start + block, h * HD : (h + 1) * HD] = jnp.dot(
                weights_now, value[:keys], preferred_element_type=jnp.float32
            ).astype(jnp.bfloat16)


def attend(places, weights, parts, carried, length, cosine, sine, model_width):
    row_count = cosine.shape[0]
    blocks, width = weights.shape[0], weights.shape[-1]
    query_width = HEADS // KVH * HD
    in_specs = [pl.BlockSpec(memory_space=pltpu.SMEM)]
    in_specs += [pl.BlockSpec(rows.shape, lambda b, places: (0, 0)) for rows, *_ in parts]
    in_specs += [weight_spec(weights, *where) for _, *where in parts]
    in_specs += [
        pl.BlockSpec((row_count, width), lambda b, places: (0, b)),
        pl.BlockSpec((1, row_count), lambda b, places: (0, 0)),
        pl.BlockSpec((row_count, HD), lambda b, places: (0, 0)),
        pl.BlockSpec((row_count, HD), lambda b, places: (0, 0)),
    ]
    return pl.pallas_call(
        functools.partial(attention_kernel, parts=len(parts), model_width=model_width),
        grid_spec=pltpu.PrefetchScalarGridSpec(
            num_scalar_prefetch=1,
            grid=(blocks,),
            in_specs=in_specs,
            out_specs=(
                pl.BlockSpec((row_count, query_width), lambda b, places: (0, b)),
                pl.BlockSpec((2, row_count, HD), lambda b, places: (0, 0, b)),
            ),
            scratch_shapes=[pltpu.VMEM((row_count, width), jnp.float32)],
        ),
        out_shape=(
            jax.ShapeDtypeStruct((row_count, blocks * query_width), jnp.bfloat16),
            jax.ShapeDtypeStruct((2, row_count, blocks * HD), jnp.bfloat16),
        ),
        compiler_params=pltpu.CompilerParams(vmem_limit_bytes=52 * 2**20),
        cost_estimate=pl.CostEstimate(
            flops=4_000_000_000, bytes_accessed=9_000_000, transcendentals=2_000_000
        ),
        name="attend",
    )(
        places,
        length,
        *[rows for rows, *_ in parts],
        *[weights] * len(parts),
        *carried,
        cosine,
        sine,
    )


def rope_tables(row_count):
    half = HD // 2
    freq = rope_theta ** (-2.0 * jnp.arange(half, dtype=jnp.float32) / HD)
    angle = jnp.arange(row_count, dtype=jnp.int32).astype(jnp.float32)[:, None] * freq[None, :]
    cosine, sine = jnp.cos(angle), jnp.sin(angle)
    return jnp.concatenate([cosine, cosine], axis=1), jnp.concatenate([-sine, sine], axis=1)


def residual_kernel(places_ref, *refs, shares):
    rows_ref, ordered_ref = refs[-2:]
    plane, ring, columns, quarter = ordered_ref.shape
    at = 0
    for turn, share in enumerate(shares):
        count = plane // share
        for piece in range(share):
            ordered_ref[piece * count : (piece + 1) * count, places_ref[turn]] = refs[at][
                ...
            ].reshape(count, columns, quarter)
            at += 1
    width = ring * columns
    for p in range(plane):
        rows_ref[:, p * width : (p + 1) * width] = jnp.transpose(
            ordered_ref[p].reshape(width, quarter).astype(jnp.float32)
        ).astype(jnp.bfloat16)


def residual(places, pieces, columns, quarter):
    flat = [rows for turn in pieces for rows in turn]
    depth = sum(rows.shape[0] for rows in flat)
    ring = len(pieces)
    return pl.pallas_call(
        functools.partial(residual_kernel, shares=[len(turn) for turn in pieces]),
        grid_spec=pltpu.PrefetchScalarGridSpec(
            num_scalar_prefetch=1,
            grid=(1,),
            in_specs=[
                pl.BlockSpec((rows.shape[0], quarter), lambda i, places: (0, places[0]))
                for rows in flat
            ],
            out_specs=pl.BlockSpec((quarter, depth), lambda i, places: (0, 0)),
            scratch_shapes=[
                pltpu.VMEM((depth // (ring * columns), ring, columns, quarter), jnp.bfloat16)
            ],
        ),
        out_shape=jax.ShapeDtypeStruct((quarter, depth), jnp.bfloat16),
        compiler_params=pltpu.CompilerParams(vmem_limit_bytes=16 * 2**20),
        cost_estimate=pl.CostEstimate(
            flops=1_000_000_000, bytes_accessed=4 * depth * quarter, transcendentals=0
        ),
        name="residual",
    )(places, *flat)


def ring_route(way):
    count = lax.axis_size(RING)
    return [(k, (k + way) % count) for k in range(count)]


def product_kernel(places_ref, rows_ref, *refs, ring):
    out_ref = refs[-1]
    width = refs[0].shape[-1]
    for k, weight_ref in enumerate(refs[:-1]):
        _, halves, depth, _ = weight_ref.shape
        total = None
        for half in range(halves):
            block = places_ref[ring] ^ half
            rows = rows_ref[:, pl.ds(pl.multiple_of(block * depth, depth), depth)]
            term = jnp.dot(rows, weight_ref[0, half], preferred_element_type=jnp.float32)
            total = term if total is None else total + term
        out_ref[:, k * width : (k + 1) * width] = total.astype(out_ref.dtype)


def product(places, rows, weights):
    sides, halves, depth, width = weights[0].shape
    row_count = rows.shape[0]
    wide = len(weights) * width
    return pl.pallas_call(
        functools.partial(product_kernel, ring=places.shape[0] - 3),
        grid_spec=pltpu.PrefetchScalarGridSpec(
            num_scalar_prefetch=1,
            grid=(sides,),
            in_specs=[pl.BlockSpec(rows.shape, lambda j, places: (0, 0))]
            + [pl.BlockSpec((1, halves, depth, width), lambda j, places: (j, 0, 0, 0))]
            * len(weights),
            out_specs=pl.BlockSpec((row_count, wide), lambda j, places: (0, j)),
        ),
        out_shape=jax.ShapeDtypeStruct((row_count, sides * wide), jnp.bfloat16),
        compiler_params=pltpu.CompilerParams(vmem_limit_bytes=16 * 2**20),
        cost_estimate=pl.CostEstimate(
            flops=2 * row_count * halves * depth * wide * sides,
            bytes_accessed=2 * (rows.size + halves * depth * wide * sides),
            transcendentals=0,
        ),
        name="product",
    )(places, rows, *weights)


def finish_kernel(where_ref, rows_ref, *refs, width):
    hidden_ref = refs[-1]
    chunks = (len(refs) - 1) // 4
    layers = refs[0].shape[1] // width // 2
    for chunk in range(chunks):
        for core in range(2):
            at = 2 * (2 * chunk + core)
            for j in range(2 * layers):
                z = lax.rem(where_ref[0] + chunks * layers - chunk * layers - j % layers, chunks * layers)
                column = (z * 2 + (where_ref[1] ^ (j // layers))) * 2 + (where_ref[2] ^ core)
                here = slice(j * width, (j + 1) * width)
                there = pl.ds(pl.multiple_of(column * width, width), width)
                total = refs[at][:, here].astype(jnp.float32) + refs[at + 1][:, here].astype(
                    jnp.float32
                )
                hidden_ref[:, there] = (
                    rows_ref[:, there].astype(jnp.float32) + total
                ).astype(jnp.bfloat16)


def finish(where, rows, sums, width):
    return pl.pallas_call(
        functools.partial(finish_kernel, width=width),
        out_shape=jax.ShapeDtypeStruct(rows.shape, jnp.bfloat16),
        in_specs=[pl.BlockSpec(memory_space=pltpu.SMEM)]
        + [pl.BlockSpec(memory_space=pltpu.VMEM)] * (1 + len(sums)),
        out_specs=pl.BlockSpec(memory_space=pltpu.VMEM),
        compiler_params=pltpu.CompilerParams(vmem_limit_bytes=16 * 2**20),
        cost_estimate=pl.CostEstimate(
            flops=4 * rows.size, bytes_accessed=8 * rows.size, transcendentals=0
        ),
        name="finish",
    )(where, rows, *sums)


CHUNKS = 2


def ring_sums(places, attended, weights, quarter):
    place = lax.axis_index(RING)
    count = lax.axis_size(RING)
    each = len(weights[0]) // CHUNKS
    sums = []
    for chunk in range(CHUNKS):
        for side, way in enumerate((1, -1)):
            partial_sums = product(
                places, attended, weights[side][chunk * each : (chunk + 1) * each]
            )

            def part(turn):
                start = (place + turn) % count * quarter
                return lax.dynamic_slice_in_dim(partial_sums, start, quarter, 0)

            running = part(-way)
            for step in range(1, count):
                running = lax.ppermute(running, RING, ring_route(way))
                mine = part(-way * (step + 1))
                if step + 1 < count:
                    running = running.astype(jnp.float32) + mine.astype(jnp.float32)
                    running = running.astype(jnp.bfloat16)
            sums += [running, mine]
    return sums


def sublayer(prompt_ids, prompt_lengths, embed_table, norm_gain, w_query, w_key, w_value, w_out):
    quarter = prompt_ids.shape[0]
    row_count = quarter * TPG
    devices = lax.axis_size(DP_TENSOR)
    columns = embed_table.shape[0]
    model_width = columns * devices
    group_count = devices // TPG
    place = lax.axis_index(RING)
    ring = lax.axis_size(RING)
    group_index = lax.axis_index(DP) * lax.axis_size("tensor_0") + lax.axis_index("tensor_0")
    length = lax.dynamic_slice_in_dim(prompt_lengths, group_index, 1, 0)
    cosine, sine = rope_tables(row_count)

    depth = w_query.shape[0]
    gain = lax.dynamic_slice_in_dim(norm_gain, lax.axis_index(DP) * depth, depth, 0)
    packed = jnp.concatenate([w_query, w_key, w_value], axis=1).astype(jnp.float32)
    packed = (packed * gain[:, None]).astype(jnp.bfloat16)
    w_in = lax.all_gather(collect_blocks(packed), DP, axis=1, tiled=True)
    w_in = w_in.reshape(w_in.shape[0], -1, ring, columns, w_in.shape[-1])
    all_ids = lax.all_to_all(
        jnp.broadcast_to(prompt_ids[None], (devices, quarter)),
        DP_TENSOR,
        split_axis=0,
        concat_axis=0,
        tiled=True,
    ).reshape(-1)
    pieces_x = [w_out]
    for axes, route in (
        ("tensor_0", [(0, 1), (1, 0)]),
        ("dp_1", [(0, 1), (1, 0)]),
        (("dp_1", "tensor_0"), [(0, 3), (1, 2), (2, 1), (3, 0)]),
    ):
        pieces_x.append(lax.ppermute(w_out, axes, route))
    outgoing = lookup(embed_table, all_ids, group_count)
    own = lax.all_to_all(outgoing, PLANE, split_axis=0, concat_axis=0, tiled=True).reshape(
        -1, row_count
    )
    pieces_x, _ = lax.optimization_barrier((pieces_x, outgoing))
    w_mine = [jnp.stack(pieces_x).reshape(2, 2, *w_out.shape)]
    layers = lax.axis_size("dp_0")
    for k in range(1, layers):
        route = [(z, (z + k) % layers) for z in range(layers)]
        w_mine.append(lax.ppermute(w_mine[0], "dp_0", route))
    w_other = []
    for k in range(layers):
        w_other.append(lax.ppermute(w_mine[k], "dp_2", [(0, 1), (1, 0)]))

    places = jnp.concatenate(
        [
            (place + jnp.arange(ring, dtype=jnp.int32)) % ring,
            jnp.stack([lax.axis_index(name) for name in ("tensor_0", "dp_1", "dp_2")]),
        ]
    )
    half = own.shape[0] // 2
    low, high = own[:half], own[half:]
    low_before = lax.ppermute(low, RING, ring_route(1))
    high_after = lax.ppermute(high, RING, ring_route(-1))
    high_before = lax.ppermute(high, RING, ring_route(1))
    low_after = lax.ppermute(low, RING, ring_route(-1))
    low_across = lax.ppermute(low_before, RING, ring_route(1))
    high_across = lax.ppermute(high_after, RING, ring_route(-1))

    first = project(places, w_in, [(own, 0, 1, 0)])
    second = project(
        places,
        w_in,
        [
            (low_before, ring - 1, 2, 0),
            (high_before, ring - 1, 2, 1),
            (low_after, 1, 2, 0),
            (high_after, 1, 2, 1),
        ],
        first,
    )
    attended, cache = attend(
        places,
        w_in,
        [(low_across, 2, 2, 0), (high_across, 2, 2, 1)],
        second,
        length,
        cosine,
        sine,
        model_width,
    )

    pieces = [[own], [low_after, high_after], [low_across, high_across], [low_before, high_before]]
    pieces, _ = lax.optimization_barrier((pieces, attended))
    own_rows = residual(places, pieces, columns, quarter)

    sums = ring_sums(places, attended, (w_mine, w_other), quarter)
    where = jnp.stack([lax.axis_index(name) for name in DP])
    hidden = finish(where, own_rows, sums, w_out.shape[1])
    return hidden, cache[None]


def solution(mesh):
    split = Mesh(
        mesh.devices.reshape(4, 2, 2, 2, 4), ("dp_0", "dp_1", "dp_2", "tensor_0", "tensor_1")
    )
    placed = (
        P(DP_TENSOR),
        P(),
        P(DP_TENSOR, None),
        P(),
        P(DP, TENSOR),
        P(DP, TENSOR),
        P(DP, TENSOR),
        P(TENSOR, DP),
    )
    return jax.shard_map(
        sublayer,
        mesh=split,
        in_specs=placed,
        out_specs=(P(DP_TENSOR, None), P(DP_TENSOR, None, None, None)),
        check_vma=False,
    )
```

```python
import functools

import jax
import jax.numpy as jnp
from jax import lax
from jax.experimental import pallas as pl
from jax.experimental.pallas import tpu as pltpu
from jax.sharding import Mesh
from jax.sharding import PartitionSpec as P


HEADS = 32
KVH = 8
HD = 128
TPG = 4
TENSOR = ("tensor_0", "tensor_1")
DP_TENSOR = ("dp_0", "dp_1", "dp_2", "tensor_0", "tensor_1")
DP = ("dp_0", "dp_1", "dp_2")
RING = "tensor_1"
PLANE = ("dp_0", "dp_1", "dp_2", "tensor_0")
LANES = 128

norm_eps = 1e-05
rope_theta = 500000.0


def swapped(block, axis, apart):
    count = lax.axis_size(axis)
    route = []
    for low in range(count):
        high = low | 1 << apart
        if high != low and high < count:
            route += [(low, high), (high, low)]
    return lax.ppermute(block, axis, route)


def ordered_pair(mine, theirs, bit_index):
    upper_half = lax.axis_index(TENSOR) >> bit_index & 1 == 1
    first_half = jnp.where(upper_half, theirs, mine)
    second_half = jnp.where(upper_half, mine, theirs)
    return jnp.concatenate([first_half, second_half], axis=0)


def collect_blocks(shard):
    stacked = shard[None]
    theirs = swapped(stacked, TENSOR, 2)
    return ordered_pair(stacked, theirs, 2)


def lane_gather(block, lanes):
    dims = lax.GatherDimensionNumbers(
        offset_dims=(),
        collapsed_slice_dims=(1,),
        start_index_map=(1,),
        operand_batching_dims=(0,),
        start_indices_batching_dims=(0,),
    )
    return lax.gather(
        block,
        lanes[..., None],
        dims,
        slice_sizes=(1, 1),
        mode=lax.GatherScatterMode.PROMISE_IN_BOUNDS,
    )


def lookup_kernel(slots_ref, lanes_ref, table_ref, out_ref, table, tiles, arrived):
    groups, columns, row_count = out_ref.shape
    tile_count = tiles.shape[0] // 2
    slabs = arrived.shape[0]
    slab = tile_count // slabs
    lane = lax.broadcasted_iota(jnp.int32, (columns, LANES), 1).astype(jnp.int16)
    left = lane < jnp.int16(LANES // 2)
    unroll = min(32, slab)

    def incoming(k):
        part = pl.ds(k * slab * LANES, slab * LANES)
        return pltpu.make_async_copy(table_ref.at[:, part], table.at[:, part], arrived.at[k])

    for k in range(slabs):
        incoming(k).start()

    for k in range(slabs):
        incoming(k).wait()

        def prepare(step, carry, k=k):
            first = k * slab + jnp.minimum(step * unroll, slab - unroll)
            for u in range(unroll):
                t = first + u
                tile = table[:, pl.ds(pl.multiple_of(t * LANES, LANES), LANES)]
                tiles[t] = tile
                tiles[t + tile_count] = lane_gather(tile, lane ^ jnp.int16(LANES // 2))
            return carry

        lax.fori_loop(0, -(-slab // unroll), prepare, 0)

    per_group = row_count // LANES
    together = 2

    def one_block(step, carry):
        for part in range(together):
            block = step * together + part
            first = block * LANES
            wanted = jnp.broadcast_to(lanes_ref[pl.ds(block, 1), :], (columns, LANES)).astype(
                jnp.int16
            )
            picked = jnp.zeros((columns, LANES), jnp.bfloat16)
            for i in range(0, LANES, 2):
                pair = jnp.where(
                    left, tiles[slots_ref[first + i]], tiles[slots_ref[first + i + 1]]
                )
                picked = jnp.where(lane >= jnp.int16(i), lane_gather(pair, wanted), picked)
            place = pl.multiple_of(lax.rem(block, per_group) * LANES, LANES)
            out_ref[lax.div(block, per_group), :, pl.ds(place, LANES)] = picked
        return carry

    lax.fori_loop(0, groups * per_group // together, one_block, 0)


def lookup(embed_table, token_ids, group_count):
    columns, vocab_size = embed_table.shape
    tile_count = vocab_size // LANES
    slabs = next(k for k in (6, 4, 3, 2, 1) if tile_count % k == 0)
    count = token_ids.shape[0]
    half = LANES // 2
    odd = jnp.arange(count, dtype=jnp.int32) & 1
    lane = token_ids & (LANES - 1)
    swapped_half = lax.shift_right_logical(lane, 6) ^ odd
    slots = lax.shift_right_logical(token_ids, 7) + tile_count * swapped_half
    lanes = ((lane & (half - 1)) | (odd * half)).reshape(count // LANES, LANES)
    return pl.pallas_call(
        lookup_kernel,
        out_shape=jax.ShapeDtypeStruct((group_count, columns, count // group_count), jnp.bfloat16),
        in_specs=[
            pl.BlockSpec(memory_space=pltpu.SMEM),
            pl.BlockSpec(memory_space=pltpu.VMEM),
            pl.BlockSpec(memory_space=pltpu.HBM),
        ],
        out_specs=pl.BlockSpec(memory_space=pltpu.VMEM),
        scratch_shapes=[
            pltpu.VMEM((columns, vocab_size), jnp.bfloat16),
            pltpu.VMEM((2 * tile_count, columns, LANES), jnp.bfloat16),
            pltpu.SemaphoreType.DMA((slabs,)),
        ],
        compiler_params=pltpu.CompilerParams(vmem_limit_bytes=60 * 2**20),
        cost_estimate=pl.CostEstimate(
            flops=30_000_000_000, bytes_accessed=embed_table.size * 2, transcendentals=0
        ),
        name="lookup",
    )(slots, lanes, embed_table)


def transposed_product(rows_ref, weight_ref):
    weight = weight_ref[...]
    width = weight.shape[-1]
    return lax.dot_general(
        rows_ref[...],
        weight.reshape(-1, width),
        (((0,), (0,)), ((), ())),
        preferred_element_type=jnp.float32,
    )


def square_sum(rows_ref):
    wide = rows_ref[...].astype(jnp.float32)
    return jnp.sum(wide * wide, axis=0, keepdims=True)


def project_kernel(places_ref, *refs, parts, carried):
    rows, weights = refs[:parts], refs[parts : 2 * parts]
    total_ref, squares_ref = refs[-2:]
    total = sum(transposed_product(r, w) for r, w in zip(rows, weights))
    squares = sum(square_sum(r) for r in rows)
    if carried:
        total += refs[2 * parts][...]
        squares += refs[2 * parts + 1][...]
    total_ref[...] = total
    squares_ref[...] = squares


def weight_spec(weights, turn, share, which):
    _, plane, _, columns, width = weights.shape
    return pl.BlockSpec(
        (1, plane // share, 1, columns, width),
        lambda b, places: (b, which, places[turn], 0, 0),
    )


def project(places, weights, parts, carried=None):
    row_count = parts[0][0].shape[1]
    blocks, width = weights.shape[0], weights.shape[-1]
    in_specs = [pl.BlockSpec(rows.shape, lambda b, places: (0, 0)) for rows, *_ in parts]
    in_specs += [weight_spec(weights, *where) for _, *where in parts]
    total_spec = pl.BlockSpec((row_count, width), lambda b, places: (0, b))
    squares_spec = pl.BlockSpec((1, row_count), lambda b, places: (0, 0))
    operands = [rows for rows, *_ in parts] + [weights] * len(parts)
    if carried is not None:
        in_specs += [total_spec, squares_spec]
        operands += list(carried)
    depth = sum(rows.shape[0] for rows, *_ in parts)
    return pl.pallas_call(
        functools.partial(project_kernel, parts=len(parts), carried=carried is not None),
        grid_spec=pltpu.PrefetchScalarGridSpec(
            num_scalar_prefetch=1,
            grid=(blocks,),
            in_specs=in_specs,
            out_specs=(total_spec, squares_spec),
        ),
        out_shape=(
            jax.ShapeDtypeStruct((row_count, blocks * width), jnp.float32),
            jax.ShapeDtypeStruct((1, row_count), jnp.float32),
        ),
        compiler_params=pltpu.CompilerParams(vmem_limit_bytes=52 * 2**20),
        cost_estimate=pl.CostEstimate(
            flops=2 * row_count * depth * blocks * width,
            bytes_accessed=2 * depth * (blocks * width + row_count),
            transcendentals=0,
        ),
        name="project",
    )(places, *operands)


def attention_kernel(
    places_ref, length_ref, *refs, parts, model_width
):
    rows, weights = refs[:parts], refs[parts : 2 * parts]
    total_ref, squares_ref, cos_ref, sin_ref, attended_ref, cache_ref, proj_ref = refs[2 * parts :]
    row_count = cos_ref.shape[0]
    q_heads = HEADS // KVH
    proj_ref[...] = total_ref[...] + sum(transposed_product(r, w) for r, w in zip(rows, weights))
    squares = squares_ref[...] + sum(square_sum(r) for r in rows)
    scale = lax.rsqrt(squares / model_width + norm_eps)
    scale = jnp.transpose(jnp.broadcast_to(scale, (HD, row_count)))
    cosine = cos_ref[...] * scale
    sine = sin_ref[...] * scale

    def rotate(part):
        return (part * cosine + pltpu.roll(part, HD // 2, 1) * sine).astype(jnp.bfloat16)

    key_rot = rotate(proj_ref[:, q_heads * HD : (q_heads + 1) * HD])
    value = (proj_ref[:, (q_heads + 1) * HD : (q_heads + 2) * HD] * scale).astype(jnp.bfloat16)
    cache_ref[0] = key_rot
    cache_ref[1] = value
    length = length_ref[0]
    block = min(128, row_count)
    power = 1.4426950408889634 / HD**0.5
    for h in range(q_heads):
        query = rotate(proj_ref[:, h * HD : (h + 1) * HD])
        for start in range(0, row_count, block):
            keys = start + block
            scores = lax.dot_general(
                query[start : start + block],
                key_rot[:keys],
                (((1,), (1,)), ((), ())),
                preferred_element_type=jnp.float32,
            )
            q_pos = start + lax.broadcasted_iota(jnp.int32, (block, 1), 0)
            k_pos = lax.broadcasted_iota(jnp.int32, (block, keys), 1)
            scores = jnp.where(k_pos < jnp.minimum(q_pos + 1, length), scores, -1e30)
            biggest = jnp.max(scores, axis=-1, keepdims=True)
            expd = jnp.exp2((scores - biggest) * power)
            weights_now = expd * (1.0 / jnp.sum(expd, axis=-1, keepdims=True))
            attended_ref[start : start + block, h * HD : (h + 1) * HD] = jnp.dot(
                weights_now.astype(jnp.bfloat16), value[:keys], preferred_element_type=jnp.float32
            ).astype(jnp.bfloat16)


def attend(places, weights, parts, carried, length, cosine, sine, model_width):
    row_count = cosine.shape[0]
    blocks, width = weights.shape[0], weights.shape[-1]
    query_width = HEADS // KVH * HD
    in_specs = [pl.BlockSpec(memory_space=pltpu.SMEM)]
    in_specs += [pl.BlockSpec(rows.shape, lambda b, places: (0, 0)) for rows, *_ in parts]
    in_specs += [weight_spec(weights, *where) for _, *where in parts]
    in_specs += [
        pl.BlockSpec((row_count, width), lambda b, places: (0, b)),
        pl.BlockSpec((1, row_count), lambda b, places: (0, 0)),
        pl.BlockSpec((row_count, HD), lambda b, places: (0, 0)),
        pl.BlockSpec((row_count, HD), lambda b, places: (0, 0)),
    ]
    return pl.pallas_call(
        functools.partial(attention_kernel, parts=len(parts), model_width=model_width),
        grid_spec=pltpu.PrefetchScalarGridSpec(
            num_scalar_prefetch=1,
            grid=(blocks,),
            in_specs=in_specs,
            out_specs=(
                pl.BlockSpec((row_count, query_width), lambda b, places: (0, b)),
                pl.BlockSpec((2, row_count, HD), lambda b, places: (0, 0, b)),
            ),
            scratch_shapes=[pltpu.VMEM((row_count, width), jnp.float32)],
        ),
        out_shape=(
            jax.ShapeDtypeStruct((row_count, blocks * query_width), jnp.bfloat16),
            jax.ShapeDtypeStruct((2, row_count, blocks * HD), jnp.bfloat16),
        ),
        compiler_params=pltpu.CompilerParams(vmem_limit_bytes=52 * 2**20),
        cost_estimate=pl.CostEstimate(
            flops=4_000_000_000, bytes_accessed=9_000_000, transcendentals=2_000_000
        ),
        name="attend",
    )(
        places,
        length,
        *[rows for rows, *_ in parts],
        *[weights] * len(parts),
        *carried,
        cosine,
        sine,
    )


def rope_tables(row_count):
    half = HD // 2
    freq = rope_theta ** (-2.0 * jnp.arange(half, dtype=jnp.float32) / HD)
    angle = jnp.arange(row_count, dtype=jnp.int32).astype(jnp.float32)[:, None] * freq[None, :]
    cosine, sine = jnp.cos(angle), jnp.sin(angle)
    return jnp.concatenate([cosine, cosine], axis=1), jnp.concatenate([-sine, sine], axis=1)


def residual_kernel(places_ref, *refs, shares):
    rows_ref, ordered_ref = refs[-2:]
    plane, ring, columns, quarter = ordered_ref.shape
    at = 0
    for turn, share in enumerate(shares):
        count = plane // share
        for piece in range(share):
            ordered_ref[piece * count : (piece + 1) * count, places_ref[turn]] = refs[at][
                ...
            ].reshape(count, columns, quarter)
            at += 1
    width = ring * columns
    for p in range(plane):
        rows_ref[:, p * width : (p + 1) * width] = jnp.transpose(
            ordered_ref[p].reshape(width, quarter).astype(jnp.float32)
        ).astype(jnp.bfloat16)


def residual(places, pieces, columns, quarter):
    flat = [rows for turn in pieces for rows in turn]
    depth = sum(rows.shape[0] for rows in flat)
    ring = len(pieces)
    return pl.pallas_call(
        functools.partial(residual_kernel, shares=[len(turn) for turn in pieces]),
        grid_spec=pltpu.PrefetchScalarGridSpec(
            num_scalar_prefetch=1,
            grid=(1,),
            in_specs=[
                pl.BlockSpec((rows.shape[0], quarter), lambda i, places: (0, places[0]))
                for rows in flat
            ],
            out_specs=pl.BlockSpec((quarter, depth), lambda i, places: (0, 0)),
            scratch_shapes=[
                pltpu.VMEM((depth // (ring * columns), ring, columns, quarter), jnp.bfloat16)
            ],
        ),
        out_shape=jax.ShapeDtypeStruct((quarter, depth), jnp.bfloat16),
        compiler_params=pltpu.CompilerParams(vmem_limit_bytes=16 * 2**20),
        cost_estimate=pl.CostEstimate(
            flops=1_000_000_000, bytes_accessed=4 * depth * quarter, transcendentals=0
        ),
        name="residual",
    )(places, *flat)


def ring_route(way):
    count = lax.axis_size(RING)
    return [(k, (k + way) % count) for k in range(count)]


def product_kernel(xh_ref, rows_ref, *refs, pieces, outs):
    held, arrived = refs[-2:]
    out_refs = refs[-2 - outs : -2]
    _, halves, depth, width = held.shape

    def incoming(k):
        array, index = pieces[k]
        return pltpu.make_async_copy(refs[array].at[index], held.at[k], arrived.at[k])

    for k in range(len(pieces)):
        incoming(k).start()
    each = len(pieces) // outs
    for k in range(len(pieces)):
        incoming(k).wait()
        total = None
        for half in range(halves):
            block = xh_ref[0] ^ half
            rows = rows_ref[:, pl.ds(pl.multiple_of(block * depth, depth), depth)]
            term = jnp.dot(rows, held[k, half], preferred_element_type=jnp.float32)
            total = term if total is None else total + term
        here = slice(k % each * width, (k % each + 1) * width)
        out_refs[k // each][:, here] = total.astype(jnp.bfloat16)


def product(xh, rows, weights, pieces, outs):
    _, halves, depth, width = weights[0].shape
    row_count = rows.shape[0]
    count = len(pieces)
    return pl.pallas_call(
        functools.partial(product_kernel, pieces=pieces, outs=outs),
        in_specs=[pl.BlockSpec(memory_space=pltpu.SMEM), pl.BlockSpec(memory_space=pltpu.VMEM)]
        + [pl.BlockSpec(memory_space=pltpu.HBM)] * len(weights),
        out_specs=tuple([pl.BlockSpec(memory_space=pltpu.VMEM)] * outs),
        out_shape=tuple(
            [jax.ShapeDtypeStruct((row_count, count // outs * width), jnp.bfloat16)] * outs
        ),
        scratch_shapes=[
            pltpu.VMEM((count, halves, depth, width), jnp.bfloat16),
            pltpu.SemaphoreType.DMA((count,)),
        ],
        compiler_params=pltpu.CompilerParams(vmem_limit_bytes=60 * 2**20),
        cost_estimate=pl.CostEstimate(
            flops=2 * row_count * halves * depth * width * count,
            bytes_accessed=2 * (rows.size + halves * depth * width * count),
            transcendentals=0,
        ),
        name="product",
    )(xh, rows, *weights)


LAYERS = (0, 1, 3, 2)


def finish_kernel(where_ref, rows_ref, *refs, width):
    hidden_ref = refs[-1]
    chunks = (len(refs) - 1) // 4
    each = refs[0].shape[1] // width
    for core in range(2):
        for chunk in range(chunks):
            at = 2 * (chunks * core + chunk)
            for j in range(each):
                layer, side = divmod(chunk * each + j, 2)
                z = lax.rem(where_ref[0] + len(LAYERS) - LAYERS[layer], len(LAYERS))
                column = (z * 2 + (where_ref[1] ^ side)) * 2 + (where_ref[2] ^ core)
                here = slice(j * width, (j + 1) * width)
                there = pl.ds(pl.multiple_of(column * width, width), width)
                total = refs[at][:, here].astype(jnp.float32) + refs[at + 1][:, here].astype(
                    jnp.float32
                )
                hidden_ref[:, there] = (
                    rows_ref[:, there].astype(jnp.float32) + total
                ).astype(jnp.bfloat16)


def finish(where, rows, sums, width):
    return pl.pallas_call(
        functools.partial(finish_kernel, width=width),
        out_shape=jax.ShapeDtypeStruct(rows.shape, jnp.bfloat16),
        in_specs=[pl.BlockSpec(memory_space=pltpu.SMEM)]
        + [pl.BlockSpec(memory_space=pltpu.VMEM)] * (1 + len(sums)),
        out_specs=pl.BlockSpec(memory_space=pltpu.VMEM),
        compiler_params=pltpu.CompilerParams(vmem_limit_bytes=16 * 2**20),
        cost_estimate=pl.CostEstimate(
            flops=4 * rows.size, bytes_accessed=8 * rows.size, transcendentals=0
        ),
        name="finish",
    )(where, rows, *sums)


CHUNKS = 2


def ring_sums(attended, weights, quarter):
    place = lax.axis_index(RING)
    count = lax.axis_size(RING)
    pieces = [(LAYERS.index(z), (side,)) for z in LAYERS[:3] for side in range(2)]
    pieces += [(3, (0,)), (4, (0,))]
    xh = lax.axis_index("tensor_0")[None]
    sums = []
    for side, way in enumerate((1, -1)):
        chunks = product(xh, attended, weights[side], pieces, CHUNKS)
        for partial_sums in chunks:

            def part(turn):
                start = (place + turn) % count * quarter
                return lax.dynamic_slice_in_dim(partial_sums, start, quarter, 0)

            running = part(-way)
            for step in range(1, count):
                running = lax.ppermute(running, RING, ring_route(way))
                mine = part(-way * (step + 1))
                if step + 1 < count:
                    running = running.astype(jnp.float32) + mine.astype(jnp.float32)
                    running = running.astype(jnp.bfloat16)
            sums += [running, mine]
    return sums


def sublayer(prompt_ids, prompt_lengths, embed_table, norm_gain, w_query, w_key, w_value, w_out):
    quarter = prompt_ids.shape[0]
    row_count = quarter * TPG
    devices = lax.axis_size(DP_TENSOR)
    columns = embed_table.shape[0]
    model_width = columns * devices
    group_count = devices // TPG
    place = lax.axis_index(RING)
    ring = lax.axis_size(RING)
    group_index = lax.axis_index(DP) * lax.axis_size("tensor_0") + lax.axis_index("tensor_0")
    length = lax.dynamic_slice_in_dim(prompt_lengths, group_index, 1, 0)
    cosine, sine = rope_tables(row_count)

    depth = w_query.shape[0]
    gain = lax.dynamic_slice_in_dim(norm_gain, lax.axis_index(DP) * depth, depth, 0)
    packed = jnp.concatenate([w_query, w_key, w_value], axis=1).astype(jnp.float32)
    packed = (packed * gain[:, None]).astype(jnp.bfloat16)
    w_in = lax.all_gather(collect_blocks(packed), DP, axis=1, tiled=True)
    w_in = w_in.reshape(w_in.shape[0], -1, ring, columns, w_in.shape[-1])
    all_ids = lax.all_to_all(
        jnp.broadcast_to(prompt_ids[None], (devices, quarter)),
        DP_TENSOR,
        split_axis=0,
        concat_axis=0,
        tiled=True,
    ).reshape(-1)
    pieces_x = [w_out]
    for axes, route in (
        ("tensor_0", [(0, 1), (1, 0)]),
        ("dp_1", [(0, 1), (1, 0)]),
        (("dp_1", "tensor_0"), [(0, 3), (1, 2), (2, 1), (3, 0)]),
    ):
        pieces_x.append(lax.ppermute(w_out, axes, route))
    outgoing = lookup(embed_table, all_ids, group_count)
    own = lax.all_to_all(outgoing, PLANE, split_axis=0, concat_axis=0, tiled=True).reshape(
        -1, row_count
    )
    pieces_x, _ = lax.optimization_barrier((pieces_x, outgoing))
    w_mine = [jnp.stack(pieces_x).reshape(2, 2, *w_out.shape)]
    layers = lax.axis_size("dp_0")
    ahead = [(z, (z + 1) % layers) for z in range(layers)]
    back = [(z, (z - 1) % layers) for z in range(layers)]
    for route in (ahead, back):
        w_mine.append(lax.ppermute(w_mine[0], "dp_0", route))
    first_side, last_side = w_mine[1][:1], w_mine[2][1:]
    w_mine.append(lax.ppermute(first_side, "dp_0", ahead))
    w_mine.append(lax.ppermute(last_side, "dp_0", back))
    w_other = []
    for k in range(len(w_mine)):
        w_other.append(lax.ppermute(w_mine[k], "dp_2", [(0, 1), (1, 0)]))

    places = (place + jnp.arange(ring, dtype=jnp.int32)) % ring
    half = own.shape[0] // 2
    low, high = own[:half], own[half:]
    low_before = lax.ppermute(low, RING, ring_route(1))
    high_after = lax.ppermute(high, RING, ring_route(-1))
    high_before = lax.ppermute(high, RING, ring_route(1))
    low_after = lax.ppermute(low, RING, ring_route(-1))
    low_across = lax.ppermute(low_before, RING, ring_route(1))
    high_across = lax.ppermute(high_after, RING, ring_route(-1))

    first = project(places, w_in, [(own, 0, 1, 0)])
    second = project(
        places,
        w_in,
        [
            (low_before, ring - 1, 2, 0),
            (high_before, ring - 1, 2, 1),
            (low_after, 1, 2, 0),
            (high_after, 1, 2, 1),
        ],
        first,
    )
    attended, cache = attend(
        places,
        w_in,
        [(low_across, 2, 2, 0), (high_across, 2, 2, 1)],
        second,
        length,
        cosine,
        sine,
        model_width,
    )

    pieces = [[own], [low_after, high_after], [low_across, high_across], [low_before, high_before]]
    pieces, _ = lax.optimization_barrier((pieces, attended))
    own_rows = residual(places, pieces, columns, quarter)

    sums = ring_sums(attended, (w_mine, w_other), quarter)
    where = jnp.stack([lax.axis_index(name) for name in DP])
    hidden = finish(where, own_rows, sums, w_out.shape[1])
    return hidden, cache[None]


def solution(mesh):
    split = Mesh(
        mesh.devices.reshape(4, 2, 2, 2, 4), ("dp_0", "dp_1", "dp_2", "tensor_0", "tensor_1")
    )
    placed = (
        P(DP_TENSOR),
        P(),
        P(DP_TENSOR, None),
        P(),
        P(DP, TENSOR),
        P(DP, TENSOR),
        P(DP, TENSOR),
        P(TENSOR, DP),
    )
    return jax.shard_map(
        sublayer,
        mesh=split,
        in_specs=placed,
        out_specs=(P(DP_TENSOR, None), P(DP_TENSOR, None, None, None)),
        check_vma=False,
    )
```

```python
import functools

import jax
import jax.numpy as jnp
from jax import lax
from jax.experimental import pallas as pl
from jax.experimental.pallas import tpu as pltpu
from jax.sharding import Mesh
from jax.sharding import PartitionSpec as P


HEADS = 32
KVH = 8
HD = 128
TPG = 4
TENSOR = ("tensor_0", "tensor_1")
DP_TENSOR = ("dp_0", "dp_1", "dp_2", "tensor_0", "tensor_1")
DP = ("dp_0", "dp_1", "dp_2")
RING = "tensor_1"
PLANE = ("dp_0", "dp_1", "dp_2", "tensor_0")
LANES = 128

norm_eps = 1e-05
rope_theta = 500000.0


def swapped(block, axis, apart):
    count = lax.axis_size(axis)
    route = []
    for low in range(count):
        high = low | 1 << apart
        if high != low and high < count:
            route += [(low, high), (high, low)]
    return lax.ppermute(block, axis, route)


def ordered_pair(mine, theirs, bit_index):
    upper_half = lax.axis_index(TENSOR) >> bit_index & 1 == 1
    first_half = jnp.where(upper_half, theirs, mine)
    second_half = jnp.where(upper_half, mine, theirs)
    return jnp.concatenate([first_half, second_half], axis=0)


def collect_blocks(shard):
    stacked = shard[None]
    theirs = swapped(stacked, TENSOR, 2)
    return ordered_pair(stacked, theirs, 2)


def lane_gather(block, lanes):
    dims = lax.GatherDimensionNumbers(
        offset_dims=(),
        collapsed_slice_dims=(1,),
        start_index_map=(1,),
        operand_batching_dims=(0,),
        start_indices_batching_dims=(0,),
    )
    return lax.gather(
        block,
        lanes[..., None],
        dims,
        slice_sizes=(1, 1),
        mode=lax.GatherScatterMode.PROMISE_IN_BOUNDS,
    )


def lookup_kernel(slots_ref, lanes_ref, table_ref, out_ref, table, tiles, arrived):
    groups, columns, row_count = out_ref.shape
    tile_count = tiles.shape[0] // 2
    slabs = arrived.shape[0]
    slab = tile_count // slabs
    lane = lax.broadcasted_iota(jnp.int32, (columns, LANES), 1).astype(jnp.int16)
    left = lane < jnp.int16(LANES // 2)
    unroll = min(56, slab)

    def incoming(k):
        part = pl.ds(k * slab * LANES, slab * LANES)
        return pltpu.make_async_copy(table_ref.at[:, part], table.at[:, part], arrived.at[k])

    for k in range(slabs):
        incoming(k).start()

    for k in range(slabs):
        incoming(k).wait()

        def prepare(step, carry, k=k):
            first = k * slab + jnp.minimum(step * unroll, slab - unroll)
            for u in range(unroll):
                t = first + u
                tile = table[:, pl.ds(pl.multiple_of(t * LANES, LANES), LANES)]
                tiles[t] = tile
                tiles[t + tile_count] = lane_gather(tile, lane ^ jnp.int16(LANES // 2))
            return carry

        lax.fori_loop(0, -(-slab // unroll), prepare, 0)

    per_group = row_count // LANES
    together = 2

    def one_block(step, carry):
        for part in range(together):
            block = step * together + part
            first = block * LANES
            wanted = jnp.broadcast_to(lanes_ref[pl.ds(block, 1), :], (columns, LANES)).astype(
                jnp.int16
            )
            picked = jnp.zeros((columns, LANES), jnp.bfloat16)
            for i in range(0, LANES, 2):
                pair = jnp.where(
                    left, tiles[slots_ref[first + i]], tiles[slots_ref[first + i + 1]]
                )
                picked = jnp.where(lane >= jnp.int16(i), lane_gather(pair, wanted), picked)
            place = pl.multiple_of(lax.rem(block, per_group) * LANES, LANES)
            out_ref[lax.div(block, per_group), :, pl.ds(place, LANES)] = picked
        return carry

    lax.fori_loop(0, groups * per_group // together, one_block, 0)


def lookup(embed_table, token_ids, group_count):
    columns, vocab_size = embed_table.shape
    tile_count = vocab_size // LANES
    slabs = next(k for k in (6, 4, 3, 2, 1) if tile_count % k == 0)
    count = token_ids.shape[0]
    half = LANES // 2
    odd = jnp.arange(count, dtype=jnp.int32) & 1
    lane = token_ids & (LANES - 1)
    swapped_half = lax.shift_right_logical(lane, 6) ^ odd
    slots = lax.shift_right_logical(token_ids, 7) + tile_count * swapped_half
    lanes = ((lane & (half - 1)) | (odd * half)).reshape(count // LANES, LANES)
    return pl.pallas_call(
        lookup_kernel,
        out_shape=jax.ShapeDtypeStruct((group_count, columns, count // group_count), jnp.bfloat16),
        in_specs=[
            pl.BlockSpec(memory_space=pltpu.SMEM),
            pl.BlockSpec(memory_space=pltpu.VMEM),
            pl.BlockSpec(memory_space=pltpu.HBM),
        ],
        out_specs=pl.BlockSpec(memory_space=pltpu.VMEM),
        scratch_shapes=[
            pltpu.VMEM((columns, vocab_size), jnp.bfloat16),
            pltpu.VMEM((2 * tile_count, columns, LANES), jnp.bfloat16),
            pltpu.SemaphoreType.DMA((slabs,)),
        ],
        compiler_params=pltpu.CompilerParams(vmem_limit_bytes=60 * 2**20),
        cost_estimate=pl.CostEstimate(
            flops=30_000_000_000, bytes_accessed=embed_table.size * 2, transcendentals=0
        ),
        name="lookup",
    )(slots, lanes, embed_table)


def transposed_product(rows_ref, weight_ref):
    weight = weight_ref[...]
    width = weight.shape[-1]
    return lax.dot_general(
        rows_ref[...],
        weight.reshape(-1, width),
        (((0,), (0,)), ((), ())),
        preferred_element_type=jnp.float32,
    )


def square_sum(rows_ref):
    wide = rows_ref[...].astype(jnp.float32)
    return jnp.sum(wide * wide, axis=0, keepdims=True)


def project_kernel(places_ref, *refs, parts, carried):
    rows, weights = refs[:parts], refs[parts : 2 * parts]
    total_ref, squares_ref = refs[-2:]
    total = sum(transposed_product(r, w) for r, w in zip(rows, weights))
    squares = sum(square_sum(r) for r in rows)
    if carried:
        total += refs[2 * parts][...]
        squares += refs[2 * parts + 1][...]
    total_ref[...] = total
    squares_ref[...] = squares


def weight_spec(weights, turn, share, which):
    _, plane, _, columns, width = weights.shape
    return pl.BlockSpec(
        (1, plane // share, 1, columns, width),
        lambda b, places: (b, which, places[turn], 0, 0),
    )


def project(places, weights, parts, carried=None):
    row_count = parts[0][0].shape[1]
    blocks, width = weights.shape[0], weights.shape[-1]
    in_specs = [pl.BlockSpec(rows.shape, lambda b, places: (0, 0)) for rows, *_ in parts]
    in_specs += [weight_spec(weights, *where) for _, *where in parts]
    total_spec = pl.BlockSpec((row_count, width), lambda b, places: (0, b))
    squares_spec = pl.BlockSpec((1, row_count), lambda b, places: (0, 0))
    operands = [rows for rows, *_ in parts] + [weights] * len(parts)
    if carried is not None:
        in_specs += [total_spec, squares_spec]
        operands += list(carried)
    depth = sum(rows.shape[0] for rows, *_ in parts)
    return pl.pallas_call(
        functools.partial(project_kernel, parts=len(parts), carried=carried is not None),
        grid_spec=pltpu.PrefetchScalarGridSpec(
            num_scalar_prefetch=1,
            grid=(blocks,),
            in_specs=in_specs,
            out_specs=(total_spec, squares_spec),
        ),
        out_shape=(
            jax.ShapeDtypeStruct((row_count, blocks * width), jnp.float32),
            jax.ShapeDtypeStruct((1, row_count), jnp.float32),
        ),
        compiler_params=pltpu.CompilerParams(vmem_limit_bytes=52 * 2**20),
        cost_estimate=pl.CostEstimate(
            flops=2 * row_count * depth * blocks * width,
            bytes_accessed=2 * depth * (blocks * width + row_count),
            transcendentals=0,
        ),
        name="project",
    )(places, *operands)


def attention_kernel(
    places_ref, length_ref, *refs, parts, model_width
):
    rows, weights = refs[:parts], refs[parts : 2 * parts]
    total_ref, squares_ref, cos_ref, sin_ref, attended_ref, cache_ref, proj_ref = refs[2 * parts :]
    row_count = cos_ref.shape[0]
    q_heads = HEADS // KVH
    proj_ref[...] = total_ref[...] + sum(transposed_product(r, w) for r, w in zip(rows, weights))
    squares = squares_ref[...] + sum(square_sum(r) for r in rows)
    scale = lax.rsqrt(squares / model_width + norm_eps)
    scale = jnp.transpose(jnp.broadcast_to(scale, (HD, row_count)))
    cosine = cos_ref[...] * scale
    sine = sin_ref[...] * scale

    def rotate(part):
        return (part * cosine + pltpu.roll(part, HD // 2, 1) * sine).astype(jnp.bfloat16)

    key_rot = rotate(proj_ref[:, q_heads * HD : (q_heads + 1) * HD])
    value = (proj_ref[:, (q_heads + 1) * HD : (q_heads + 2) * HD] * scale).astype(jnp.bfloat16)
    cache_ref[0] = key_rot
    cache_ref[1] = value
    length = length_ref[0]
    block = min(256, row_count)
    power = 1.4426950408889634 / HD**0.5
    for h in range(q_heads):
        query = rotate(proj_ref[:, h * HD : (h + 1) * HD])
        for start in range(0, row_count, block):
            keys = start + block
            scores = lax.dot_general(
                key_rot[:keys],
                query[start : start + block],
                (((1,), (1,)), ((), ())),
                preferred_element_type=jnp.float32,
            )
            q_pos = start + lax.broadcasted_iota(jnp.int32, (1, block), 1)
            k_pos = lax.broadcasted_iota(jnp.int32, (keys, block), 0)
            scores = jnp.where(k_pos < jnp.minimum(q_pos + 1, length), scores, -1e30)
            biggest = jnp.max(scores, axis=0, keepdims=True)
            expd = jnp.exp2((scores - biggest) * power)
            weights_now = expd * (1.0 / jnp.sum(expd, axis=0, keepdims=True))
            attended_ref[start : start + block, h * HD : (h + 1) * HD] = lax.dot_general(
                weights_now.astype(jnp.bfloat16),
                value[:keys],
                (((0,), (0,)), ((), ())),
                preferred_element_type=jnp.float32,
            ).astype(jnp.bfloat16)


def attend(places, weights, parts, carried, length, cosine, sine, model_width):
    row_count = cosine.shape[0]
    blocks, width = weights.shape[0], weights.shape[-1]
    query_width = HEADS // KVH * HD
    in_specs = [pl.BlockSpec(memory_space=pltpu.SMEM)]
    in_specs += [pl.BlockSpec(rows.shape, lambda b, places: (0, 0)) for rows, *_ in parts]
    in_specs += [weight_spec(weights, *where) for _, *where in parts]
    in_specs += [
        pl.BlockSpec((row_count, width), lambda b, places: (0, b)),
        pl.BlockSpec((1, row_count), lambda b, places: (0, 0)),
        pl.BlockSpec((row_count, HD), lambda b, places: (0, 0)),
        pl.BlockSpec((row_count, HD), lambda b, places: (0, 0)),
    ]
    return pl.pallas_call(
        functools.partial(attention_kernel, parts=len(parts), model_width=model_width),
        grid_spec=pltpu.PrefetchScalarGridSpec(
            num_scalar_prefetch=1,
            grid=(blocks,),
            in_specs=in_specs,
            out_specs=(
                pl.BlockSpec((row_count, query_width), lambda b, places: (0, b)),
                pl.BlockSpec((2, row_count, HD), lambda b, places: (0, 0, b)),
            ),
            scratch_shapes=[pltpu.VMEM((row_count, width), jnp.float32)],
        ),
        out_shape=(
            jax.ShapeDtypeStruct((row_count, blocks * query_width), jnp.bfloat16),
            jax.ShapeDtypeStruct((2, row_count, blocks * HD), jnp.bfloat16),
        ),
        compiler_params=pltpu.CompilerParams(vmem_limit_bytes=52 * 2**20),
        cost_estimate=pl.CostEstimate(
            flops=4_000_000_000, bytes_accessed=9_000_000, transcendentals=2_000_000
        ),
        name="attend",
    )(
        places,
        length,
        *[rows for rows, *_ in parts],
        *[weights] * len(parts),
        *carried,
        cosine,
        sine,
    )


def rope_tables(row_count):
    half = HD // 2
    freq = rope_theta ** (-2.0 * jnp.arange(half, dtype=jnp.float32) / HD)
    angle = jnp.arange(row_count, dtype=jnp.int32).astype(jnp.float32)[:, None] * freq[None, :]
    cosine, sine = jnp.cos(angle), jnp.sin(angle)
    return jnp.concatenate([cosine, cosine], axis=1), jnp.concatenate([-sine, sine], axis=1)


def residual_kernel(places_ref, *refs, shares):
    rows_ref, ordered_ref = refs[-2:]
    plane, ring, columns, quarter = ordered_ref.shape
    at = 0
    for turn, share in enumerate(shares):
        count = plane // share
        for piece in range(share):
            ordered_ref[piece * count : (piece + 1) * count, places_ref[turn]] = refs[at][
                ...
            ].reshape(count, columns, quarter)
            at += 1
    width = ring * columns
    for p in range(plane):
        rows_ref[:, p * width : (p + 1) * width] = jnp.transpose(
            ordered_ref[p].reshape(width, quarter).astype(jnp.float32)
        ).astype(jnp.bfloat16)


def residual(places, pieces, columns, quarter):
    flat = [rows for turn in pieces for rows in turn]
    depth = sum(rows.shape[0] for rows in flat)
    ring = len(pieces)
    return pl.pallas_call(
        functools.partial(residual_kernel, shares=[len(turn) for turn in pieces]),
        grid_spec=pltpu.PrefetchScalarGridSpec(
            num_scalar_prefetch=1,
            grid=(1,),
            in_specs=[
                pl.BlockSpec((rows.shape[0], quarter), lambda i, places: (0, places[0]))
                for rows in flat
            ],
            out_specs=pl.BlockSpec((quarter, depth), lambda i, places: (0, 0)),
            scratch_shapes=[
                pltpu.VMEM((depth // (ring * columns), ring, columns, quarter), jnp.bfloat16)
            ],
        ),
        out_shape=jax.ShapeDtypeStruct((quarter, depth), jnp.bfloat16),
        compiler_params=pltpu.CompilerParams(vmem_limit_bytes=16 * 2**20),
        cost_estimate=pl.CostEstimate(
            flops=1_000_000_000, bytes_accessed=4 * depth * quarter, transcendentals=0
        ),
        name="residual",
    )(places, *flat)


def ring_route(way):
    count = lax.axis_size(RING)
    return [(k, (k + way) % count) for k in range(count)]


def product_kernel(where_ref, rows_ref, *refs, pieces, turns, chunks):
    turned, held, arrived = refs[-3:]
    out_refs = refs[-3 - len(turns) * chunks : -3]
    quarter = out_refs[0].shape[0]
    ring = rows_ref.shape[0] // quarter
    _, halves, depth, width = refs[0].shape

    def incoming(k, half):
        array, index = pieces[k]
        block = where_ref[1] ^ half
        return pltpu.make_async_copy(
            refs[array].at[index, half],
            held.at[pl.ds(pl.multiple_of(block * depth, depth), depth), pl.ds(k * width, width)],
            arrived.at[k, half],
        )

    copies = [(k, half) for k in range(len(pieces)) for half in range(halves)]
    for copy in copies:
        incoming(*copy).start()
    for at, turn in enumerate(turns):
        block = lax.rem(where_ref[0] + ring + turn, ring)
        turned[at * quarter : (at + 1) * quarter] = rows_ref[
            pl.ds(pl.multiple_of(block * quarter, quarter), quarter)
        ]
    each = len(pieces) // chunks
    for chunk in range(chunks):
        for copy in copies[chunk * each * halves : (chunk + 1) * each * halves]:
            incoming(*copy).wait()
        total = jnp.dot(
            turned[...],
            held[:, chunk * each * width : (chunk + 1) * each * width],
            preferred_element_type=jnp.float32,
        ).astype(jnp.bfloat16)
        for at in range(len(turns)):
            out_refs[chunk * len(turns) + at][...] = total[at * quarter : (at + 1) * quarter]


def product(where, rows, weights, pieces, turns, chunks):
    _, halves, depth, width = weights[0].shape
    row_count = rows.shape[0]
    count = len(pieces)
    return pl.pallas_call(
        functools.partial(product_kernel, pieces=pieces, turns=turns, chunks=chunks),
        in_specs=[pl.BlockSpec(memory_space=pltpu.SMEM), pl.BlockSpec(memory_space=pltpu.VMEM)]
        + [pl.BlockSpec(memory_space=pltpu.HBM)] * len(weights),
        out_specs=tuple([pl.BlockSpec(memory_space=pltpu.VMEM)] * (len(turns) * chunks)),
        out_shape=tuple(
            [jax.ShapeDtypeStruct((row_count // len(turns), count // chunks * width), jnp.bfloat16)]
            * (len(turns) * chunks)
        ),
        scratch_shapes=[
            pltpu.VMEM(rows.shape, jnp.bfloat16),
            pltpu.VMEM((halves * depth, count * width), jnp.bfloat16),
            pltpu.SemaphoreType.DMA((count, halves)),
        ],
        compiler_params=pltpu.CompilerParams(vmem_limit_bytes=60 * 2**20),
        cost_estimate=pl.CostEstimate(
            flops=2 * row_count * halves * depth * width * count,
            bytes_accessed=2 * (rows.size + halves * depth * width * count),
            transcendentals=0,
        ),
        name="product",
    )(where, rows, *weights)


LAYERS = (0, 1, 3, 2)


def finish_kernel(where_ref, rows_ref, *refs, width):
    hidden_ref = refs[-1]
    chunks = (len(refs) - 1) // 4
    each = refs[0].shape[1] // width
    for core in range(2):
        for chunk in range(chunks):
            at = 2 * (chunks * core + chunk)
            for j in range(each):
                layer, side = divmod(chunk * each + j, 2)
                z = lax.rem(where_ref[0] + len(LAYERS) - LAYERS[layer], len(LAYERS))
                column = (z * 2 + (where_ref[1] ^ side)) * 2 + (where_ref[2] ^ core)
                here = slice(j * width, (j + 1) * width)
                there = pl.ds(pl.multiple_of(column * width, width), width)
                total = refs[at][:, here].astype(jnp.float32) + refs[at + 1][:, here].astype(
                    jnp.float32
                )
                hidden_ref[:, there] = (
                    rows_ref[:, there].astype(jnp.float32) + total
                ).astype(jnp.bfloat16)


def finish(where, rows, sums, width):
    return pl.pallas_call(
        functools.partial(finish_kernel, width=width),
        out_shape=jax.ShapeDtypeStruct(rows.shape, jnp.bfloat16),
        in_specs=[pl.BlockSpec(memory_space=pltpu.SMEM)]
        + [pl.BlockSpec(memory_space=pltpu.VMEM)] * (1 + len(sums)),
        out_specs=pl.BlockSpec(memory_space=pltpu.VMEM),
        compiler_params=pltpu.CompilerParams(vmem_limit_bytes=16 * 2**20),
        cost_estimate=pl.CostEstimate(
            flops=4 * rows.size, bytes_accessed=8 * rows.size, transcendentals=0
        ),
        name="finish",
    )(where, rows, *sums)


CHUNKS = 2


def ring_sums(attended, weights):
    count = lax.axis_size(RING)
    pieces = [(LAYERS.index(z), side) for z in LAYERS[:3] for side in range(2)]
    pieces += [(3, 0), (4, 0)]
    where = jnp.stack([lax.axis_index(RING), lax.axis_index("tensor_0")])
    sums = []
    for side, way in enumerate((1, -1)):
        turns = [-way * (step + 1) for step in range(count)]
        parts = product(where, attended, weights[side], pieces, turns, CHUNKS)
        for chunk in range(CHUNKS):
            running, *mine = parts[chunk * count : (chunk + 1) * count]
            for step in range(1, count):
                running = lax.ppermute(running, RING, ring_route(way))
                if step + 1 < count:
                    running = running.astype(jnp.float32) + mine[step - 1].astype(jnp.float32)
                    running = running.astype(jnp.bfloat16)
            sums += [running, mine[-1]]
    return sums


def sublayer(prompt_ids, prompt_lengths, embed_table, norm_gain, w_query, w_key, w_value, w_out):
    quarter = prompt_ids.shape[0]
    row_count = quarter * TPG
    devices = lax.axis_size(DP_TENSOR)
    columns = embed_table.shape[0]
    model_width = columns * devices
    group_count = devices // TPG
    place = lax.axis_index(RING)
    ring = lax.axis_size(RING)
    group_index = lax.axis_index(DP) * lax.axis_size("tensor_0") + lax.axis_index("tensor_0")
    length = lax.dynamic_slice_in_dim(prompt_lengths, group_index, 1, 0)
    cosine, sine = rope_tables(row_count)

    depth = w_query.shape[0]
    gain = lax.dynamic_slice_in_dim(norm_gain, lax.axis_index(DP) * depth, depth, 0)
    packed = jnp.concatenate([w_query, w_key, w_value], axis=1).astype(jnp.float32)
    packed = (packed * gain[:, None]).astype(jnp.bfloat16)
    w_in = lax.all_gather(collect_blocks(packed), DP, axis=1, tiled=True)
    w_in = w_in.reshape(w_in.shape[0], -1, ring, columns, w_in.shape[-1])
    all_ids = lax.all_to_all(
        jnp.broadcast_to(prompt_ids[None], (devices, quarter)),
        DP_TENSOR,
        split_axis=0,
        concat_axis=0,
        tiled=True,
    ).reshape(-1)
    pieces_x = [w_out]
    for axes, route in (
        ("tensor_0", [(0, 1), (1, 0)]),
        ("dp_1", [(0, 1), (1, 0)]),
        (("dp_1", "tensor_0"), [(0, 3), (1, 2), (2, 1), (3, 0)]),
    ):
        pieces_x.append(lax.ppermute(w_out, axes, route))
    outgoing = lookup(embed_table, all_ids, group_count)
    own = lax.all_to_all(outgoing, PLANE, split_axis=0, concat_axis=0, tiled=True).reshape(
        -1, row_count
    )
    pieces_x, _ = lax.optimization_barrier((pieces_x, outgoing))
    w_mine = [jnp.stack(pieces_x).reshape(2, 2, *w_out.shape)]
    layers = lax.axis_size("dp_0")
    ahead = [(z, (z + 1) % layers) for z in range(layers)]
    back = [(z, (z - 1) % layers) for z in range(layers)]
    for route in (ahead, back):
        w_mine.append(lax.ppermute(w_mine[0], "dp_0", route))
    places = (place + jnp.arange(ring, dtype=jnp.int32)) % ring
    half = own.shape[0] // 2
    low, high = own[:half], own[half:]
    low_before = lax.ppermute(low, RING, ring_route(1))
    high_after = lax.ppermute(high, RING, ring_route(-1))
    high_before = lax.ppermute(high, RING, ring_route(1))
    low_after = lax.ppermute(low, RING, ring_route(-1))
    low_across = lax.ppermute(low_before, RING, ring_route(1))
    high_across = lax.ppermute(high_after, RING, ring_route(-1))

    first = project(places, w_in, [(own, 0, 1, 0)])
    second = project(
        places,
        w_in,
        [
            (low_before, ring - 1, 2, 0),
            (high_before, ring - 1, 2, 1),
            (low_after, 1, 2, 0),
            (high_after, 1, 2, 1),
        ],
        first,
    )
    z_sides, _ = lax.optimization_barrier((w_mine[1:], second))
    first_side, last_side = z_sides[0][:1], z_sides[1][1:]
    w_mine.append(lax.ppermute(first_side, "dp_0", ahead))
    w_mine.append(lax.ppermute(last_side, "dp_0", back))
    w_other = []
    for k in range(len(w_mine)):
        w_other.append(lax.ppermute(w_mine[k], "dp_2", [(0, 1), (1, 0)]))
    attended, cache = attend(
        places,
        w_in,
        [(low_across, 2, 2, 0), (high_across, 2, 2, 1)],
        second,
        length,
        cosine,
        sine,
        model_width,
    )

    pieces = [[own], [low_after, high_after], [low_across, high_across], [low_before, high_before]]
    pieces, _ = lax.optimization_barrier((pieces, attended))
    own_rows = residual(places, pieces, columns, quarter)

    sums = ring_sums(attended, (w_mine, w_other))
    where = jnp.stack([lax.axis_index(name) for name in DP])
    hidden = finish(where, own_rows, sums, w_out.shape[1])
    return hidden, cache[None]


def solution(mesh):
    split = Mesh(
        mesh.devices.reshape(4, 2, 2, 2, 4), ("dp_0", "dp_1", "dp_2", "tensor_0", "tensor_1")
    )
    placed = (
        P(DP_TENSOR),
        P(),
        P(DP_TENSOR, None),
        P(),
        P(DP, TENSOR),
        P(DP, TENSOR),
        P(DP, TENSOR),
        P(TENSOR, DP),
    )
    return jax.shard_map(
        sublayer,
        mesh=split,
        in_specs=placed,
        out_specs=(P(DP_TENSOR, None), P(DP_TENSOR, None, None, None)),
        check_vma=False,
    )
```

```python
import functools

import jax
import jax.numpy as jnp
from jax import lax
from jax.experimental import pallas as pl
from jax.experimental.pallas import tpu as pltpu
from jax.sharding import Mesh
from jax.sharding import PartitionSpec as P


HEADS = 32
KVH = 8
HD = 128
TPG = 4
TENSOR = ("tensor_0", "tensor_1")
DP_TENSOR = ("dp_0", "dp_1", "dp_2", "tensor_0", "tensor_1")
DP = ("dp_0", "dp_1", "dp_2")
RING = "tensor_1"
PLANE = ("dp_0", "dp_1", "dp_2", "tensor_0")
LANES = 128

norm_eps = 1e-05
rope_theta = 500000.0


def swapped(block, axis, apart):
    count = lax.axis_size(axis)
    route = []
    for low in range(count):
        high = low | 1 << apart
        if high != low and high < count:
            route += [(low, high), (high, low)]
    return lax.ppermute(block, axis, route)


def ordered_pair(mine, theirs, bit_index):
    upper_half = lax.axis_index(TENSOR) >> bit_index & 1 == 1
    first_half = jnp.where(upper_half, theirs, mine)
    second_half = jnp.where(upper_half, mine, theirs)
    return jnp.concatenate([first_half, second_half], axis=0)


def collect_blocks(shard):
    stacked = shard[None]
    theirs = swapped(stacked, TENSOR, 2)
    return ordered_pair(stacked, theirs, 2)


def lane_gather(block, lanes):
    dims = lax.GatherDimensionNumbers(
        offset_dims=(),
        collapsed_slice_dims=(1,),
        start_index_map=(1,),
        operand_batching_dims=(0,),
        start_indices_batching_dims=(0,),
    )
    return lax.gather(
        block,
        lanes[..., None],
        dims,
        slice_sizes=(1, 1),
        mode=lax.GatherScatterMode.PROMISE_IN_BOUNDS,
    )


def lookup_kernel(slots_ref, lanes_ref, table_ref, out_ref, table, tiles, arrived, *, cores):
    groups, columns, row_count = out_ref.shape
    tile_count = tiles.shape[0] // 2
    slabs = arrived.shape[0]
    slab = tile_count // slabs
    lane = lax.broadcasted_iota(jnp.int32, (columns, LANES), 1).astype(jnp.int16)
    left = lane < jnp.int16(LANES // 2)
    unroll = min(56, slab)

    def incoming(k):
        part = pl.ds(k * slab * LANES, slab * LANES)
        return pltpu.make_async_copy(table_ref.at[:, part], table.at[:, part], arrived.at[k])

    for k in range(slabs):
        incoming(k).start()

    for k in range(slabs):
        incoming(k).wait()

        def prepare(step, carry, k=k):
            first = k * slab + jnp.minimum(step * unroll, slab - unroll)
            for u in range(unroll):
                t = first + u
                tile = table[:, pl.ds(pl.multiple_of(t * LANES, LANES), LANES)]
                tiles[t] = tile
                tiles[t + tile_count] = lane_gather(tile, lane ^ jnp.int16(LANES // 2))
            return carry

        lax.fori_loop(0, -(-slab // unroll), prepare, 0)

    per_group = row_count // LANES
    tensor_size = lax.axis_size(TENSOR)
    together = 2

    def one_block(step, carry):
        for part in range(together):
            block = step * together + part
            first = block * LANES
            wanted = jnp.broadcast_to(lanes_ref[pl.ds(block, 1), :], (columns, LANES)).astype(
                jnp.int16
            )
            picked = jnp.zeros((columns, LANES), jnp.bfloat16)
            for i in range(0, LANES, 2):
                pair = jnp.where(
                    left, tiles[slots_ref[first + i]], tiles[slots_ref[first + i + 1]]
                )
                picked = jnp.where(lane >= jnp.int16(i), lane_gather(pair, wanted), picked)
            span = cores * tensor_size
            within = lax.rem(block, span)
            device = block - within + lax.rem(within, cores) * tensor_size + lax.div(within, cores)
            place = pl.multiple_of(lax.rem(device, per_group) * LANES, LANES)
            out_ref[lax.div(device, per_group), :, pl.ds(place, LANES)] = picked
        return carry

    lax.fori_loop(0, groups * per_group // together, one_block, 0)


def lookup(embed_table, token_ids, group_count):
    columns, vocab_size = embed_table.shape
    tile_count = vocab_size // LANES
    slabs = next(k for k in (6, 4, 3, 2, 1) if tile_count % k == 0)
    count = token_ids.shape[0]
    half = LANES // 2
    odd = jnp.arange(count, dtype=jnp.int32) & 1
    lane = token_ids & (LANES - 1)
    swapped_half = lax.shift_right_logical(lane, 6) ^ odd
    slots = lax.shift_right_logical(token_ids, 7) + tile_count * swapped_half
    lanes = ((lane & (half - 1)) | (odd * half)).reshape(count // LANES, LANES)
    return pl.pallas_call(
        functools.partial(lookup_kernel, cores=lax.axis_size("dp_2")),
        out_shape=jax.ShapeDtypeStruct((group_count, columns, count // group_count), jnp.bfloat16),
        in_specs=[
            pl.BlockSpec(memory_space=pltpu.SMEM),
            pl.BlockSpec(memory_space=pltpu.VMEM),
            pl.BlockSpec(memory_space=pltpu.HBM),
        ],
        out_specs=pl.BlockSpec(memory_space=pltpu.VMEM),
        scratch_shapes=[
            pltpu.VMEM((columns, vocab_size), jnp.bfloat16),
            pltpu.VMEM((2 * tile_count, columns, LANES), jnp.bfloat16),
            pltpu.SemaphoreType.DMA((slabs,)),
        ],
        compiler_params=pltpu.CompilerParams(vmem_limit_bytes=60 * 2**20),
        cost_estimate=pl.CostEstimate(
            flops=30_000_000_000, bytes_accessed=embed_table.size * 2, transcendentals=0
        ),
        name="lookup",
    )(slots, lanes, embed_table)


def transposed_product(rows_ref, weight_ref):
    weight = weight_ref[...]
    width = weight.shape[-1]
    return lax.dot_general(
        rows_ref[...],
        weight.reshape(-1, width),
        (((0,), (0,)), ((), ())),
        preferred_element_type=jnp.float32,
    )


def square_sum(rows_ref):
    wide = rows_ref[...].astype(jnp.float32)
    return jnp.sum(wide * wide, axis=0, keepdims=True)


def project_kernel(places_ref, *refs, parts, carried):
    rows, weights = refs[:parts], refs[parts : 2 * parts]
    total_ref, squares_ref = refs[-2:]
    total = sum(transposed_product(r, w) for r, w in zip(rows, weights))
    squares = sum(square_sum(r) for r in rows)
    if carried:
        total += refs[2 * parts][...]
        squares += refs[2 * parts + 1][...]
    total_ref[...] = total
    squares_ref[...] = squares


def weight_spec(weights, turn, share, which):
    _, plane, _, columns, width = weights.shape
    return pl.BlockSpec(
        (1, plane // share, 1, columns, width),
        lambda b, places: (b, which, places[turn], 0, 0),
    )


def project(places, weights, parts, carried=None):
    row_count = parts[0][0].shape[1]
    blocks, width = weights.shape[0], weights.shape[-1]
    in_specs = [pl.BlockSpec(rows.shape, lambda b, places: (0, 0)) for rows, *_ in parts]
    in_specs += [weight_spec(weights, *where) for _, *where in parts]
    total_spec = pl.BlockSpec((row_count, width), lambda b, places: (0, b))
    squares_spec = pl.BlockSpec((1, row_count), lambda b, places: (0, 0))
    operands = [rows for rows, *_ in parts] + [weights] * len(parts)
    if carried is not None:
        in_specs += [total_spec, squares_spec]
        operands += list(carried)
    depth = sum(rows.shape[0] for rows, *_ in parts)
    return pl.pallas_call(
        functools.partial(project_kernel, parts=len(parts), carried=carried is not None),
        grid_spec=pltpu.PrefetchScalarGridSpec(
            num_scalar_prefetch=1,
            grid=(blocks,),
            in_specs=in_specs,
            out_specs=(total_spec, squares_spec),
        ),
        out_shape=(
            jax.ShapeDtypeStruct((row_count, blocks * width), jnp.float32),
            jax.ShapeDtypeStruct((1, row_count), jnp.float32),
        ),
        compiler_params=pltpu.CompilerParams(vmem_limit_bytes=52 * 2**20),
        cost_estimate=pl.CostEstimate(
            flops=2 * row_count * depth * blocks * width,
            bytes_accessed=2 * depth * (blocks * width + row_count),
            transcendentals=0,
        ),
        name="project",
    )(places, *operands)


def attention_kernel(
    places_ref, length_ref, *refs, parts, model_width
):
    rows, weights = refs[:parts], refs[parts : 2 * parts]
    total_ref, squares_ref, cos_ref, sin_ref, attended_ref, cache_ref, proj_ref = refs[2 * parts :]
    row_count = cos_ref.shape[0]
    q_heads = HEADS // KVH
    proj_ref[...] = total_ref[...] + sum(transposed_product(r, w) for r, w in zip(rows, weights))
    squares = squares_ref[...] + sum(square_sum(r) for r in rows)
    scale = lax.rsqrt(squares / model_width + norm_eps)
    scale = jnp.transpose(jnp.broadcast_to(scale, (HD, row_count)))
    cosine = cos_ref[...] * scale
    sine = sin_ref[...] * scale

    def rotate(part):
        return (part * cosine + pltpu.roll(part, HD // 2, 1) * sine).astype(jnp.bfloat16)

    key_rot = rotate(proj_ref[:, q_heads * HD : (q_heads + 1) * HD])
    value = (proj_ref[:, (q_heads + 1) * HD : (q_heads + 2) * HD] * scale).astype(jnp.bfloat16)
    cache_ref[0] = key_rot
    cache_ref[1] = value
    length = length_ref[0]
    block = min(256, row_count)
    power = 1.4426950408889634 / HD**0.5
    for h in range(q_heads):
        query = rotate(proj_ref[:, h * HD : (h + 1) * HD])
        for start in range(0, row_count, block):
            keys = start + block
            scores = lax.dot_general(
                key_rot[:keys],
                query[start : start + block],
                (((1,), (1,)), ((), ())),
                preferred_element_type=jnp.float32,
            )
            q_pos = start + lax.broadcasted_iota(jnp.int32, (1, block), 1)
            k_pos = lax.broadcasted_iota(jnp.int32, (keys, block), 0)
            scores = jnp.where(k_pos < jnp.minimum(q_pos + 1, length), scores, -1e30)
            biggest = jnp.max(scores, axis=0, keepdims=True)
            expd = jnp.exp2((scores - biggest) * power)
            weights_now = expd * (1.0 / jnp.sum(expd, axis=0, keepdims=True))
            attended_ref[start : start + block, h * HD : (h + 1) * HD] = lax.dot_general(
                weights_now.astype(jnp.bfloat16),
                value[:keys],
                (((0,), (0,)), ((), ())),
                preferred_element_type=jnp.float32,
            ).astype(jnp.bfloat16)


def attend(places, weights, parts, carried, length, cosine, sine, model_width):
    row_count = cosine.shape[0]
    blocks, width = weights.shape[0], weights.shape[-1]
    query_width = HEADS // KVH * HD
    in_specs = [pl.BlockSpec(memory_space=pltpu.SMEM)]
    in_specs += [pl.BlockSpec(rows.shape, lambda b, places: (0, 0)) for rows, *_ in parts]
    in_specs += [weight_spec(weights, *where) for _, *where in parts]
    in_specs += [
        pl.BlockSpec((row_count, width), lambda b, places: (0, b)),
        pl.BlockSpec((1, row_count), lambda b, places: (0, 0)),
        pl.BlockSpec((row_count, HD), lambda b, places: (0, 0)),
        pl.BlockSpec((row_count, HD), lambda b, places: (0, 0)),
    ]
    return pl.pallas_call(
        functools.partial(attention_kernel, parts=len(parts), model_width=model_width),
        grid_spec=pltpu.PrefetchScalarGridSpec(
            num_scalar_prefetch=1,
            grid=(blocks,),
            in_specs=in_specs,
            out_specs=(
                pl.BlockSpec((row_count, query_width), lambda b, places: (0, b)),
                pl.BlockSpec((2, row_count, HD), lambda b, places: (0, 0, b)),
            ),
            scratch_shapes=[pltpu.VMEM((row_count, width), jnp.float32)],
        ),
        out_shape=(
            jax.ShapeDtypeStruct((row_count, blocks * query_width), jnp.bfloat16),
            jax.ShapeDtypeStruct((2, row_count, blocks * HD), jnp.bfloat16),
        ),
        compiler_params=pltpu.CompilerParams(vmem_limit_bytes=52 * 2**20),
        cost_estimate=pl.CostEstimate(
            flops=4_000_000_000, bytes_accessed=9_000_000, transcendentals=2_000_000
        ),
        name="attend",
    )(
        places,
        length,
        *[rows for rows, *_ in parts],
        *[weights] * len(parts),
        *carried,
        cosine,
        sine,
    )


def rope_tables(row_count):
    half = HD // 2
    freq = rope_theta ** (-2.0 * jnp.arange(half, dtype=jnp.float32) / HD)
    angle = jnp.arange(row_count, dtype=jnp.int32).astype(jnp.float32)[:, None] * freq[None, :]
    cosine, sine = jnp.cos(angle), jnp.sin(angle)
    return jnp.concatenate([cosine, cosine], axis=1), jnp.concatenate([-sine, sine], axis=1)


def residual_kernel(places_ref, *refs, shares):
    rows_ref, ordered_ref = refs[-2:]
    plane, ring, columns, quarter = ordered_ref.shape
    at = 0
    for turn, share in enumerate(shares):
        count = plane // share
        for piece in range(share):
            ordered_ref[piece * count : (piece + 1) * count, places_ref[turn]] = refs[at][
                ...
            ].reshape(count, columns, quarter)
            at += 1
    width = ring * columns
    for p in range(plane):
        rows_ref[:, p * width : (p + 1) * width] = jnp.transpose(
            ordered_ref[p].reshape(width, quarter).astype(jnp.float32)
        ).astype(jnp.bfloat16)


def residual(places, pieces, columns, quarter):
    flat = [rows for turn in pieces for rows in turn]
    depth = sum(rows.shape[0] for rows in flat)
    ring = len(pieces)
    return pl.pallas_call(
        functools.partial(residual_kernel, shares=[len(turn) for turn in pieces]),
        grid_spec=pltpu.PrefetchScalarGridSpec(
            num_scalar_prefetch=1,
            grid=(1,),
            in_specs=[
                pl.BlockSpec((rows.shape[0], quarter), lambda i, places: (0, places[0]))
                for rows in flat
            ],
            out_specs=pl.BlockSpec((quarter, depth), lambda i, places: (0, 0)),
            scratch_shapes=[
                pltpu.VMEM((depth // (ring * columns), ring, columns, quarter), jnp.bfloat16)
            ],
        ),
        out_shape=jax.ShapeDtypeStruct((quarter, depth), jnp.bfloat16),
        compiler_params=pltpu.CompilerParams(vmem_limit_bytes=16 * 2**20),
        cost_estimate=pl.CostEstimate(
            flops=1_000_000_000, bytes_accessed=4 * depth * quarter, transcendentals=0
        ),
        name="residual",
    )(places, *flat)


def ring_route(way):
    count = lax.axis_size(RING)
    return [(k, (k + way) % count) for k in range(count)]


def product_kernel(where_ref, rows_ref, *refs, pieces, turns, chunks):
    turned, held, arrived = refs[-3:]
    out_refs = refs[-3 - len(turns) * chunks : -3]
    quarter = out_refs[0].shape[0]
    ring = rows_ref.shape[0] // quarter
    _, halves, depth, width = refs[0].shape

    def incoming(k, half):
        array, index = pieces[k]
        block = where_ref[1] ^ half
        return pltpu.make_async_copy(
            refs[array].at[index, half],
            held.at[pl.ds(pl.multiple_of(block * depth, depth), depth), pl.ds(k * width, width)],
            arrived.at[k, half],
        )

    copies = [(k, half) for k in range(len(pieces)) for half in range(halves)]
    for copy in copies:
        incoming(*copy).start()
    for at, turn in enumerate(turns):
        block = lax.rem(where_ref[0] + ring + turn, ring)
        turned[at * quarter : (at + 1) * quarter] = rows_ref[
            pl.ds(pl.multiple_of(block * quarter, quarter), quarter)
        ]
    each = len(pieces) // chunks
    for chunk in range(chunks):
        for copy in copies[chunk * each * halves : (chunk + 1) * each * halves]:
            incoming(*copy).wait()
        total = jnp.dot(
            turned[...],
            held[:, chunk * each * width : (chunk + 1) * each * width],
            preferred_element_type=jnp.float32,
        ).astype(jnp.bfloat16)
        for at in range(len(turns)):
            out_refs[chunk * len(turns) + at][...] = total[at * quarter : (at + 1) * quarter]


def product(where, rows, weights, pieces, turns, chunks):
    _, halves, depth, width = weights[0].shape
    row_count = rows.shape[0]
    count = len(pieces)
    return pl.pallas_call(
        functools.partial(product_kernel, pieces=pieces, turns=turns, chunks=chunks),
        in_specs=[pl.BlockSpec(memory_space=pltpu.SMEM), pl.BlockSpec(memory_space=pltpu.VMEM)]
        + [pl.BlockSpec(memory_space=pltpu.HBM)] * len(weights),
        out_specs=tuple([pl.BlockSpec(memory_space=pltpu.VMEM)] * (len(turns) * chunks)),
        out_shape=tuple(
            [jax.ShapeDtypeStruct((row_count // len(turns), count // chunks * width), jnp.bfloat16)]
            * (len(turns) * chunks)
        ),
        scratch_shapes=[
            pltpu.VMEM(rows.shape, jnp.bfloat16),
            pltpu.VMEM((halves * depth, count * width), jnp.bfloat16),
            pltpu.SemaphoreType.DMA((count, halves)),
        ],
        compiler_params=pltpu.CompilerParams(vmem_limit_bytes=60 * 2**20),
        cost_estimate=pl.CostEstimate(
            flops=2 * row_count * halves * depth * width * count,
            bytes_accessed=2 * (rows.size + halves * depth * width * count),
            transcendentals=0,
        ),
        name="product",
    )(where, rows, *weights)


LAYERS = (0, 1, 3, 2)


def finish_kernel(where_ref, rows_ref, *refs, width):
    hidden_ref = refs[-1]
    chunks = (len(refs) - 1) // 4
    each = refs[0].shape[1] // width
    for core in range(2):
        for chunk in range(chunks):
            at = 2 * (chunks * core + chunk)
            for j in range(each):
                layer, side = divmod(chunk * each + j, 2)
                z = lax.rem(where_ref[0] + len(LAYERS) - LAYERS[layer], len(LAYERS))
                column = (z * 2 + (where_ref[1] ^ side)) * 2 + (where_ref[2] ^ core)
                here = slice(j * width, (j + 1) * width)
                there = pl.ds(pl.multiple_of(column * width, width), width)
                total = refs[at][:, here].astype(jnp.float32) + refs[at + 1][:, here].astype(
                    jnp.float32
                )
                hidden_ref[:, there] = (
                    rows_ref[:, there].astype(jnp.float32) + total
                ).astype(jnp.bfloat16)


def finish(where, rows, sums, width):
    return pl.pallas_call(
        functools.partial(finish_kernel, width=width),
        out_shape=jax.ShapeDtypeStruct(rows.shape, jnp.bfloat16),
        in_specs=[pl.BlockSpec(memory_space=pltpu.SMEM)]
        + [pl.BlockSpec(memory_space=pltpu.VMEM)] * (1 + len(sums)),
        out_specs=pl.BlockSpec(memory_space=pltpu.VMEM),
        compiler_params=pltpu.CompilerParams(vmem_limit_bytes=16 * 2**20),
        cost_estimate=pl.CostEstimate(
            flops=4 * rows.size, bytes_accessed=8 * rows.size, transcendentals=0
        ),
        name="finish",
    )(where, rows, *sums)


CHUNKS = 2


def ring_sums(attended, weights):
    count = lax.axis_size(RING)
    pieces = [(k, side) for k in range(len(LAYERS)) for side in range(2)]
    where = jnp.stack([lax.axis_index(RING), lax.axis_index("tensor_0")])
    sums = []
    for side, way in enumerate((1, -1)):
        turns = [-way * (step + 1) for step in range(count)]
        parts = product(where, attended, weights[side], pieces, turns, CHUNKS)
        for chunk in range(CHUNKS):
            running, *mine = parts[chunk * count : (chunk + 1) * count]
            for step in range(1, count):
                running = lax.ppermute(running, RING, ring_route(way))
                if step + 1 < count:
                    running = running.astype(jnp.float32) + mine[step - 1].astype(jnp.float32)
                    running = running.astype(jnp.bfloat16)
            sums += [running, mine[-1]]
    return sums


def sublayer(prompt_ids, prompt_lengths, embed_table, norm_gain, w_query, w_key, w_value, w_out):
    quarter = prompt_ids.shape[0]
    row_count = quarter * TPG
    devices = lax.axis_size(DP_TENSOR)
    columns = embed_table.shape[0]
    model_width = columns * devices
    group_count = devices // TPG
    place = lax.axis_index(RING)
    ring = lax.axis_size(RING)
    group_index = lax.axis_index(DP) * lax.axis_size("tensor_0") + lax.axis_index("tensor_0")
    length = lax.dynamic_slice_in_dim(prompt_lengths, group_index, 1, 0)
    cosine, sine = rope_tables(row_count)

    depth = w_query.shape[0]
    gain = lax.dynamic_slice_in_dim(norm_gain, lax.axis_index(DP) * depth, depth, 0)
    packed = jnp.concatenate([w_query, w_key, w_value], axis=1).astype(jnp.float32)
    packed = (packed * gain[:, None]).astype(jnp.bfloat16)
    w_in = lax.all_gather(collect_blocks(packed), DP, axis=1, tiled=True)
    w_in = w_in.reshape(w_in.shape[0], -1, ring, columns, w_in.shape[-1])
    cores = lax.axis_size("dp_2")
    chip_ids = lax.all_gather(prompt_ids, "dp_2")
    others = ("dp_0", "dp_1", "tensor_0", "tensor_1")
    all_ids = lax.all_to_all(
        jnp.broadcast_to(chip_ids[None], (devices // cores, cores, quarter)),
        others,
        split_axis=0,
        concat_axis=0,
        tiled=True,
    )
    all_ids = all_ids.reshape(-1)
    pieces_x = [w_out]
    for axes, route in (
        ("tensor_0", [(0, 1), (1, 0)]),
        ("dp_1", [(0, 1), (1, 0)]),
        (("dp_1", "tensor_0"), [(0, 3), (1, 2), (2, 1), (3, 0)]),
    ):
        pieces_x.append(lax.ppermute(w_out, axes, route))
    outgoing = lookup(embed_table, all_ids, group_count)
    own = lax.all_to_all(outgoing, PLANE, split_axis=0, concat_axis=0, tiled=True).reshape(
        -1, row_count
    )
    pieces_x, _ = lax.optimization_barrier((pieces_x, outgoing))
    w_mine = [jnp.stack(pieces_x).reshape(2, 2, *w_out.shape)]
    layers = lax.axis_size("dp_0")
    for k in LAYERS[1:]:
        route = [(z, (z + k) % layers) for z in range(layers)]
        w_mine.append(lax.ppermute(w_mine[0], "dp_0", route))
    w_other = []
    for k in range(layers):
        w_other.append(lax.ppermute(w_mine[k], "dp_2", [(0, 1), (1, 0)]))

    places = (place + jnp.arange(ring, dtype=jnp.int32)) % ring
    half = own.shape[0] // 2
    low, high = own[:half], own[half:]
    low_before = lax.ppermute(low, RING, ring_route(1))
    high_after = lax.ppermute(high, RING, ring_route(-1))
    high_before = lax.ppermute(high, RING, ring_route(1))
    low_after = lax.ppermute(low, RING, ring_route(-1))
    low_across = lax.ppermute(low_before, RING, ring_route(1))
    high_across = lax.ppermute(high_after, RING, ring_route(-1))

    first = project(places, w_in, [(own, 0, 1, 0)])
    second = project(
        places,
        w_in,
        [
            (low_before, ring - 1, 2, 0),
            (high_before, ring - 1, 2, 1),
            (low_after, 1, 2, 0),
            (high_after, 1, 2, 1),
        ],
        first,
    )
    attended, cache = attend(
        places,
        w_in,
        [(low_across, 2, 2, 0), (high_across, 2, 2, 1)],
        second,
        length,
        cosine,
        sine,
        model_width,
    )

    pieces = [[own], [low_after, high_after], [low_across, high_across], [low_before, high_before]]
    pieces, _ = lax.optimization_barrier((pieces, attended))
    own_rows = residual(places, pieces, columns, quarter)

    sums = ring_sums(attended, (w_mine, w_other))
    where = jnp.stack([lax.axis_index(name) for name in DP])
    hidden = finish(where, own_rows, sums, w_out.shape[1])
    return hidden, cache[None]


def solution(mesh):
    split = Mesh(
        mesh.devices.reshape(4, 2, 2, 2, 4), ("dp_0", "dp_1", "dp_2", "tensor_0", "tensor_1")
    )
    placed = (
        P(DP_TENSOR),
        P(),
        P(DP_TENSOR, None),
        P(),
        P(DP, TENSOR),
        P(DP, TENSOR),
        P(DP, TENSOR),
        P(TENSOR, DP),
    )
    return jax.shard_map(
        sublayer,
        mesh=split,
        in_specs=placed,
        out_specs=(P(DP_TENSOR, None), P(DP_TENSOR, None, None, None)),
        check_vma=False,
    )
```

```python
import functools

import jax
import jax.numpy as jnp
from jax import lax
from jax.experimental import pallas as pl
from jax.experimental.pallas import tpu as pltpu
from jax.sharding import Mesh
from jax.sharding import PartitionSpec as P


HEADS = 32
KVH = 8
HD = 128
TPG = 4
TENSOR = ("tensor_0", "tensor_1")
DP_TENSOR = ("dp_0", "dp_1", "dp_2", "tensor_0", "tensor_1")
DP = ("dp_0", "dp_1", "dp_2")
RING = "tensor_1"
PLANE = ("dp_0", "dp_1", "dp_2", "tensor_0")
LANES = 128

norm_eps = 1e-05
rope_theta = 500000.0


def swapped(block, axis, apart):
    count = lax.axis_size(axis)
    route = []
    for low in range(count):
        high = low | 1 << apart
        if high != low and high < count:
            route += [(low, high), (high, low)]
    return lax.ppermute(block, axis, route)


def ordered_pair(mine, theirs, bit_index):
    upper_half = lax.axis_index(TENSOR) >> bit_index & 1 == 1
    first_half = jnp.where(upper_half, theirs, mine)
    second_half = jnp.where(upper_half, mine, theirs)
    return jnp.concatenate([first_half, second_half], axis=0)


def collect_blocks(shard):
    stacked = shard[None]
    theirs = swapped(stacked, TENSOR, 2)
    return ordered_pair(stacked, theirs, 2)


def lane_gather(block, lanes):
    dims = lax.GatherDimensionNumbers(
        offset_dims=(),
        collapsed_slice_dims=(1,),
        start_index_map=(1,),
        operand_batching_dims=(0,),
        start_indices_batching_dims=(0,),
    )
    return lax.gather(
        block,
        lanes[..., None],
        dims,
        slice_sizes=(1, 1),
        mode=lax.GatherScatterMode.PROMISE_IN_BOUNDS,
    )


def lookup_kernel(slots_ref, lanes_ref, table_ref, out_ref, table, tiles, arrived):
    groups, columns, row_count = out_ref.shape
    tile_count = tiles.shape[0] // 2
    slabs = arrived.shape[0]
    slab = tile_count // slabs
    lane = lax.broadcasted_iota(jnp.int32, (columns, LANES), 1).astype(jnp.int16)
    left = lane < jnp.int16(LANES // 2)
    unroll = min(56, slab)

    def incoming(k):
        part = pl.ds(k * slab * LANES, slab * LANES)
        return pltpu.make_async_copy(table_ref.at[:, part], table.at[:, part], arrived.at[k])

    for k in range(slabs):
        incoming(k).start()

    for k in range(slabs):
        incoming(k).wait()

        def prepare(step, carry, k=k):
            first = k * slab + jnp.minimum(step * unroll, slab - unroll)
            for u in range(unroll):
                t = first + u
                tile = table[:, pl.ds(pl.multiple_of(t * LANES, LANES), LANES)]
                tiles[t] = tile
                tiles[t + tile_count] = lane_gather(tile, lane ^ jnp.int16(LANES // 2))
            return carry

        lax.fori_loop(0, -(-slab // unroll), prepare, 0)

    per_group = row_count // LANES
    together = 4

    def one_block(step, carry):
        for part in range(together):
            block = step * together + part
            first = block * LANES
            wanted = jnp.broadcast_to(lanes_ref[pl.ds(block, 1), :], (columns, LANES)).astype(
                jnp.int16
            )
            picked = jnp.zeros((columns, LANES), jnp.bfloat16)
            for i in range(0, LANES, 2):
                pair = jnp.where(
                    left, tiles[slots_ref[first + i]], tiles[slots_ref[first + i + 1]]
                )
                picked = jnp.where(lane >= jnp.int16(i), lane_gather(pair, wanted), picked)
            place = pl.multiple_of(lax.rem(block, per_group) * LANES, LANES)
            out_ref[lax.div(block, per_group), :, pl.ds(place, LANES)] = picked
        return carry

    lax.fori_loop(0, groups * per_group // together, one_block, 0)


def lookup(embed_table, token_ids, group_count):
    columns, vocab_size = embed_table.shape
    tile_count = vocab_size // LANES
    slabs = next(k for k in (6, 4, 3, 2, 1) if tile_count % k == 0)
    count = token_ids.shape[0]
    half = LANES // 2
    odd = jnp.arange(count, dtype=jnp.int32) & 1
    lane = token_ids & (LANES - 1)
    swapped_half = lax.shift_right_logical(lane, 6) ^ odd
    slots = lax.shift_right_logical(token_ids, 7) + tile_count * swapped_half
    lanes = ((lane & (half - 1)) | (odd * half)).reshape(count // LANES, LANES)
    return pl.pallas_call(
        lookup_kernel,
        out_shape=jax.ShapeDtypeStruct((group_count, columns, count // group_count), jnp.bfloat16),
        in_specs=[
            pl.BlockSpec(memory_space=pltpu.SMEM),
            pl.BlockSpec(memory_space=pltpu.VMEM),
            pl.BlockSpec(memory_space=pltpu.HBM),
        ],
        out_specs=pl.BlockSpec(memory_space=pltpu.VMEM),
        scratch_shapes=[
            pltpu.VMEM((columns, vocab_size), jnp.bfloat16),
            pltpu.VMEM((2 * tile_count, columns, LANES), jnp.bfloat16),
            pltpu.SemaphoreType.DMA((slabs,)),
        ],
        compiler_params=pltpu.CompilerParams(vmem_limit_bytes=60 * 2**20),
        cost_estimate=pl.CostEstimate(
            flops=30_000_000_000, bytes_accessed=embed_table.size * 2, transcendentals=0
        ),
        name="lookup",
    )(slots, lanes, embed_table)


def transposed_product(rows_ref, weight_ref):
    weight = weight_ref[...]
    width = weight.shape[-1]
    return lax.dot_general(
        rows_ref[...],
        weight.reshape(-1, width),
        (((0,), (0,)), ((), ())),
        preferred_element_type=jnp.float32,
    )


def square_sum(rows_ref):
    wide = rows_ref[...].astype(jnp.float32)
    return jnp.sum(wide * wide, axis=0, keepdims=True)


def project_kernel(places_ref, *refs, parts, carried):
    rows, weights = refs[:parts], refs[parts : 2 * parts]
    total_ref, squares_ref = refs[-2:]
    total = sum(transposed_product(r, w) for r, w in zip(rows, weights))
    squares = sum(square_sum(r) for r in rows)
    if carried:
        total += refs[2 * parts][...]
        squares += refs[2 * parts + 1][...]
    total_ref[...] = total
    squares_ref[...] = squares


def weight_spec(weights, turn, share, which):
    _, plane, _, columns, width = weights.shape
    return pl.BlockSpec(
        (1, plane // share, 1, columns, width),
        lambda b, places: (b, which, places[turn], 0, 0),
    )


def project(places, weights, parts, carried=None):
    row_count = parts[0][0].shape[1]
    blocks, width = weights.shape[0], weights.shape[-1]
    in_specs = [pl.BlockSpec(rows.shape, lambda b, places: (0, 0)) for rows, *_ in parts]
    in_specs += [weight_spec(weights, *where) for _, *where in parts]
    total_spec = pl.BlockSpec((row_count, width), lambda b, places: (0, b))
    squares_spec = pl.BlockSpec((1, row_count), lambda b, places: (0, 0))
    operands = [rows for rows, *_ in parts] + [weights] * len(parts)
    if carried is not None:
        in_specs += [total_spec, squares_spec]
        operands += list(carried)
    depth = sum(rows.shape[0] for rows, *_ in parts)
    return pl.pallas_call(
        functools.partial(project_kernel, parts=len(parts), carried=carried is not None),
        grid_spec=pltpu.PrefetchScalarGridSpec(
            num_scalar_prefetch=1,
            grid=(blocks,),
            in_specs=in_specs,
            out_specs=(total_spec, squares_spec),
        ),
        out_shape=(
            jax.ShapeDtypeStruct((row_count, blocks * width), jnp.float32),
            jax.ShapeDtypeStruct((1, row_count), jnp.float32),
        ),
        compiler_params=pltpu.CompilerParams(vmem_limit_bytes=52 * 2**20),
        cost_estimate=pl.CostEstimate(
            flops=2 * row_count * depth * blocks * width,
            bytes_accessed=2 * depth * (blocks * width + row_count),
            transcendentals=0,
        ),
        name="project",
    )(places, *operands)


def attention_kernel(
    places_ref, length_ref, *refs, parts, model_width
):
    rows, weights = refs[:parts], refs[parts : 2 * parts]
    total_ref, squares_ref, cos_ref, sin_ref, attended_ref, cache_ref, proj_ref = refs[2 * parts :]
    row_count = cos_ref.shape[0]
    q_heads = HEADS // KVH
    proj_ref[...] = total_ref[...] + sum(transposed_product(r, w) for r, w in zip(rows, weights))
    squares = squares_ref[...] + sum(square_sum(r) for r in rows)
    scale = lax.rsqrt(squares / model_width + norm_eps)
    scale = jnp.transpose(jnp.broadcast_to(scale, (HD, row_count)))
    cosine = cos_ref[...] * scale
    sine = sin_ref[...] * scale

    def rotate(part):
        return (part * cosine + pltpu.roll(part, HD // 2, 1) * sine).astype(jnp.bfloat16)

    key_rot = rotate(proj_ref[:, q_heads * HD : (q_heads + 1) * HD])
    value = (proj_ref[:, (q_heads + 1) * HD : (q_heads + 2) * HD] * scale).astype(jnp.bfloat16)
    cache_ref[0] = key_rot
    cache_ref[1] = value
    length = length_ref[0]
    block = min(256, row_count)
    power = 1.4426950408889634 / HD**0.5
    for h in range(q_heads):
        query = rotate(proj_ref[:, h * HD : (h + 1) * HD])
        for start in range(0, row_count, block):
            keys = start + block
            scores = lax.dot_general(
                key_rot[:keys],
                query[start : start + block],
                (((1,), (1,)), ((), ())),
                preferred_element_type=jnp.float32,
            )
            q_pos = start + lax.broadcasted_iota(jnp.int32, (1, block), 1)
            k_pos = lax.broadcasted_iota(jnp.int32, (keys, block), 0)
            scores = jnp.where(k_pos < jnp.minimum(q_pos + 1, length), scores, -1e30)
            biggest = jnp.max(scores, axis=0, keepdims=True)
            expd = jnp.exp2((scores - biggest) * power)
            weights_now = expd * (1.0 / jnp.sum(expd, axis=0, keepdims=True))
            attended_ref[start : start + block, h * HD : (h + 1) * HD] = lax.dot_general(
                weights_now.astype(jnp.bfloat16),
                value[:keys],
                (((0,), (0,)), ((), ())),
                preferred_element_type=jnp.float32,
            ).astype(jnp.bfloat16)


def attend(places, weights, parts, carried, length, cosine, sine, model_width):
    row_count = cosine.shape[0]
    blocks, width = weights.shape[0], weights.shape[-1]
    query_width = HEADS // KVH * HD
    in_specs = [pl.BlockSpec(memory_space=pltpu.SMEM)]
    in_specs += [pl.BlockSpec(rows.shape, lambda b, places: (0, 0)) for rows, *_ in parts]
    in_specs += [weight_spec(weights, *where) for _, *where in parts]
    in_specs += [
        pl.BlockSpec((row_count, width), lambda b, places: (0, b)),
        pl.BlockSpec((1, row_count), lambda b, places: (0, 0)),
        pl.BlockSpec((row_count, HD), lambda b, places: (0, 0)),
        pl.BlockSpec((row_count, HD), lambda b, places: (0, 0)),
    ]
    return pl.pallas_call(
        functools.partial(attention_kernel, parts=len(parts), model_width=model_width),
        grid_spec=pltpu.PrefetchScalarGridSpec(
            num_scalar_prefetch=1,
            grid=(blocks,),
            in_specs=in_specs,
            out_specs=(
                pl.BlockSpec((row_count, query_width), lambda b, places: (0, b)),
                pl.BlockSpec((2, row_count, HD), lambda b, places: (0, 0, b)),
            ),
            scratch_shapes=[pltpu.VMEM((row_count, width), jnp.float32)],
        ),
        out_shape=(
            jax.ShapeDtypeStruct((row_count, blocks * query_width), jnp.bfloat16),
            jax.ShapeDtypeStruct((2, row_count, blocks * HD), jnp.bfloat16),
        ),
        compiler_params=pltpu.CompilerParams(vmem_limit_bytes=52 * 2**20),
        cost_estimate=pl.CostEstimate(
            flops=4_000_000_000, bytes_accessed=9_000_000, transcendentals=2_000_000
        ),
        name="attend",
    )(
        places,
        length,
        *[rows for rows, *_ in parts],
        *[weights] * len(parts),
        *carried,
        cosine,
        sine,
    )


def rope_tables(row_count):
    half = HD // 2
    freq = rope_theta ** (-2.0 * jnp.arange(half, dtype=jnp.float32) / HD)
    angle = jnp.arange(row_count, dtype=jnp.int32).astype(jnp.float32)[:, None] * freq[None, :]
    cosine, sine = jnp.cos(angle), jnp.sin(angle)
    return jnp.concatenate([cosine, cosine], axis=1), jnp.concatenate([-sine, sine], axis=1)


def residual_kernel(places_ref, *refs, shares):
    rows_ref, ordered_ref = refs[-2:]
    plane, ring, columns, quarter = ordered_ref.shape
    at = 0
    for turn, share in enumerate(shares):
        count = plane // share
        for piece in range(share):
            ordered_ref[piece * count : (piece + 1) * count, places_ref[turn]] = refs[at][
                ...
            ].reshape(count, columns, quarter)
            at += 1
    width = ring * columns
    for p in range(plane):
        rows_ref[:, p * width : (p + 1) * width] = jnp.transpose(
            ordered_ref[p].reshape(width, quarter).astype(jnp.float32)
        ).astype(jnp.bfloat16)


def residual(places, pieces, columns, quarter):
    flat = [rows for turn in pieces for rows in turn]
    depth = sum(rows.shape[0] for rows in flat)
    ring = len(pieces)
    return pl.pallas_call(
        functools.partial(residual_kernel, shares=[len(turn) for turn in pieces]),
        grid_spec=pltpu.PrefetchScalarGridSpec(
            num_scalar_prefetch=1,
            grid=(1,),
            in_specs=[
                pl.BlockSpec((rows.shape[0], quarter), lambda i, places: (0, places[0]))
                for rows in flat
            ],
            out_specs=pl.BlockSpec((quarter, depth), lambda i, places: (0, 0)),
            scratch_shapes=[
                pltpu.VMEM((depth // (ring * columns), ring, columns, quarter), jnp.bfloat16)
            ],
        ),
        out_shape=jax.ShapeDtypeStruct((quarter, depth), jnp.bfloat16),
        compiler_params=pltpu.CompilerParams(vmem_limit_bytes=16 * 2**20),
        cost_estimate=pl.CostEstimate(
            flops=1_000_000_000, bytes_accessed=4 * depth * quarter, transcendentals=0
        ),
        name="residual",
    )(places, *flat)


def ring_route(way):
    count = lax.axis_size(RING)
    return [(k, (k + way) % count) for k in range(count)]


def product_kernel(where_ref, rows_ref, *refs, turns, chunks):
    turned, held, arrived = refs[-3:]
    out_refs = refs[-3 - len(turns) : -3]
    weights = refs[: -3 - len(turns)]
    quarter = out_refs[0].shape[0]
    ring = rows_ref.shape[0] // quarter
    halves, depth, width = weights[0].shape

    def incoming(k, half):
        block = where_ref[1] ^ half
        return pltpu.make_async_copy(
            weights[k].at[half],
            held.at[pl.ds(pl.multiple_of(block * depth, depth), depth), pl.ds(k * width, width)],
            arrived.at[k, half],
        )

    copies = [(k, half) for k in range(len(weights)) for half in range(halves)]
    for copy in copies:
        incoming(*copy).start()
    for at, turn in enumerate(turns):
        block = lax.rem(where_ref[0] + ring + turn, ring)
        turned[at * quarter : (at + 1) * quarter] = rows_ref[
            pl.ds(pl.multiple_of(block * quarter, quarter), quarter)
        ]
    each = len(weights) // chunks
    for chunk in range(chunks):
        for copy in copies[chunk * each * halves : (chunk + 1) * each * halves]:
            incoming(*copy).wait()
        here = slice(chunk * each * width, (chunk + 1) * each * width)
        total = jnp.dot(
            turned[...], held[:, here], preferred_element_type=jnp.float32
        ).astype(jnp.bfloat16)
        for at in range(len(turns)):
            out_refs[at][:, here] = total[at * quarter : (at + 1) * quarter]


def product(where, rows, weights, turns, chunks=2):
    halves, depth, width = weights[0].shape
    row_count = rows.shape[0]
    count = len(weights)
    return pl.pallas_call(
        functools.partial(product_kernel, turns=turns, chunks=chunks),
        in_specs=[pl.BlockSpec(memory_space=pltpu.SMEM), pl.BlockSpec(memory_space=pltpu.VMEM)]
        + [pl.BlockSpec(memory_space=pltpu.HBM)] * count,
        out_specs=tuple([pl.BlockSpec(memory_space=pltpu.VMEM)] * len(turns)),
        out_shape=tuple(
            [jax.ShapeDtypeStruct((row_count // len(turns), count * width), jnp.bfloat16)]
            * len(turns)
        ),
        scratch_shapes=[
            pltpu.VMEM(rows.shape, jnp.bfloat16),
            pltpu.VMEM((halves * depth, count * width), jnp.bfloat16),
            pltpu.SemaphoreType.DMA((count, halves)),
        ],
        compiler_params=pltpu.CompilerParams(vmem_limit_bytes=60 * 2**20),
        cost_estimate=pl.CostEstimate(
            flops=2 * row_count * halves * depth * width * count,
            bytes_accessed=2 * (rows.size + halves * depth * width * count),
            transcendentals=0,
        ),
        name="product",
    )(where, rows, *weights)


LAYERS = (0, 1, 3, 2)


def finish_kernel(where_ref, rows_ref, *refs, width):
    hidden_ref = refs[-1]
    for core in range(2):
        terms = refs[3 * core : 3 * core + 3]
        for j in range(2 * len(LAYERS)):
            z = lax.rem(where_ref[0] + len(LAYERS) - LAYERS[j // 2], len(LAYERS))
            column = (z * 2 + (where_ref[1] ^ (j % 2))) * 2 + (where_ref[2] ^ core)
            here = slice(j * width, (j + 1) * width)
            there = pl.ds(pl.multiple_of(column * width, width), width)
            total = sum(term[:, here].astype(jnp.float32) for term in terms)
            hidden_ref[:, there] = (rows_ref[:, there].astype(jnp.float32) + total).astype(
                jnp.bfloat16
            )


def finish(where, rows, sums, width):
    return pl.pallas_call(
        functools.partial(finish_kernel, width=width),
        out_shape=jax.ShapeDtypeStruct(rows.shape, jnp.bfloat16),
        in_specs=[pl.BlockSpec(memory_space=pltpu.SMEM)]
        + [pl.BlockSpec(memory_space=pltpu.VMEM)] * (1 + len(sums)),
        out_specs=pl.BlockSpec(memory_space=pltpu.VMEM),
        compiler_params=pltpu.CompilerParams(vmem_limit_bytes=16 * 2**20),
        cost_estimate=pl.CostEstimate(
            flops=4 * rows.size, bytes_accessed=8 * rows.size, transcendentals=0
        ),
        name="finish",
    )(where, rows, *sums)


def ring_sums(attended, w_mine, w_other):
    where = jnp.stack([lax.axis_index(RING), lax.axis_index("tensor_0")])
    order = [(z, side) for z in LAYERS for side in range(2)]
    own, first, onward = [], [], []
    for way, weights in ((1, w_mine), (-1, w_other)):
        across, against, along, mine = product(
            where, attended, [weights[name] for name in order], [2, -way, way, 0]
        )
        passed = lax.ppermute(across, RING, ring_route(way))
        first.append(lax.ppermute(against, RING, ring_route(-way)))
        own.append(mine)
        onward.append((way, along, passed))
    last = []
    for way, along, passed in onward:
        both = (along.astype(jnp.float32) + passed.astype(jnp.float32)).astype(jnp.bfloat16)
        last.append(lax.ppermute(both, RING, ring_route(way)))
    return [term for core in range(2) for term in (own[core], first[core], last[core])]


def sublayer(prompt_ids, prompt_lengths, embed_table, norm_gain, w_query, w_key, w_value, w_out):
    quarter = prompt_ids.shape[0]
    row_count = quarter * TPG
    devices = lax.axis_size(DP_TENSOR)
    columns = embed_table.shape[0]
    model_width = columns * devices
    group_count = devices // TPG
    place = lax.axis_index(RING)
    ring = lax.axis_size(RING)
    group_index = lax.axis_index(DP) * lax.axis_size("tensor_0") + lax.axis_index("tensor_0")
    length = lax.dynamic_slice_in_dim(prompt_lengths, group_index, 1, 0)
    cosine, sine = rope_tables(row_count)

    depth = w_query.shape[0]
    gain = lax.dynamic_slice_in_dim(norm_gain, lax.axis_index(DP) * depth, depth, 0)
    packed = jnp.concatenate([w_query, w_key, w_value], axis=1).astype(jnp.float32)
    packed = (packed * gain[:, None]).astype(jnp.bfloat16)
    w_in = lax.all_gather(collect_blocks(packed), DP, axis=1, tiled=True)
    w_in = w_in.reshape(w_in.shape[0], -1, ring, columns, w_in.shape[-1])
    all_ids = lax.all_to_all(
        jnp.broadcast_to(prompt_ids[None], (devices, quarter)),
        DP_TENSOR,
        split_axis=0,
        concat_axis=0,
        tiled=True,
    ).reshape(-1)
    pieces_x = [w_out]
    for axes, route in (
        ("tensor_0", [(0, 1), (1, 0)]),
        ("dp_1", [(0, 1), (1, 0)]),
        (("dp_1", "tensor_0"), [(0, 3), (1, 2), (2, 1), (3, 0)]),
    ):
        pieces_x.append(lax.ppermute(w_out, axes, route))
    outgoing = lookup(embed_table, all_ids, group_count)
    own = lax.all_to_all(outgoing, PLANE, split_axis=0, concat_axis=0, tiled=True).reshape(
        -1, row_count
    )
    pieces_x, _ = lax.optimization_barrier((pieces_x, outgoing))
    w_mine = {(0, side): jnp.stack(pieces_x[2 * side : 2 * side + 2]) for side in range(2)}
    layers = lax.axis_size("dp_0")
    ahead = [(z, (z + 1) % layers) for z in range(layers)]
    back = [(z, (z - 1) % layers) for z in range(layers)]
    for z, side, before, route in (
        (1, 0, 0, ahead),
        (3, 1, 0, back),
        (1, 1, 0, ahead),
        (3, 0, 0, back),
        (2, 0, 1, ahead),
        (2, 1, 3, back),
    ):
        w_mine[z, side] = lax.ppermute(w_mine[before, side], "dp_0", route)
    w_other = {}
    for z, side in w_mine:
        w_other[z, side] = lax.ppermute(w_mine[z, side], "dp_2", [(0, 1), (1, 0)])

    places = (place + jnp.arange(ring, dtype=jnp.int32)) % ring
    half = own.shape[0] // 2
    low, high = own[:half], own[half:]
    low_before = lax.ppermute(low, RING, ring_route(1))
    high_after = lax.ppermute(high, RING, ring_route(-1))
    high_before = lax.ppermute(high, RING, ring_route(1))
    low_after = lax.ppermute(low, RING, ring_route(-1))
    low_across = lax.ppermute(low_before, RING, ring_route(1))
    high_across = lax.ppermute(high_after, RING, ring_route(-1))

    first = project(places, w_in, [(own, 0, 1, 0)])
    second = project(
        places,
        w_in,
        [
            (low_before, ring - 1, 2, 0),
            (high_before, ring - 1, 2, 1),
            (low_after, 1, 2, 0),
            (high_after, 1, 2, 1),
        ],
        first,
    )
    attended, cache = attend(
        places,
        w_in,
        [(low_across, 2, 2, 0), (high_across, 2, 2, 1)],
        second,
        length,
        cosine,
        sine,
        model_width,
    )

    pieces = [[own], [low_after, high_after], [low_across, high_across], [low_before, high_before]]
    pieces, _ = lax.optimization_barrier((pieces, attended))
    own_rows = residual(places, pieces, columns, quarter)

    sums = ring_sums(attended, w_mine, w_other)
    where = jnp.stack([lax.axis_index(name) for name in DP])
    hidden = finish(where, own_rows, sums, w_out.shape[1])
    return hidden, cache[None]


def solution(mesh):
    split = Mesh(
        mesh.devices.reshape(4, 2, 2, 2, 4), ("dp_0", "dp_1", "dp_2", "tensor_0", "tensor_1")
    )
    placed = (
        P(DP_TENSOR),
        P(),
        P(DP_TENSOR, None),
        P(),
        P(DP, TENSOR),
        P(DP, TENSOR),
        P(DP, TENSOR),
        P(TENSOR, DP),
    )
    return jax.shard_map(
        sublayer,
        mesh=split,
        in_specs=placed,
        out_specs=(P(DP_TENSOR, None), P(DP_TENSOR, None, None, None)),
        check_vma=False,
    )
```

```python
import functools

import jax
import jax.numpy as jnp
from jax import lax
from jax.experimental import pallas as pl
from jax.experimental.pallas import tpu as pltpu
from jax.sharding import Mesh
from jax.sharding import PartitionSpec as P


HEADS = 32
KVH = 8
HD = 128
TPG = 4
AXES = DP_TENSOR = ("dp_0", "dp_1", "dp_2", "tensor_0", "tensor_1")
CHIP_Z, CHIP_X, CORE, FAR_X, RING = AXES
TENSOR = (FAR_X, RING)
DP = (CHIP_Z, CHIP_X, CORE)
PLANE = (CHIP_Z, CHIP_X, CORE, FAR_X)
LANES = 128

norm_eps = 1e-05
rope_theta = 500000.0


def swapped(block, axis, apart):
    count = lax.axis_size(axis)
    route = []
    for low in range(count):
        high = low | 1 << apart
        if high != low and high < count:
            route += [(low, high), (high, low)]
    return lax.ppermute(block, axis, route)


def ordered_pair(mine, theirs, bit_index):
    upper_half = lax.axis_index(TENSOR) >> bit_index & 1 == 1
    first_half = jnp.where(upper_half, theirs, mine)
    second_half = jnp.where(upper_half, mine, theirs)
    return jnp.concatenate([first_half, second_half], axis=0)


def collect_blocks(shard):
    stacked = shard[None]
    theirs = swapped(stacked, TENSOR, 2)
    return ordered_pair(stacked, theirs, 2)


def lane_gather(block, lanes):
    dims = lax.GatherDimensionNumbers(
        offset_dims=(),
        collapsed_slice_dims=(1,),
        start_index_map=(1,),
        operand_batching_dims=(0,),
        start_indices_batching_dims=(0,),
    )
    return lax.gather(
        block,
        lanes[..., None],
        dims,
        slice_sizes=(1, 1),
        mode=lax.GatherScatterMode.PROMISE_IN_BOUNDS,
    )


def lookup_kernel(slots_ref, lanes_ref, table_ref, out_ref, table, tiles, arrived):
    groups, columns, row_count = out_ref.shape
    tile_count = tiles.shape[0] // 2
    slabs = arrived.shape[0]
    slab = tile_count // slabs
    lane = lax.broadcasted_iota(jnp.int32, (columns, LANES), 1).astype(jnp.int16)
    left = lane < jnp.int16(LANES // 2)
    unroll = min(56, slab)

    def incoming(k):
        part = pl.ds(k * slab * LANES, slab * LANES)
        return pltpu.make_async_copy(table_ref.at[:, part], table.at[:, part], arrived.at[k])

    for k in range(slabs):
        incoming(k).start()

    for k in range(slabs):
        incoming(k).wait()

        def prepare(step, carry, k=k):
            first = k * slab + jnp.minimum(step * unroll, slab - unroll)
            for u in range(unroll):
                t = first + u
                tile = table[:, pl.ds(pl.multiple_of(t * LANES, LANES), LANES)]
                tiles[t] = tile
                tiles[t + tile_count] = lane_gather(tile, lane ^ jnp.int16(LANES // 2))
            return carry

        lax.fori_loop(0, -(-slab // unroll), prepare, 0)

    per_group = row_count // LANES
    together = 4

    def one_block(step, carry):
        for part in range(together):
            block = step * together + part
            first = block * LANES
            wanted = jnp.broadcast_to(lanes_ref[pl.ds(block, 1), :], (columns, LANES)).astype(
                jnp.int16
            )
            picked = jnp.zeros((columns, LANES), jnp.bfloat16)
            for i in range(0, LANES, 2):
                pair = jnp.where(
                    left, tiles[slots_ref[first + i]], tiles[slots_ref[first + i + 1]]
                )
                picked = jnp.where(lane >= jnp.int16(i), lane_gather(pair, wanted), picked)
            place = pl.multiple_of(lax.rem(block, per_group) * LANES, LANES)
            out_ref[lax.div(block, per_group), :, pl.ds(place, LANES)] = picked
        return carry

    lax.fori_loop(0, groups * per_group // together, one_block, 0)


def lookup(embed_table, token_ids, group_count):
    columns, vocab_size = embed_table.shape
    tile_count = vocab_size // LANES
    slabs = next(k for k in (6, 4, 3, 2, 1) if tile_count % k == 0)
    count = token_ids.shape[0]
    half = LANES // 2
    odd = jnp.arange(count, dtype=jnp.int32) & 1
    lane = token_ids & (LANES - 1)
    swapped_half = lax.shift_right_logical(lane, 6) ^ odd
    slots = lax.shift_right_logical(token_ids, 7) + tile_count * swapped_half
    lanes = ((lane & (half - 1)) | (odd * half)).reshape(count // LANES, LANES)
    return pl.pallas_call(
        lookup_kernel,
        out_shape=jax.ShapeDtypeStruct((group_count, columns, count // group_count), jnp.bfloat16),
        in_specs=[
            pl.BlockSpec(memory_space=pltpu.SMEM),
            pl.BlockSpec(memory_space=pltpu.VMEM),
            pl.BlockSpec(memory_space=pltpu.HBM),
        ],
        out_specs=pl.BlockSpec(memory_space=pltpu.VMEM),
        scratch_shapes=[
            pltpu.VMEM((columns, vocab_size), jnp.bfloat16),
            pltpu.VMEM((2 * tile_count, columns, LANES), jnp.bfloat16),
            pltpu.SemaphoreType.DMA((slabs,)),
        ],
        compiler_params=pltpu.CompilerParams(vmem_limit_bytes=60 * 2**20),
        cost_estimate=pl.CostEstimate(
            flops=30_000_000_000, bytes_accessed=embed_table.size * 2, transcendentals=0
        ),
    )(slots, lanes, embed_table)


def transposed_product(rows_ref, weight_ref):
    weight = weight_ref[...]
    width = weight.shape[-1]
    return lax.dot_general(
        rows_ref[...],
        weight.reshape(-1, width),
        (((0,), (0,)), ((), ())),
        preferred_element_type=jnp.float32,
    )


def square_sum(rows_ref):
    wide = rows_ref[...].astype(jnp.float32)
    return jnp.sum(wide * wide, axis=0, keepdims=True)


def project_kernel(places_ref, *refs, parts, carried):
    rows, weights = refs[:parts], refs[parts : 2 * parts]
    total_ref, squares_ref = refs[-2:]
    total = sum(transposed_product(r, w) for r, w in zip(rows, weights))
    squares = sum(square_sum(r) for r in rows)
    if carried:
        total += refs[2 * parts][...]
        squares += refs[2 * parts + 1][...]
    total_ref[...] = total
    squares_ref[...] = squares


def weight_spec(weights, turn, share, which):
    _, plane, _, columns, width = weights.shape
    return pl.BlockSpec(
        (1, plane // share, 1, columns, width),
        lambda b, places: (b, which, places[turn], 0, 0),
    )


def project(places, weights, parts, carried=None):
    row_count = parts[0][0].shape[1]
    blocks, width = weights.shape[0], weights.shape[-1]
    in_specs = [pl.BlockSpec(rows.shape, lambda b, places: (0, 0)) for rows, *_ in parts]
    in_specs += [weight_spec(weights, *where) for _, *where in parts]
    total_spec = pl.BlockSpec((row_count, width), lambda b, places: (0, b))
    squares_spec = pl.BlockSpec((1, row_count), lambda b, places: (0, 0))
    operands = [rows for rows, *_ in parts] + [weights] * len(parts)
    if carried is not None:
        in_specs += [total_spec, squares_spec]
        operands += list(carried)
    depth = sum(rows.shape[0] for rows, *_ in parts)
    return pl.pallas_call(
        functools.partial(project_kernel, parts=len(parts), carried=carried is not None),
        grid_spec=pltpu.PrefetchScalarGridSpec(
            num_scalar_prefetch=1,
            grid=(blocks,),
            in_specs=in_specs,
            out_specs=(total_spec, squares_spec),
        ),
        out_shape=(
            jax.ShapeDtypeStruct((row_count, blocks * width), jnp.float32),
            jax.ShapeDtypeStruct((1, row_count), jnp.float32),
        ),
        compiler_params=pltpu.CompilerParams(vmem_limit_bytes=52 * 2**20),
        cost_estimate=pl.CostEstimate(
            flops=2 * row_count * depth * blocks * width,
            bytes_accessed=2 * depth * (blocks * width + row_count),
            transcendentals=0,
        ),
    )(places, *operands)


def attention_kernel(
    places_ref, length_ref, *refs, parts, model_width
):
    rows, weights = refs[:parts], refs[parts : 2 * parts]
    total_ref, squares_ref, cos_ref, sin_ref, attended_ref, cache_ref, proj_ref = refs[2 * parts :]
    row_count = cos_ref.shape[0]
    q_heads = HEADS // KVH
    proj_ref[...] = total_ref[...] + sum(transposed_product(r, w) for r, w in zip(rows, weights))
    squares = squares_ref[...] + sum(square_sum(r) for r in rows)
    scale = lax.rsqrt(squares / model_width + norm_eps)
    scale = jnp.transpose(jnp.broadcast_to(scale, (HD, row_count)))
    cosine = cos_ref[...] * scale
    sine = sin_ref[...] * scale

    def rotate(part):
        return (part * cosine + pltpu.roll(part, HD // 2, 1) * sine).astype(jnp.bfloat16)

    key_rot = rotate(proj_ref[:, q_heads * HD : (q_heads + 1) * HD])
    value = (proj_ref[:, (q_heads + 1) * HD : (q_heads + 2) * HD] * scale).astype(jnp.bfloat16)
    cache_ref[0] = key_rot
    cache_ref[1] = value
    length = length_ref[0]
    block = min(256, row_count)
    power = 1.4426950408889634 / HD**0.5
    for h in range(q_heads):
        query = rotate(proj_ref[:, h * HD : (h + 1) * HD])
        for start in range(0, row_count, block):
            keys = start + block
            scores = lax.dot_general(
                key_rot[:keys],
                query[start : start + block],
                (((1,), (1,)), ((), ())),
                preferred_element_type=jnp.float32,
            )
            q_pos = start + lax.broadcasted_iota(jnp.int32, (1, block), 1)
            k_pos = lax.broadcasted_iota(jnp.int32, (keys, block), 0)
            scores = jnp.where(k_pos < jnp.minimum(q_pos + 1, length), scores, -1e30)
            biggest = jnp.max(scores, axis=0, keepdims=True)
            expd = jnp.exp2((scores - biggest) * power)
            weights_now = expd * (1.0 / jnp.sum(expd, axis=0, keepdims=True))
            attended_ref[start : start + block, h * HD : (h + 1) * HD] = lax.dot_general(
                weights_now.astype(jnp.bfloat16),
                value[:keys],
                (((0,), (0,)), ((), ())),
                preferred_element_type=jnp.float32,
            ).astype(jnp.bfloat16)


def attend(places, weights, parts, carried, length, cosine, sine, model_width):
    row_count = cosine.shape[0]
    blocks, width = weights.shape[0], weights.shape[-1]
    query_width = HEADS // KVH * HD
    in_specs = [pl.BlockSpec(memory_space=pltpu.SMEM)]
    in_specs += [pl.BlockSpec(rows.shape, lambda b, places: (0, 0)) for rows, *_ in parts]
    in_specs += [weight_spec(weights, *where) for _, *where in parts]
    in_specs += [
        pl.BlockSpec((row_count, width), lambda b, places: (0, b)),
        pl.BlockSpec((1, row_count), lambda b, places: (0, 0)),
        pl.BlockSpec((row_count, HD), lambda b, places: (0, 0)),
        pl.BlockSpec((row_count, HD), lambda b, places: (0, 0)),
    ]
    return pl.pallas_call(
        functools.partial(attention_kernel, parts=len(parts), model_width=model_width),
        grid_spec=pltpu.PrefetchScalarGridSpec(
            num_scalar_prefetch=1,
            grid=(blocks,),
            in_specs=in_specs,
            out_specs=(
                pl.BlockSpec((row_count, query_width), lambda b, places: (0, b)),
                pl.BlockSpec((2, row_count, HD), lambda b, places: (0, 0, b)),
            ),
            scratch_shapes=[pltpu.VMEM((row_count, width), jnp.float32)],
        ),
        out_shape=(
            jax.ShapeDtypeStruct((row_count, blocks * query_width), jnp.bfloat16),
            jax.ShapeDtypeStruct((2, row_count, blocks * HD), jnp.bfloat16),
        ),
        compiler_params=pltpu.CompilerParams(vmem_limit_bytes=52 * 2**20),
        cost_estimate=pl.CostEstimate(
            flops=4_000_000_000, bytes_accessed=9_000_000, transcendentals=2_000_000
        ),
        name="attend",
    )(
        places,
        length,
        *[rows for rows, *_ in parts],
        *[weights] * len(parts),
        *carried,
        cosine,
        sine,
    )


def rope_tables(row_count):
    half = HD // 2
    freq = rope_theta ** (-2.0 * jnp.arange(half, dtype=jnp.float32) / HD)
    angle = jnp.arange(row_count, dtype=jnp.int32).astype(jnp.float32)[:, None] * freq[None, :]
    cosine, sine = jnp.cos(angle), jnp.sin(angle)
    return jnp.concatenate([cosine, cosine], axis=1), jnp.concatenate([-sine, sine], axis=1)


def residual_kernel(places_ref, *refs, shares):
    rows_ref, ordered_ref = refs[-2:]
    plane, ring, columns, quarter = ordered_ref.shape
    at = 0
    for turn, share in enumerate(shares):
        count = plane // share
        for piece in range(share):
            ordered_ref[piece * count : (piece + 1) * count, places_ref[turn]] = refs[at][
                ...
            ].reshape(count, columns, quarter)
            at += 1
    width = ring * columns
    for p in range(plane):
        rows_ref[:, p * width : (p + 1) * width] = jnp.transpose(
            ordered_ref[p].reshape(width, quarter).astype(jnp.float32)
        ).astype(jnp.bfloat16)


def residual(places, pieces, columns, quarter):
    flat = [rows for turn in pieces for rows in turn]
    depth = sum(rows.shape[0] for rows in flat)
    ring = len(pieces)
    return pl.pallas_call(
        functools.partial(residual_kernel, shares=[len(turn) for turn in pieces]),
        grid_spec=pltpu.PrefetchScalarGridSpec(
            num_scalar_prefetch=1,
            grid=(1,),
            in_specs=[
                pl.BlockSpec((rows.shape[0], quarter), lambda i, places: (0, places[0]))
                for rows in flat
            ],
            out_specs=pl.BlockSpec((quarter, depth), lambda i, places: (0, 0)),
            scratch_shapes=[
                pltpu.VMEM((depth // (ring * columns), ring, columns, quarter), jnp.bfloat16)
            ],
        ),
        out_shape=jax.ShapeDtypeStruct((quarter, depth), jnp.bfloat16),
        compiler_params=pltpu.CompilerParams(vmem_limit_bytes=16 * 2**20),
        cost_estimate=pl.CostEstimate(
            flops=1_000_000_000, bytes_accessed=4 * depth * quarter, transcendentals=0
        ),
    )(places, *flat)


def ring_route(way):
    count = lax.axis_size(RING)
    return [(k, (k + way) % count) for k in range(count)]


def product_kernel(where_ref, rows_ref, *refs, turns, chunks):
    turned, held, arrived = refs[-3:]
    out_refs = refs[-3 - len(turns) : -3]
    weights = refs[: -3 - len(turns)]
    quarter = out_refs[0].shape[0]
    ring = rows_ref.shape[0] // quarter
    halves, depth, width = weights[0].shape

    def incoming(k, half):
        block = where_ref[1] ^ half
        return pltpu.make_async_copy(
            weights[k].at[half],
            held.at[pl.ds(pl.multiple_of(block * depth, depth), depth), pl.ds(k * width, width)],
            arrived.at[k, half],
        )

    copies = [(k, half) for k in range(len(weights)) for half in range(halves)]
    for copy in copies:
        incoming(*copy).start()
    for at, turn in enumerate(turns):
        block = lax.rem(where_ref[0] + ring + turn, ring)
        turned[at * quarter : (at + 1) * quarter] = rows_ref[
            pl.ds(pl.multiple_of(block * quarter, quarter), quarter)
        ]
    each = len(weights) // chunks
    for chunk in range(chunks):
        for copy in copies[chunk * each * halves : (chunk + 1) * each * halves]:
            incoming(*copy).wait()
        here = slice(chunk * each * width, (chunk + 1) * each * width)
        total = jnp.dot(
            turned[...], held[:, here], preferred_element_type=jnp.float32
        ).astype(jnp.bfloat16)
        for at in range(len(turns)):
            out_refs[at][:, here] = total[at * quarter : (at + 1) * quarter]


def product(where, rows, weights, turns, chunks=2):
    halves, depth, width = weights[0].shape
    row_count = rows.shape[0]
    count = len(weights)
    return pl.pallas_call(
        functools.partial(product_kernel, turns=turns, chunks=chunks),
        in_specs=[pl.BlockSpec(memory_space=pltpu.SMEM), pl.BlockSpec(memory_space=pltpu.VMEM)]
        + [pl.BlockSpec(memory_space=pltpu.HBM)] * count,
        out_specs=tuple([pl.BlockSpec(memory_space=pltpu.VMEM)] * len(turns)),
        out_shape=tuple(
            [jax.ShapeDtypeStruct((row_count // len(turns), count * width), jnp.bfloat16)]
            * len(turns)
        ),
        scratch_shapes=[
            pltpu.VMEM(rows.shape, jnp.bfloat16),
            pltpu.VMEM((halves * depth, count * width), jnp.bfloat16),
            pltpu.SemaphoreType.DMA((count, halves)),
        ],
        compiler_params=pltpu.CompilerParams(vmem_limit_bytes=60 * 2**20),
        cost_estimate=pl.CostEstimate(
            flops=2 * row_count * halves * depth * width * count,
            bytes_accessed=2 * (rows.size + halves * depth * width * count),
            transcendentals=0,
        ),
    )(where, rows, *weights)


LAYERS = (0, 1, 3, 2)


def finish_kernel(where_ref, rows_ref, *refs, width):
    hidden_ref = refs[-1]
    for core in range(2):
        terms = refs[3 * core : 3 * core + 3]
        for j in range(2 * len(LAYERS)):
            z = lax.rem(where_ref[0] + len(LAYERS) - LAYERS[j // 2], len(LAYERS))
            column = (z * 2 + (where_ref[1] ^ (j % 2))) * 2 + (where_ref[2] ^ core)
            here = slice(j * width, (j + 1) * width)
            there = pl.ds(pl.multiple_of(column * width, width), width)
            total = sum(term[:, here].astype(jnp.float32) for term in terms)
            hidden_ref[:, there] = (rows_ref[:, there].astype(jnp.float32) + total).astype(
                jnp.bfloat16
            )


def finish(where, rows, sums, width):
    return pl.pallas_call(
        functools.partial(finish_kernel, width=width),
        out_shape=jax.ShapeDtypeStruct(rows.shape, jnp.bfloat16),
        in_specs=[pl.BlockSpec(memory_space=pltpu.SMEM)]
        + [pl.BlockSpec(memory_space=pltpu.VMEM)] * (1 + len(sums)),
        out_specs=pl.BlockSpec(memory_space=pltpu.VMEM),
        compiler_params=pltpu.CompilerParams(vmem_limit_bytes=16 * 2**20),
        cost_estimate=pl.CostEstimate(
            flops=4 * rows.size, bytes_accessed=8 * rows.size, transcendentals=0
        ),
    )(where, rows, *sums)


def ring_sums(attended, w_mine, w_other):
    where = jnp.stack([lax.axis_index(RING), lax.axis_index(FAR_X)])
    order = [(z, side) for z in LAYERS for side in range(2)]
    own, first, onward = [], [], []
    for way, weights in ((1, w_mine), (-1, w_other)):
        across, against, along, mine = product(
            where, attended, [weights[name] for name in order], [2, -way, way, 0]
        )
        passed = lax.ppermute(across, RING, ring_route(way))
        first.append(lax.ppermute(against, RING, ring_route(-way)))
        own.append(mine)
        onward.append((way, along, passed))
    last = []
    for way, along, passed in onward:
        both = (along.astype(jnp.float32) + passed.astype(jnp.float32)).astype(jnp.bfloat16)
        last.append(lax.ppermute(both, RING, ring_route(way)))
    return [term for core in range(2) for term in (own[core], first[core], last[core])]


def sublayer(prompt_ids, prompt_lengths, embed_table, norm_gain, w_query, w_key, w_value, w_out):
    quarter = prompt_ids.shape[0]
    row_count = quarter * TPG
    devices = lax.axis_size(DP_TENSOR)
    columns = embed_table.shape[0]
    model_width = columns * devices
    group_count = devices // TPG
    place = lax.axis_index(RING)
    ring = lax.axis_size(RING)
    group_index = lax.axis_index(DP) * lax.axis_size(FAR_X) + lax.axis_index(FAR_X)
    length = lax.dynamic_slice_in_dim(prompt_lengths, group_index, 1, 0)
    cosine, sine = rope_tables(row_count)

    depth = w_query.shape[0]
    gain = lax.dynamic_slice_in_dim(norm_gain, lax.axis_index(DP) * depth, depth, 0)
    packed = jnp.concatenate([w_query, w_key, w_value], axis=1).astype(jnp.float32)
    packed = (packed * gain[:, None]).astype(jnp.bfloat16)
    w_in = lax.all_gather(collect_blocks(packed), DP, axis=1, tiled=True)
    w_in = w_in.reshape(w_in.shape[0], -1, ring, columns, w_in.shape[-1])
    all_ids = lax.all_to_all(
        jnp.broadcast_to(prompt_ids[None], (devices, quarter)),
        DP_TENSOR,
        split_axis=0,
        concat_axis=0,
        tiled=True,
    ).reshape(-1)
    pieces_x = [w_out]
    for axes, route in (
        (FAR_X, [(0, 1), (1, 0)]),
        (CHIP_X, [(0, 1), (1, 0)]),
        ((CHIP_X, FAR_X), [(0, 3), (1, 2), (2, 1), (3, 0)]),
    ):
        pieces_x.append(lax.ppermute(w_out, axes, route))
    outgoing = lookup(embed_table, all_ids, group_count)
    own = lax.all_to_all(outgoing, PLANE, split_axis=0, concat_axis=0, tiled=True).reshape(
        -1, row_count
    )
    pieces_x, _ = lax.optimization_barrier((pieces_x, outgoing))
    w_mine = {(0, side): jnp.stack(pieces_x[2 * side : 2 * side + 2]) for side in range(2)}
    layers = lax.axis_size(CHIP_Z)
    ahead = [(z, (z + 1) % layers) for z in range(layers)]
    back = [(z, (z - 1) % layers) for z in range(layers)]
    for z, side, before, route in (
        (1, 0, 0, ahead),
        (3, 1, 0, back),
        (1, 1, 0, ahead),
        (3, 0, 0, back),
        (2, 0, 1, ahead),
        (2, 1, 3, back),
    ):
        w_mine[z, side] = lax.ppermute(w_mine[before, side], CHIP_Z, route)
    w_other = {}
    for z, side in w_mine:
        w_other[z, side] = lax.ppermute(w_mine[z, side], CORE, [(0, 1), (1, 0)])

    places = (place + jnp.arange(ring, dtype=jnp.int32)) % ring
    half = own.shape[0] // 2
    low, high = own[:half], own[half:]
    low_before = lax.ppermute(low, RING, ring_route(1))
    high_after = lax.ppermute(high, RING, ring_route(-1))
    high_before = lax.ppermute(high, RING, ring_route(1))
    low_after = lax.ppermute(low, RING, ring_route(-1))
    low_across = lax.ppermute(low_before, RING, ring_route(1))
    high_across = lax.ppermute(high_after, RING, ring_route(-1))

    first = project(places, w_in, [(own, 0, 1, 0)])
    second = project(
        places,
        w_in,
        [
            (low_before, ring - 1, 2, 0),
            (high_before, ring - 1, 2, 1),
            (low_after, 1, 2, 0),
            (high_after, 1, 2, 1),
        ],
        first,
    )
    attended, cache = attend(
        places,
        w_in,
        [(low_across, 2, 2, 0), (high_across, 2, 2, 1)],
        second,
        length,
        cosine,
        sine,
        model_width,
    )

    pieces = [[own], [low_after, high_after], [low_across, high_across], [low_before, high_before]]
    pieces, _ = lax.optimization_barrier((pieces, attended))
    own_rows = residual(places, pieces, columns, quarter)

    sums = ring_sums(attended, w_mine, w_other)
    where = jnp.stack([lax.axis_index(name) for name in DP])
    hidden = finish(where, own_rows, sums, w_out.shape[1])
    return hidden, cache[None]


def solution(mesh):
    split = Mesh(
        mesh.devices.reshape(4, 2, 2, 2, 4), AXES
    )
    placed = (
        P(DP_TENSOR),
        P(),
        P(DP_TENSOR, None),
        P(),
        P(DP, TENSOR),
        P(DP, TENSOR),
        P(DP, TENSOR),
        P(TENSOR, DP),
    )
    return jax.shard_map(
        sublayer,
        mesh=split,
        in_specs=placed,
        out_specs=(P(DP_TENSOR, None), P(DP_TENSOR, None, None, None)),
        check_vma=False,
    )
```

```python
import functools

import jax
import jax.numpy as jnp
from jax import lax
from jax.experimental import pallas as pl
from jax.experimental.pallas import tpu as pltpu
from jax.sharding import Mesh
from jax.sharding import PartitionSpec as P


HEADS = 32
KVH = 8
HD = 128
TPG = 4
AXES = DP_TENSOR = ("dp_0", "dp_1", "dp_2", "tensor_0", "tensor_1")
CHIP_Z, CHIP_X, CORE, FAR_X, RING = AXES
TENSOR = (FAR_X, RING)
DP = (CHIP_Z, CHIP_X, CORE)
PLANE = (CHIP_Z, CHIP_X, CORE, FAR_X)
LANES = 128

norm_eps = 1e-05
rope_theta = 500000.0


def swapped(block, axis, apart):
    count = lax.axis_size(axis)
    route = []
    for low in range(count):
        high = low | 1 << apart
        if high != low and high < count:
            route += [(low, high), (high, low)]
    return lax.ppermute(block, axis, route)


def ordered_pair(mine, theirs, bit_index):
    upper_half = lax.axis_index(TENSOR) >> bit_index & 1 == 1
    first_half = jnp.where(upper_half, theirs, mine)
    second_half = jnp.where(upper_half, mine, theirs)
    return jnp.concatenate([first_half, second_half], axis=0)


def collect_blocks(shard):
    stacked = shard[None]
    theirs = swapped(stacked, TENSOR, 2)
    return ordered_pair(stacked, theirs, 2)


def lane_gather(block, lanes):
    dims = lax.GatherDimensionNumbers(
        offset_dims=(),
        collapsed_slice_dims=(1,),
        start_index_map=(1,),
        operand_batching_dims=(0,),
        start_indices_batching_dims=(0,),
    )
    return lax.gather(
        block,
        lanes[..., None],
        dims,
        slice_sizes=(1, 1),
        mode=lax.GatherScatterMode.PROMISE_IN_BOUNDS,
    )


def lookup_kernel(slots_ref, lanes_ref, table_ref, out_ref, table, tiles, arrived):
    groups, columns, row_count = out_ref.shape
    tile_count = tiles.shape[0] // 2
    slabs = arrived.shape[0]
    slab = tile_count // slabs
    lane = lax.broadcasted_iota(jnp.int32, (columns, LANES), 1).astype(jnp.int16)
    left = lane < jnp.int16(LANES // 2)
    unroll = min(56, slab)

    def incoming(k):
        part = pl.ds(k * slab * LANES, slab * LANES)
        return pltpu.make_async_copy(table_ref.at[:, part], table.at[:, part], arrived.at[k])

    for k in range(slabs):
        incoming(k).start()

    for k in range(slabs):
        incoming(k).wait()

        def prepare(step, carry, k=k):
            first = k * slab + jnp.minimum(step * unroll, slab - unroll)
            for u in range(unroll):
                t = first + u
                tile = table[:, pl.ds(pl.multiple_of(t * LANES, LANES), LANES)]
                tiles[t] = tile
                tiles[t + tile_count] = lane_gather(tile, lane ^ jnp.int16(LANES // 2))
            return carry

        lax.fori_loop(0, -(-slab // unroll), prepare, 0)

    per_group = row_count // LANES
    together = 4

    def one_block(step, carry):
        for part in range(together):
            block = step * together + part
            first = block * LANES
            wanted = jnp.broadcast_to(lanes_ref[pl.ds(block, 1), :], (columns, LANES)).astype(
                jnp.int16
            )
            picked = jnp.zeros((columns, LANES), jnp.bfloat16)
            for i in range(0, LANES, 2):
                pair = jnp.where(
                    left, tiles[slots_ref[first + i]], tiles[slots_ref[first + i + 1]]
                )
                picked = jnp.where(lane >= jnp.int16(i), lane_gather(pair, wanted), picked)
            place = pl.multiple_of(lax.rem(block, per_group) * LANES, LANES)
            out_ref[lax.div(block, per_group), :, pl.ds(place, LANES)] = picked
        return carry

    lax.fori_loop(0, groups * per_group // together, one_block, 0)


def lookup(embed_table, token_ids, group_count):
    columns, vocab_size = embed_table.shape
    tile_count = vocab_size // LANES
    slabs = next(k for k in (6, 4, 3, 2, 1) if tile_count % k == 0)
    count = token_ids.shape[0]
    half = LANES // 2
    odd = jnp.arange(count, dtype=jnp.int32) & 1
    lane = token_ids & (LANES - 1)
    swapped_half = lax.shift_right_logical(lane, 6) ^ odd
    slots = lax.shift_right_logical(token_ids, 7) + tile_count * swapped_half
    lanes = ((lane & (half - 1)) | (odd * half)).reshape(count // LANES, LANES)
    return pl.pallas_call(
        lookup_kernel,
        out_shape=jax.ShapeDtypeStruct((group_count, columns, count // group_count), jnp.bfloat16),
        in_specs=[
            pl.BlockSpec(memory_space=pltpu.SMEM),
            pl.BlockSpec(memory_space=pltpu.VMEM),
            pl.BlockSpec(memory_space=pltpu.HBM),
        ],
        out_specs=pl.BlockSpec(memory_space=pltpu.VMEM),
        scratch_shapes=[
            pltpu.VMEM((columns, vocab_size), jnp.bfloat16),
            pltpu.VMEM((2 * tile_count, columns, LANES), jnp.bfloat16),
            pltpu.SemaphoreType.DMA((slabs,)),
        ],
        compiler_params=pltpu.CompilerParams(vmem_limit_bytes=60 * 2**20),
        cost_estimate=pl.CostEstimate(
            flops=30_000_000_000, bytes_accessed=embed_table.size * 2, transcendentals=0
        ),
    )(slots, lanes, embed_table)


def transposed_product(rows_ref, weight_ref):
    weight = weight_ref[...]
    width = weight.shape[-1]
    return lax.dot_general(
        rows_ref[...],
        weight.reshape(-1, width),
        (((0,), (0,)), ((), ())),
        preferred_element_type=jnp.float32,
    )


def square_sum(rows_ref):
    wide = rows_ref[...].astype(jnp.float32)
    return jnp.sum(wide * wide, axis=0, keepdims=True)


def project_kernel(places_ref, *refs, parts, carried):
    rows, weights = refs[:parts], refs[parts : 2 * parts]
    total_ref, squares_ref = refs[-2:]
    total = sum(transposed_product(r, w) for r, w in zip(rows, weights))
    squares = sum(square_sum(r) for r in rows)
    if carried:
        total += refs[2 * parts][...]
        squares += refs[2 * parts + 1][...]
    total_ref[...] = total
    squares_ref[...] = squares


def weight_spec(weights, turn, share, which):
    _, plane, _, columns, width = weights.shape
    return pl.BlockSpec(
        (1, plane // share, 1, columns, width),
        lambda b, places: (b, which, places[turn], 0, 0),
    )


def project(places, weights, parts, carried=None):
    row_count = parts[0][0].shape[1]
    blocks, width = weights.shape[0], weights.shape[-1]
    in_specs = [pl.BlockSpec(rows.shape, lambda b, places: (0, 0)) for rows, *_ in parts]
    in_specs += [weight_spec(weights, *where) for _, *where in parts]
    total_spec = pl.BlockSpec((row_count, width), lambda b, places: (0, b))
    squares_spec = pl.BlockSpec((1, row_count), lambda b, places: (0, 0))
    operands = [rows for rows, *_ in parts] + [weights] * len(parts)
    if carried is not None:
        in_specs += [total_spec, squares_spec]
        operands += list(carried)
    depth = sum(rows.shape[0] for rows, *_ in parts)
    return pl.pallas_call(
        functools.partial(project_kernel, parts=len(parts), carried=carried is not None),
        grid_spec=pltpu.PrefetchScalarGridSpec(
            num_scalar_prefetch=1,
            grid=(blocks,),
            in_specs=in_specs,
            out_specs=(total_spec, squares_spec),
        ),
        out_shape=(
            jax.ShapeDtypeStruct((row_count, blocks * width), jnp.float32),
            jax.ShapeDtypeStruct((1, row_count), jnp.float32),
        ),
        compiler_params=pltpu.CompilerParams(vmem_limit_bytes=52 * 2**20),
        cost_estimate=pl.CostEstimate(
            flops=2 * row_count * depth * blocks * width,
            bytes_accessed=2 * depth * (blocks * width + row_count),
            transcendentals=0,
        ),
    )(places, *operands)


def attention_kernel(
    places_ref, length_ref, *refs, parts, model_width
):
    rows, weights = refs[:parts], refs[parts : 2 * parts]
    total_ref, squares_ref, cos_ref, sin_ref, attended_ref, cache_ref, proj_ref = refs[2 * parts :]
    row_count = cos_ref.shape[0]
    q_heads = HEADS // KVH
    proj_ref[...] = total_ref[...] + sum(transposed_product(r, w) for r, w in zip(rows, weights))
    squares = squares_ref[...] + sum(square_sum(r) for r in rows)
    scale = lax.rsqrt(squares / model_width + norm_eps)
    scale = jnp.transpose(jnp.broadcast_to(scale, (HD, row_count)))
    cosine = cos_ref[...] * scale
    sine = sin_ref[...] * scale

    def rotate(part):
        return (part * cosine + pltpu.roll(part, HD // 2, 1) * sine).astype(jnp.bfloat16)

    key_rot = rotate(proj_ref[:, q_heads * HD : (q_heads + 1) * HD])
    value = (proj_ref[:, (q_heads + 1) * HD : (q_heads + 2) * HD] * scale).astype(jnp.bfloat16)
    cache_ref[0] = key_rot
    cache_ref[1] = value
    length = length_ref[0]
    block = min(256, row_count)
    power = 1.4426950408889634 / HD**0.5
    for h in range(q_heads):
        query = rotate(proj_ref[:, h * HD : (h + 1) * HD])
        for start in range(0, row_count, block):
            keys = start + block
            scores = lax.dot_general(
                key_rot[:keys],
                query[start : start + block],
                (((1,), (1,)), ((), ())),
                preferred_element_type=jnp.float32,
            )
            q_pos = start + lax.broadcasted_iota(jnp.int32, (1, block), 1)
            k_pos = lax.broadcasted_iota(jnp.int32, (keys, block), 0)
            scores = jnp.where(k_pos < jnp.minimum(q_pos + 1, length), scores, -1e30)
            biggest = jnp.max(scores, axis=0, keepdims=True)
            expd = jnp.exp2((scores - biggest) * power)
            weights_now = expd * (1.0 / jnp.sum(expd, axis=0, keepdims=True))
            attended_ref[start : start + block, h * HD : (h + 1) * HD] = lax.dot_general(
                weights_now.astype(jnp.bfloat16),
                value[:keys],
                (((0,), (0,)), ((), ())),
                preferred_element_type=jnp.float32,
            ).astype(jnp.bfloat16)


def attend(places, weights, parts, carried, length, cosine, sine, model_width):
    row_count = cosine.shape[0]
    blocks, width = weights.shape[0], weights.shape[-1]
    query_width = HEADS // KVH * HD
    in_specs = [pl.BlockSpec(memory_space=pltpu.SMEM)]
    in_specs += [pl.BlockSpec(rows.shape, lambda b, places: (0, 0)) for rows, *_ in parts]
    in_specs += [weight_spec(weights, *where) for _, *where in parts]
    in_specs += [
        pl.BlockSpec((row_count, width), lambda b, places: (0, b)),
        pl.BlockSpec((1, row_count), lambda b, places: (0, 0)),
        pl.BlockSpec((row_count, HD), lambda b, places: (0, 0)),
        pl.BlockSpec((row_count, HD), lambda b, places: (0, 0)),
    ]
    return pl.pallas_call(
        functools.partial(attention_kernel, parts=len(parts), model_width=model_width),
        grid_spec=pltpu.PrefetchScalarGridSpec(
            num_scalar_prefetch=1,
            grid=(blocks,),
            in_specs=in_specs,
            out_specs=(
                pl.BlockSpec((row_count, query_width), lambda b, places: (0, b)),
                pl.BlockSpec((2, row_count, HD), lambda b, places: (0, 0, b)),
            ),
            scratch_shapes=[pltpu.VMEM((row_count, width), jnp.float32)],
        ),
        out_shape=(
            jax.ShapeDtypeStruct((row_count, blocks * query_width), jnp.bfloat16),
            jax.ShapeDtypeStruct((2, row_count, blocks * HD), jnp.bfloat16),
        ),
        compiler_params=pltpu.CompilerParams(vmem_limit_bytes=52 * 2**20),
        cost_estimate=pl.CostEstimate(
            flops=4_000_000_000, bytes_accessed=9_000_000, transcendentals=2_000_000
        ),
        name="attend",
    )(
        places,
        length,
        *[rows for rows, *_ in parts],
        *[weights] * len(parts),
        *carried,
        cosine,
        sine,
    )


def rope_tables(row_count):
    half = HD // 2
    freq = rope_theta ** (-2.0 * jnp.arange(half, dtype=jnp.float32) / HD)
    angle = jnp.arange(row_count, dtype=jnp.int32).astype(jnp.float32)[:, None] * freq[None, :]
    cosine, sine = jnp.cos(angle), jnp.sin(angle)
    return jnp.concatenate([cosine, cosine], axis=1), jnp.concatenate([-sine, sine], axis=1)


def residual_kernel(places_ref, *refs, shares):
    rows_ref, ordered_ref = refs[-2:]
    plane, ring, columns, quarter = ordered_ref.shape
    at = 0
    for turn, share in enumerate(shares):
        count = plane // share
        for piece in range(share):
            ordered_ref[piece * count : (piece + 1) * count, places_ref[turn]] = refs[at][
                ...
            ].reshape(count, columns, quarter)
            at += 1
    width = ring * columns
    for p in range(plane):
        rows_ref[:, p * width : (p + 1) * width] = jnp.transpose(
            ordered_ref[p].reshape(width, quarter).astype(jnp.float32)
        ).astype(jnp.bfloat16)


def residual(places, pieces, columns, quarter):
    flat = [rows for turn in pieces for rows in turn]
    depth = sum(rows.shape[0] for rows in flat)
    ring = len(pieces)
    return pl.pallas_call(
        functools.partial(residual_kernel, shares=[len(turn) for turn in pieces]),
        grid_spec=pltpu.PrefetchScalarGridSpec(
            num_scalar_prefetch=1,
            grid=(1,),
            in_specs=[
                pl.BlockSpec((rows.shape[0], quarter), lambda i, places: (0, places[0]))
                for rows in flat
            ],
            out_specs=pl.BlockSpec((quarter, depth), lambda i, places: (0, 0)),
            scratch_shapes=[
                pltpu.VMEM((depth // (ring * columns), ring, columns, quarter), jnp.bfloat16)
            ],
        ),
        out_shape=jax.ShapeDtypeStruct((quarter, depth), jnp.bfloat16),
        compiler_params=pltpu.CompilerParams(vmem_limit_bytes=16 * 2**20),
        cost_estimate=pl.CostEstimate(
            flops=1_000_000_000, bytes_accessed=4 * depth * quarter, transcendentals=0
        ),
    )(places, *flat)


def ring_route(way):
    count = lax.axis_size(RING)
    return [(k, (k + way) % count) for k in range(count)]


def product_kernel(where_ref, rows_ref, *refs, turns, chunks):
    turned, held, arrived = refs[-3:]
    out_refs = refs[-3 - len(turns) : -3]
    weights = refs[: -3 - len(turns)]
    quarter = out_refs[0].shape[0]
    ring = rows_ref.shape[0] // quarter
    halves, depth, width = weights[0].shape

    def incoming(k, half):
        block = where_ref[1] ^ half
        return pltpu.make_async_copy(
            weights[k].at[half],
            held.at[pl.ds(pl.multiple_of(block * depth, depth), depth), pl.ds(k * width, width)],
            arrived.at[k, half],
        )

    copies = [(k, half) for k in range(len(weights)) for half in range(halves)]
    for copy in copies:
        incoming(*copy).start()
    for at, turn in enumerate(turns):
        block = lax.rem(where_ref[0] + ring + turn, ring)
        turned[at * quarter : (at + 1) * quarter] = rows_ref[
            pl.ds(pl.multiple_of(block * quarter, quarter), quarter)
        ]
    each = len(weights) // chunks
    for chunk in range(chunks):
        for copy in copies[chunk * each * halves : (chunk + 1) * each * halves]:
            incoming(*copy).wait()
        here = slice(chunk * each * width, (chunk + 1) * each * width)
        total = jnp.dot(
            turned[...], held[:, here], preferred_element_type=jnp.float32
        ).astype(jnp.bfloat16)
        for at in range(len(turns)):
            out_refs[at][:, here] = total[at * quarter : (at + 1) * quarter]


def product(where, rows, weights, turns, chunks=2):
    halves, depth, width = weights[0].shape
    quarter = rows.shape[0] // lax.axis_size(RING)
    count = len(weights)
    return pl.pallas_call(
        functools.partial(product_kernel, turns=turns, chunks=chunks),
        in_specs=[pl.BlockSpec(memory_space=pltpu.SMEM), pl.BlockSpec(memory_space=pltpu.VMEM)]
        + [pl.BlockSpec(memory_space=pltpu.HBM)] * count,
        out_specs=tuple([pl.BlockSpec(memory_space=pltpu.VMEM)] * len(turns)),
        out_shape=tuple(
            [jax.ShapeDtypeStruct((quarter, count * width), jnp.bfloat16)] * len(turns)
        ),
        scratch_shapes=[
            pltpu.VMEM((len(turns) * quarter, rows.shape[1]), jnp.bfloat16),
            pltpu.VMEM((halves * depth, count * width), jnp.bfloat16),
            pltpu.SemaphoreType.DMA((count, halves)),
        ],
        compiler_params=pltpu.CompilerParams(vmem_limit_bytes=60 * 2**20),
        cost_estimate=pl.CostEstimate(
            flops=2 * len(turns) * quarter * halves * depth * width * count,
            bytes_accessed=2 * (rows.size + halves * depth * width * count),
            transcendentals=0,
        ),
    )(where, rows, *weights)


LAYERS = (0, 1, 3, 2)


def added(where_ref, rows_ref, terms, core, width):
    for j in range(2 * len(LAYERS)):
        z = lax.rem(where_ref[0] + len(LAYERS) - LAYERS[j // 2], len(LAYERS))
        column = (z * 2 + (where_ref[1] ^ (j % 2))) * 2 + (where_ref[2] ^ core)
        here = slice(j * width, (j + 1) * width)
        there = pl.ds(pl.multiple_of(column * width, width), width)
        total = sum(term[:, here].astype(jnp.float32) for term in terms)
        yield here, there, (rows_ref[:, there].astype(jnp.float32) + total).astype(jnp.bfloat16)


def first_half_kernel(where_ref, rows_ref, *refs, width):
    for here, _, values in added(where_ref, rows_ref, refs[:-1], 0, width):
        refs[-1][:, here] = values


def second_half_kernel(where_ref, rows_ref, first_ref, *refs, width):
    hidden_ref = refs[-1]
    for here, there, values in added(where_ref, rows_ref, refs[:-1], 1, width):
        hidden_ref[:, there] = values
        other = pl.ds(pl.multiple_of(there.start + (2 * where_ref[2] - 1) * width, width), width)
        hidden_ref[:, other] = first_ref[:, here]


def add_call(kernel, columns, where, operands, width):
    shape = (operands[0].shape[0], columns)
    return pl.pallas_call(
        functools.partial(kernel, width=width),
        out_shape=jax.ShapeDtypeStruct(shape, jnp.bfloat16),
        in_specs=[pl.BlockSpec(memory_space=pltpu.SMEM)]
        + [pl.BlockSpec(memory_space=pltpu.VMEM)] * len(operands),
        out_specs=pl.BlockSpec(memory_space=pltpu.VMEM),
        compiler_params=pltpu.CompilerParams(vmem_limit_bytes=16 * 2**20),
        cost_estimate=pl.CostEstimate(
            flops=4 * shape[0] * columns, bytes_accessed=8 * shape[0] * columns, transcendentals=0
        ),
    )(where, *operands)


def finish(where, rows, sums, width):
    half = sums[0].shape[1]
    first = add_call(first_half_kernel, half, where, [rows, *sums[:3]], width)
    return add_call(second_half_kernel, rows.shape[1], where, [rows, first, *sums[3:]], width)


def ring_sums(attended, w_mine, w_other):
    where = jnp.stack([lax.axis_index(RING), lax.axis_index(FAR_X)])
    order = [(z, side) for z in LAYERS for side in range(2)]
    own, first, onward = [], [], []
    for way, weights in ((1, w_mine), (-1, w_other)):
        pieces = [weights[name] for name in order]
        across, against = product(where, attended, pieces, [2, -way])
        passed = lax.ppermute(across, RING, ring_route(way))
        first.append(lax.ppermute(against, RING, ring_route(-way)))
        onward.append((way, pieces, passed))
    last = []
    for way, pieces, passed in onward:
        along, mine = product(where, attended, pieces, [way, 0])
        own.append(mine)
        both = (along.astype(jnp.float32) + passed.astype(jnp.float32)).astype(jnp.bfloat16)
        last.append(lax.ppermute(both, RING, ring_route(way)))
    return [term for core in range(2) for term in (own[core], first[core], last[core])]


def sublayer(prompt_ids, prompt_lengths, embed_table, norm_gain, w_query, w_key, w_value, w_out):
    quarter = prompt_ids.shape[0]
    row_count = quarter * TPG
    devices = lax.axis_size(DP_TENSOR)
    columns = embed_table.shape[0]
    model_width = columns * devices
    group_count = devices // TPG
    place = lax.axis_index(RING)
    ring = lax.axis_size(RING)
    group_index = lax.axis_index(DP) * lax.axis_size(FAR_X) + lax.axis_index(FAR_X)
    length = lax.dynamic_slice_in_dim(prompt_lengths, group_index, 1, 0)
    cosine, sine = rope_tables(row_count)

    depth = w_query.shape[0]
    gain = lax.dynamic_slice_in_dim(norm_gain, lax.axis_index(DP) * depth, depth, 0)
    packed = jnp.concatenate([w_query, w_key, w_value], axis=1).astype(jnp.float32)
    packed = (packed * gain[:, None]).astype(jnp.bfloat16)
    w_in = lax.all_gather(collect_blocks(packed), DP, axis=1, tiled=True)
    w_in = w_in.reshape(w_in.shape[0], -1, ring, columns, w_in.shape[-1])
    all_ids = lax.all_to_all(
        jnp.broadcast_to(prompt_ids[None], (devices, quarter)),
        DP_TENSOR,
        split_axis=0,
        concat_axis=0,
        tiled=True,
    ).reshape(-1)
    pieces_x = [w_out]
    for axes, route in (
        (FAR_X, [(0, 1), (1, 0)]),
        (CHIP_X, [(0, 1), (1, 0)]),
        ((CHIP_X, FAR_X), [(0, 3), (1, 2), (2, 1), (3, 0)]),
    ):
        pieces_x.append(lax.ppermute(w_out, axes, route))
    outgoing = lookup(embed_table, all_ids, group_count)
    own = lax.all_to_all(outgoing, PLANE, split_axis=0, concat_axis=0, tiled=True).reshape(
        -1, row_count
    )
    pieces_x, _ = lax.optimization_barrier((pieces_x, outgoing))
    w_mine = {(0, side): jnp.stack(pieces_x[2 * side : 2 * side + 2]) for side in range(2)}
    layers = lax.axis_size(CHIP_Z)
    ahead = [(z, (z + 1) % layers) for z in range(layers)]
    back = [(z, (z - 1) % layers) for z in range(layers)]
    for z, side, before, route in (
        (1, 0, 0, ahead),
        (3, 1, 0, back),
        (1, 1, 0, ahead),
        (3, 0, 0, back),
        (2, 0, 1, ahead),
        (2, 1, 3, back),
    ):
        w_mine[z, side] = lax.ppermute(w_mine[before, side], CHIP_Z, route)
    w_other = {}
    for z, side in w_mine:
        w_other[z, side] = lax.ppermute(w_mine[z, side], CORE, [(0, 1), (1, 0)])

    places = (place + jnp.arange(ring, dtype=jnp.int32)) % ring
    half = own.shape[0] // 2
    low, high = own[:half], own[half:]
    low_before = lax.ppermute(low, RING, ring_route(1))
    high_after = lax.ppermute(high, RING, ring_route(-1))
    high_before = lax.ppermute(high, RING, ring_route(1))
    low_after = lax.ppermute(low, RING, ring_route(-1))
    low_across = lax.ppermute(low_before, RING, ring_route(1))
    high_across = lax.ppermute(high_after, RING, ring_route(-1))

    first = project(places, w_in, [(own, 0, 1, 0)])
    second = project(
        places,
        w_in,
        [
            (low_before, ring - 1, 2, 0),
            (high_before, ring - 1, 2, 1),
            (low_after, 1, 2, 0),
            (high_after, 1, 2, 1),
        ],
        first,
    )
    attended, cache = attend(
        places,
        w_in,
        [(low_across, 2, 2, 0), (high_across, 2, 2, 1)],
        second,
        length,
        cosine,
        sine,
        model_width,
    )

    pieces = [[own], [low_after, high_after], [low_across, high_across], [low_before, high_before]]
    pieces, _ = lax.optimization_barrier((pieces, attended))
    own_rows = residual(places, pieces, columns, quarter)

    sums = ring_sums(attended, w_mine, w_other)
    where = jnp.stack([lax.axis_index(name) for name in DP])
    hidden = finish(where, own_rows, sums, w_out.shape[1])
    return hidden, cache[None]


def solution(mesh):
    split = Mesh(
        mesh.devices.reshape(4, 2, 2, 2, 4), AXES
    )
    placed = (
        P(DP_TENSOR),
        P(),
        P(DP_TENSOR, None),
        P(),
        P(DP, TENSOR),
        P(DP, TENSOR),
        P(DP, TENSOR),
        P(TENSOR, DP),
    )
    return jax.shard_map(
        sublayer,
        mesh=split,
        in_specs=placed,
        out_specs=(P(DP_TENSOR, None), P(DP_TENSOR, None, None, None)),
        check_vma=False,
    )
```

```python
import functools

import jax
import jax.numpy as jnp
from jax import lax
from jax.experimental import pallas as pl
from jax.experimental.pallas import tpu as pltpu
from jax.sharding import Mesh
from jax.sharding import PartitionSpec as P


HEADS = 32
KVH = 8
HD = 128
TPG = 4
AXES = DP_TENSOR = ("dp_0", "dp_1", "dp_2", "tensor_0", "tensor_1")
CHIP_Z, CHIP_X, CORE, FAR_X, RING = AXES
TENSOR = (FAR_X, RING)
DP = (CHIP_Z, CHIP_X, CORE)
PLANE = (CHIP_Z, CHIP_X, CORE, FAR_X)
LANES = 128

norm_eps = 1e-05
rope_theta = 500000.0


def swapped(block, axis, apart):
    count = lax.axis_size(axis)
    route = []
    for low in range(count):
        high = low | 1 << apart
        if high != low and high < count:
            route += [(low, high), (high, low)]
    return lax.ppermute(block, axis, route)


def ordered_pair(mine, theirs, bit_index):
    upper_half = lax.axis_index(TENSOR) >> bit_index & 1 == 1
    first_half = jnp.where(upper_half, theirs, mine)
    second_half = jnp.where(upper_half, mine, theirs)
    return jnp.concatenate([first_half, second_half], axis=0)


def collect_blocks(shard):
    stacked = shard[None]
    theirs = swapped(stacked, TENSOR, 2)
    return ordered_pair(stacked, theirs, 2)


def lane_gather(block, lanes):
    dims = lax.GatherDimensionNumbers(
        offset_dims=(),
        collapsed_slice_dims=(1,),
        start_index_map=(1,),
        operand_batching_dims=(0,),
        start_indices_batching_dims=(0,),
    )
    return lax.gather(
        block,
        lanes[..., None],
        dims,
        slice_sizes=(1, 1),
        mode=lax.GatherScatterMode.PROMISE_IN_BOUNDS,
    )


def lookup_kernel(slots_ref, lanes_ref, table_ref, out_ref, table, tiles, arrived):
    groups, columns, row_count = out_ref.shape
    tile_count = tiles.shape[0] // 2
    slabs = arrived.shape[0]
    slab = tile_count // slabs
    lane = lax.broadcasted_iota(jnp.int32, (columns, LANES), 1).astype(jnp.int16)
    left = lane < jnp.int16(LANES // 2)
    unroll = min(84, slab)

    def incoming(k):
        part = pl.ds(k * slab * LANES, slab * LANES)
        return pltpu.make_async_copy(table_ref.at[:, part], table.at[:, part], arrived.at[k])

    for k in range(slabs):
        incoming(k).start()

    for k in range(slabs):
        incoming(k).wait()

        def prepare(step, carry, k=k):
            first = k * slab + jnp.minimum(step * unroll, slab - unroll)
            for u in range(unroll):
                t = first + u
                tile = table[:, pl.ds(pl.multiple_of(t * LANES, LANES), LANES)]
                tiles[t] = tile
                tiles[t + tile_count] = lane_gather(tile, lane ^ jnp.int16(LANES // 2))
            return carry

        lax.fori_loop(0, -(-slab // unroll), prepare, 0)

    per_group = row_count // LANES
    together = 8

    def one_block(step, carry):
        for part in range(together):
            block = step * together + part
            first = block * LANES
            wanted = jnp.broadcast_to(lanes_ref[pl.ds(block, 1), :], (columns, LANES)).astype(
                jnp.int16
            )
            picked = jnp.zeros((columns, LANES), jnp.bfloat16)
            for i in range(0, LANES, 2):
                pair = jnp.where(
                    left, tiles[slots_ref[first + i]], tiles[slots_ref[first + i + 1]]
                )
                picked = jnp.where(lane >= jnp.int16(i), lane_gather(pair, wanted), picked)
            place = pl.multiple_of(lax.rem(block, per_group) * LANES, LANES)
            out_ref[lax.div(block, per_group), :, pl.ds(place, LANES)] = picked
        return carry

    lax.fori_loop(0, groups * per_group // together, one_block, 0)


def lookup(embed_table, token_ids, group_count):
    columns, vocab_size = embed_table.shape
    tile_count = vocab_size // LANES
    slabs = next(k for k in (6, 4, 3, 2, 1) if tile_count % k == 0)
    count = token_ids.shape[0]
    half = LANES // 2
    odd = jnp.arange(count, dtype=jnp.int32) & 1
    lane = token_ids & (LANES - 1)
    swapped_half = lax.shift_right_logical(lane, 6) ^ odd
    slots = lax.shift_right_logical(token_ids, 7) + tile_count * swapped_half
    lanes = ((lane & (half - 1)) | (odd * half)).reshape(count // LANES, LANES)
    return pl.pallas_call(
        lookup_kernel,
        out_shape=jax.ShapeDtypeStruct((group_count, columns, count // group_count), jnp.bfloat16),
        in_specs=[
            pl.BlockSpec(memory_space=pltpu.SMEM),
            pl.BlockSpec(memory_space=pltpu.VMEM),
            pl.BlockSpec(memory_space=pltpu.HBM),
        ],
        out_specs=pl.BlockSpec(memory_space=pltpu.VMEM),
        scratch_shapes=[
            pltpu.VMEM((columns, vocab_size), jnp.bfloat16),
            pltpu.VMEM((2 * tile_count, columns, LANES), jnp.bfloat16),
            pltpu.SemaphoreType.DMA((slabs,)),
        ],
        compiler_params=pltpu.CompilerParams(vmem_limit_bytes=60 * 2**20),
        cost_estimate=pl.CostEstimate(
            flops=30_000_000_000, bytes_accessed=embed_table.size * 2, transcendentals=0
        ),
    )(slots, lanes, embed_table)


def transposed_product(rows_ref, weight_ref):
    weight = weight_ref[...]
    width = weight.shape[-1]
    return lax.dot_general(
        rows_ref[...],
        weight.reshape(-1, width),
        (((0,), (0,)), ((), ())),
        preferred_element_type=jnp.float32,
    )


def square_sum(rows_ref):
    wide = rows_ref[...].astype(jnp.float32)
    return jnp.sum(wide * wide, axis=0, keepdims=True)


def project_kernel(places_ref, *refs, parts, carried):
    rows, weights = refs[:parts], refs[parts : 2 * parts]
    total_ref, squares_ref = refs[-2:]
    total = sum(transposed_product(r, w) for r, w in zip(rows, weights))
    squares = sum(square_sum(r) for r in rows)
    if carried:
        total += refs[2 * parts][...]
        squares += refs[2 * parts + 1][...]
    total_ref[...] = total
    squares_ref[...] = squares


def weight_spec(weights, turn, share, which):
    _, plane, _, columns, width = weights.shape
    return pl.BlockSpec(
        (1, plane // share, 1, columns, width),
        lambda b, places: (b, which, places[turn], 0, 0),
    )


def project(places, weights, parts, carried=None):
    row_count = parts[0][0].shape[1]
    blocks, width = weights.shape[0], weights.shape[-1]
    in_specs = [pl.BlockSpec(rows.shape, lambda b, places: (0, 0)) for rows, *_ in parts]
    in_specs += [weight_spec(weights, *where) for _, *where in parts]
    total_spec = pl.BlockSpec((row_count, width), lambda b, places: (0, b))
    squares_spec = pl.BlockSpec((1, row_count), lambda b, places: (0, 0))
    operands = [rows for rows, *_ in parts] + [weights] * len(parts)
    if carried is not None:
        in_specs += [total_spec, squares_spec]
        operands += list(carried)
    depth = sum(rows.shape[0] for rows, *_ in parts)
    return pl.pallas_call(
        functools.partial(project_kernel, parts=len(parts), carried=carried is not None),
        grid_spec=pltpu.PrefetchScalarGridSpec(
            num_scalar_prefetch=1,
            grid=(blocks,),
            in_specs=in_specs,
            out_specs=(total_spec, squares_spec),
        ),
        out_shape=(
            jax.ShapeDtypeStruct((row_count, blocks * width), jnp.float32),
            jax.ShapeDtypeStruct((1, row_count), jnp.float32),
        ),
        compiler_params=pltpu.CompilerParams(vmem_limit_bytes=52 * 2**20),
        cost_estimate=pl.CostEstimate(
            flops=2 * row_count * depth * blocks * width,
            bytes_accessed=2 * depth * (blocks * width + row_count),
            transcendentals=0,
        ),
    )(places, *operands)


def attention_kernel(
    places_ref, length_ref, *refs, parts, model_width
):
    rows, weights = refs[:parts], refs[parts : 2 * parts]
    total_ref, squares_ref, cos_ref, sin_ref, attended_ref, cache_ref, proj_ref = refs[2 * parts :]
    row_count = cos_ref.shape[0]
    q_heads = HEADS // KVH
    proj_ref[...] = total_ref[...] + sum(transposed_product(r, w) for r, w in zip(rows, weights))
    squares = squares_ref[...] + sum(square_sum(r) for r in rows)
    scale = lax.rsqrt(squares / model_width + norm_eps)
    scale = jnp.transpose(jnp.broadcast_to(scale, (HD, row_count)))
    cosine = cos_ref[...] * scale
    sine = sin_ref[...] * scale

    def rotate(part):
        return (part * cosine + pltpu.roll(part, HD // 2, 1) * sine).astype(jnp.bfloat16)

    key_rot = rotate(proj_ref[:, q_heads * HD : (q_heads + 1) * HD])
    value = (proj_ref[:, (q_heads + 1) * HD : (q_heads + 2) * HD] * scale).astype(jnp.bfloat16)
    cache_ref[0] = key_rot
    cache_ref[1] = value
    length = length_ref[0]
    block = min(256, row_count)
    power = 1.4426950408889634 / HD**0.5
    for h in range(q_heads):
        query = rotate(proj_ref[:, h * HD : (h + 1) * HD])
        for start in range(0, row_count, block):
            keys = start + block
            scores = lax.dot_general(
                key_rot[:keys],
                query[start : start + block],
                (((1,), (1,)), ((), ())),
                preferred_element_type=jnp.float32,
            )
            q_pos = start + lax.broadcasted_iota(jnp.int32, (1, block), 1)
            k_pos = lax.broadcasted_iota(jnp.int32, (keys, block), 0)
            scores = jnp.where(k_pos < jnp.minimum(q_pos + 1, length), scores, -1e30)
            biggest = jnp.max(scores, axis=0, keepdims=True)
            expd = jnp.exp2((scores - biggest) * power)
            weights_now = expd * (1.0 / jnp.sum(expd, axis=0, keepdims=True))
            attended_ref[start : start + block, h * HD : (h + 1) * HD] = lax.dot_general(
                weights_now.astype(jnp.bfloat16),
                value[:keys],
                (((0,), (0,)), ((), ())),
                preferred_element_type=jnp.float32,
            ).astype(jnp.bfloat16)


def attend(places, weights, parts, carried, length, cosine, sine, model_width):
    row_count = cosine.shape[0]
    blocks, width = weights.shape[0], weights.shape[-1]
    query_width = HEADS // KVH * HD
    in_specs = [pl.BlockSpec(memory_space=pltpu.SMEM)]
    in_specs += [pl.BlockSpec(rows.shape, lambda b, places: (0, 0)) for rows, *_ in parts]
    in_specs += [weight_spec(weights, *where) for _, *where in parts]
    in_specs += [
        pl.BlockSpec((row_count, width), lambda b, places: (0, b)),
        pl.BlockSpec((1, row_count), lambda b, places: (0, 0)),
        pl.BlockSpec((row_count, HD), lambda b, places: (0, 0)),
        pl.BlockSpec((row_count, HD), lambda b, places: (0, 0)),
    ]
    return pl.pallas_call(
        functools.partial(attention_kernel, parts=len(parts), model_width=model_width),
        grid_spec=pltpu.PrefetchScalarGridSpec(
            num_scalar_prefetch=1,
            grid=(blocks,),
            in_specs=in_specs,
            out_specs=(
                pl.BlockSpec((row_count, query_width), lambda b, places: (0, b)),
                pl.BlockSpec((2, row_count, HD), lambda b, places: (0, 0, b)),
            ),
            scratch_shapes=[pltpu.VMEM((row_count, width), jnp.float32)],
        ),
        out_shape=(
            jax.ShapeDtypeStruct((row_count, blocks * query_width), jnp.bfloat16),
            jax.ShapeDtypeStruct((2, row_count, blocks * HD), jnp.bfloat16),
        ),
        compiler_params=pltpu.CompilerParams(vmem_limit_bytes=52 * 2**20),
        cost_estimate=pl.CostEstimate(
            flops=4_000_000_000, bytes_accessed=9_000_000, transcendentals=2_000_000
        ),
        name="attend",
    )(
        places,
        length,
        *[rows for rows, *_ in parts],
        *[weights] * len(parts),
        *carried,
        cosine,
        sine,
    )


def rope_tables(row_count):
    half = HD // 2
    freq = rope_theta ** (-2.0 * jnp.arange(half, dtype=jnp.float32) / HD)
    angle = jnp.arange(row_count, dtype=jnp.int32).astype(jnp.float32)[:, None] * freq[None, :]
    cosine, sine = jnp.cos(angle), jnp.sin(angle)
    return jnp.concatenate([cosine, cosine], axis=1), jnp.concatenate([-sine, sine], axis=1)


def residual_kernel(places_ref, *refs, shares):
    rows_ref, ordered_ref = refs[-2:]
    plane, ring, columns, quarter = ordered_ref.shape
    at = 0
    for turn, share in enumerate(shares):
        count = plane // share
        for piece in range(share):
            ordered_ref[piece * count : (piece + 1) * count, places_ref[turn]] = refs[at][
                ...
            ].reshape(count, columns, quarter)
            at += 1
    width = ring * columns
    for p in range(plane):
        rows_ref[:, p * width : (p + 1) * width] = jnp.transpose(
            ordered_ref[p].reshape(width, quarter).astype(jnp.float32)
        ).astype(jnp.bfloat16)


def residual(places, pieces, columns, quarter):
    flat = [rows for turn in pieces for rows in turn]
    depth = sum(rows.shape[0] for rows in flat)
    ring = len(pieces)
    return pl.pallas_call(
        functools.partial(residual_kernel, shares=[len(turn) for turn in pieces]),
        grid_spec=pltpu.PrefetchScalarGridSpec(
            num_scalar_prefetch=1,
            grid=(1,),
            in_specs=[
                pl.BlockSpec((rows.shape[0], quarter), lambda i, places: (0, places[0]))
                for rows in flat
            ],
            out_specs=pl.BlockSpec((quarter, depth), lambda i, places: (0, 0)),
            scratch_shapes=[
                pltpu.VMEM((depth // (ring * columns), ring, columns, quarter), jnp.bfloat16)
            ],
        ),
        out_shape=jax.ShapeDtypeStruct((quarter, depth), jnp.bfloat16),
        compiler_params=pltpu.CompilerParams(vmem_limit_bytes=16 * 2**20),
        cost_estimate=pl.CostEstimate(
            flops=1_000_000_000, bytes_accessed=4 * depth * quarter, transcendentals=0
        ),
    )(places, *flat)


def ring_route(way):
    count = lax.axis_size(RING)
    return [(k, (k + way) % count) for k in range(count)]


def product_kernel(where_ref, rows_ref, *refs, turns, chunks):
    turned, held, arrived = refs[-3:]
    out_refs = refs[-3 - len(turns) : -3]
    weights = refs[: -3 - len(turns)]
    quarter = out_refs[0].shape[0]
    ring = rows_ref.shape[0] // quarter
    halves, depth, width = weights[0].shape

    def incoming(k, half):
        block = where_ref[1] ^ half
        return pltpu.make_async_copy(
            weights[k].at[half],
            held.at[pl.ds(pl.multiple_of(block * depth, depth), depth), pl.ds(k * width, width)],
            arrived.at[k, half],
        )

    copies = [(k, half) for k in range(len(weights)) for half in range(halves)]
    for copy in copies:
        incoming(*copy).start()
    for at, turn in enumerate(turns):
        block = lax.rem(where_ref[0] + ring + turn, ring)
        turned[at * quarter : (at + 1) * quarter] = rows_ref[
            pl.ds(pl.multiple_of(block * quarter, quarter), quarter)
        ]
    each = len(weights) // chunks
    for chunk in range(chunks):
        for copy in copies[chunk * each * halves : (chunk + 1) * each * halves]:
            incoming(*copy).wait()
        here = slice(chunk * each * width, (chunk + 1) * each * width)
        total = jnp.dot(
            turned[...], held[:, here], preferred_element_type=jnp.float32
        ).astype(jnp.bfloat16)
        for at in range(len(turns)):
            out_refs[at][:, here] = total[at * quarter : (at + 1) * quarter]


def product(where, rows, weights, turns, chunks=2):
    halves, depth, width = weights[0].shape
    quarter = rows.shape[0] // lax.axis_size(RING)
    count = len(weights)
    return pl.pallas_call(
        functools.partial(product_kernel, turns=turns, chunks=chunks),
        in_specs=[pl.BlockSpec(memory_space=pltpu.SMEM), pl.BlockSpec(memory_space=pltpu.VMEM)]
        + [pl.BlockSpec(memory_space=pltpu.HBM)] * count,
        out_specs=tuple([pl.BlockSpec(memory_space=pltpu.VMEM)] * len(turns)),
        out_shape=tuple(
            [jax.ShapeDtypeStruct((quarter, count * width), jnp.bfloat16)] * len(turns)
        ),
        scratch_shapes=[
            pltpu.VMEM((len(turns) * quarter, rows.shape[1]), jnp.bfloat16),
            pltpu.VMEM((halves * depth, count * width), jnp.bfloat16),
            pltpu.SemaphoreType.DMA((count, halves)),
        ],
        compiler_params=pltpu.CompilerParams(vmem_limit_bytes=60 * 2**20),
        cost_estimate=pl.CostEstimate(
            flops=2 * len(turns) * quarter * halves * depth * width * count,
            bytes_accessed=2 * (rows.size + halves * depth * width * count),
            transcendentals=0,
        ),
    )(where, rows, *weights)


LAYERS = (0, 1, 3, 2)


def added(where_ref, rows_ref, terms, core, width):
    for j in range(2 * len(LAYERS)):
        z = lax.rem(where_ref[0] + len(LAYERS) - LAYERS[j // 2], len(LAYERS))
        column = (z * 2 + (where_ref[1] ^ (j % 2))) * 2 + (where_ref[2] ^ core)
        here = slice(j * width, (j + 1) * width)
        there = pl.ds(pl.multiple_of(column * width, width), width)
        total = sum(term[:, here].astype(jnp.float32) for term in terms)
        yield here, there, (rows_ref[:, there].astype(jnp.float32) + total).astype(jnp.bfloat16)


def first_half_kernel(where_ref, rows_ref, *refs, width):
    for here, _, values in added(where_ref, rows_ref, refs[:-1], 0, width):
        refs[-1][:, here] = values


def second_half_kernel(where_ref, rows_ref, first_ref, *refs, width):
    hidden_ref = refs[-1]
    for here, there, values in added(where_ref, rows_ref, refs[:-1], 1, width):
        hidden_ref[:, there] = values
        other = pl.ds(pl.multiple_of(there.start + (2 * where_ref[2] - 1) * width, width), width)
        hidden_ref[:, other] = first_ref[:, here]


def add_call(kernel, columns, where, operands, width):
    shape = (operands[0].shape[0], columns)
    return pl.pallas_call(
        functools.partial(kernel, width=width),
        out_shape=jax.ShapeDtypeStruct(shape, jnp.bfloat16),
        in_specs=[pl.BlockSpec(memory_space=pltpu.SMEM)]
        + [pl.BlockSpec(memory_space=pltpu.VMEM)] * len(operands),
        out_specs=pl.BlockSpec(memory_space=pltpu.VMEM),
        compiler_params=pltpu.CompilerParams(vmem_limit_bytes=16 * 2**20),
        cost_estimate=pl.CostEstimate(
            flops=4 * shape[0] * columns, bytes_accessed=8 * shape[0] * columns, transcendentals=0
        ),
    )(where, *operands)


def finish(where, rows, sums, width):
    half = sums[0].shape[1]
    first = add_call(first_half_kernel, half, where, [rows, *sums[:3]], width)
    return add_call(second_half_kernel, rows.shape[1], where, [rows, first, *sums[3:]], width)


def ring_sums(attended, w_mine, w_other):
    where = jnp.stack([lax.axis_index(RING), lax.axis_index(FAR_X)])
    order = [(z, side) for z in LAYERS for side in range(2)]
    own, first, onward = [], [], []
    for way, weights in ((1, w_mine), (-1, w_other)):
        pieces = [weights[name] for name in order]
        across, against = product(where, attended, pieces, [2, -way])
        passed = lax.ppermute(across, RING, ring_route(way))
        first.append(lax.ppermute(against, RING, ring_route(-way)))
        onward.append((way, pieces, passed))
    last = []
    for way, pieces, passed in onward:
        along, mine = product(where, attended, pieces, [way, 0])
        own.append(mine)
        both = (along.astype(jnp.float32) + passed.astype(jnp.float32)).astype(jnp.bfloat16)
        last.append(lax.ppermute(both, RING, ring_route(way)))
    return [term for core in range(2) for term in (own[core], first[core], last[core])]


def sublayer(prompt_ids, prompt_lengths, embed_table, norm_gain, w_query, w_key, w_value, w_out):
    quarter = prompt_ids.shape[0]
    row_count = quarter * TPG
    devices = lax.axis_size(DP_TENSOR)
    columns = embed_table.shape[0]
    model_width = columns * devices
    group_count = devices // TPG
    place = lax.axis_index(RING)
    ring = lax.axis_size(RING)
    group_index = lax.axis_index(DP) * lax.axis_size(FAR_X) + lax.axis_index(FAR_X)
    length = lax.dynamic_slice_in_dim(prompt_lengths, group_index, 1, 0)
    cosine, sine = rope_tables(row_count)

    depth = w_query.shape[0]
    gain = lax.dynamic_slice_in_dim(norm_gain, lax.axis_index(DP) * depth, depth, 0)
    packed = jnp.concatenate([w_query, w_key, w_value], axis=1).astype(jnp.float32)
    packed = (packed * gain[:, None]).astype(jnp.bfloat16)
    w_in = lax.all_gather(collect_blocks(packed), DP, axis=1, tiled=True)
    w_in = w_in.reshape(w_in.shape[0], -1, ring, columns, w_in.shape[-1])
    all_ids = lax.all_to_all(
        jnp.broadcast_to(prompt_ids[None], (devices, quarter)),
        DP_TENSOR,
        split_axis=0,
        concat_axis=0,
        tiled=True,
    ).reshape(-1)
    pieces_x = [w_out]
    for axes, route in (
        (FAR_X, [(0, 1), (1, 0)]),
        (CHIP_X, [(0, 1), (1, 0)]),
        ((CHIP_X, FAR_X), [(0, 3), (1, 2), (2, 1), (3, 0)]),
    ):
        pieces_x.append(lax.ppermute(w_out, axes, route))
    outgoing = lookup(embed_table, all_ids, group_count)
    own = lax.all_to_all(outgoing, PLANE, split_axis=0, concat_axis=0, tiled=True).reshape(
        -1, row_count
    )
    pieces_x, _ = lax.optimization_barrier((pieces_x, outgoing))
    w_mine = {(0, side): jnp.stack(pieces_x[2 * side : 2 * side + 2]) for side in range(2)}
    layers = lax.axis_size(CHIP_Z)
    ahead = [(z, (z + 1) % layers) for z in range(layers)]
    back = [(z, (z - 1) % layers) for z in range(layers)]
    for z, side, before, route in (
        (1, 0, 0, ahead),
        (3, 1, 0, back),
        (1, 1, 0, ahead),
        (3, 0, 0, back),
        (2, 0, 1, ahead),
        (2, 1, 3, back),
    ):
        w_mine[z, side] = lax.ppermute(w_mine[before, side], CHIP_Z, route)
    w_other = {}
    for z, side in w_mine:
        w_other[z, side] = lax.ppermute(w_mine[z, side], CORE, [(0, 1), (1, 0)])

    places = (place + jnp.arange(ring, dtype=jnp.int32)) % ring
    half = own.shape[0] // 2
    low, high = own[:half], own[half:]
    low_before = lax.ppermute(low, RING, ring_route(1))
    high_after = lax.ppermute(high, RING, ring_route(-1))
    high_before = lax.ppermute(high, RING, ring_route(1))
    low_after = lax.ppermute(low, RING, ring_route(-1))
    low_across = lax.ppermute(low_before, RING, ring_route(1))
    high_across = lax.ppermute(high_after, RING, ring_route(-1))

    second = project(
        places,
        w_in,
        [
            (own, 0, 1, 0),
            (low_before, ring - 1, 2, 0),
            (high_before, ring - 1, 2, 1),
            (low_after, 1, 2, 0),
            (high_after, 1, 2, 1),
        ],
    )
    attended, cache = attend(
        places,
        w_in,
        [(low_across, 2, 2, 0), (high_across, 2, 2, 1)],
        second,
        length,
        cosine,
        sine,
        model_width,
    )

    pieces = [[own], [low_after, high_after], [low_across, high_across], [low_before, high_before]]
    pieces, _ = lax.optimization_barrier((pieces, attended))
    own_rows = residual(places, pieces, columns, quarter)

    sums = ring_sums(attended, w_mine, w_other)
    where = jnp.stack([lax.axis_index(name) for name in DP])
    hidden = finish(where, own_rows, sums, w_out.shape[1])
    return hidden, cache[None]


def solution(mesh):
    split = Mesh(
        mesh.devices.reshape(4, 2, 2, 2, 4), AXES
    )
    placed = (
        P(DP_TENSOR),
        P(),
        P(DP_TENSOR, None),
        P(),
        P(DP, TENSOR),
        P(DP, TENSOR),
        P(DP, TENSOR),
        P(TENSOR, DP),
    )
    return jax.shard_map(
        sublayer,
        mesh=split,
        in_specs=placed,
        out_specs=(P(DP_TENSOR, None), P(DP_TENSOR, None, None, None)),
        check_vma=False,
    )
```
